32 devices in a mesh: ctx: 8 (over z, y), tp: 4 (over x, core).
Axes of the slice: x: 2, y: 2, z: 4, core: 2. Of those that a mesh axis runs over, the one named last changes fastest.
Arguments:
- block_input: bfloat16 [2048, 2048], P(('ctx', 'tp')), may hold values from -6 to 6
- qkv_weight: bfloat16 [3, 2048, 2048], P(None, 'ctx', 'tp'), may hold values from -1 to 1
- out_weight: bfloat16 [2048, 2048], P('tp', 'ctx'), may hold values from -4 to 4
- gate_up_weight: bfloat16 [2, 2048, 8192], P(None, 'ctx', 'tp'), may hold values from -0.125 to 0.125
- down_weight: bfloat16 [8192, 2048], P('tp', 'ctx'), may hold values from -0.0625 to 0.0625
- norm_gains: bfloat16 [2, 2048], P(None, 'ctx'), may hold values from 0.5 to 1.5
- positions: int32 [2048], replicated, may hold values from 0 to 2047, as said below
- layer_output_gradient: bfloat16 [2048, 2048], P(('ctx', 'tp')), may hold values from -6 to 6
Outputs:
- block_output: bfloat16 [2048, 2048], P(('ctx', 'tp'))
- layer_input_gradient: float32 [2048, 2048], P(('ctx', 'tp'))
- qkv_grad: float32 [3, 2048, 2048], P(None, 'ctx', 'tp')
- out_weight_grad: float32 [2048, 2048], P('tp', 'ctx')
- gate_up_grad: float32 [2, 2048, 8192], P(None, 'ctx', 'tp')
- down_grad: float32 [8192, 2048], P('tp', 'ctx')
- gain_grad: float32 [2, 2048], P(None, ('ctx', 'tp'))
The draws below stay inside these ranges and needn't reach their ends.
Inputs may be any that keep to these rules, and one draw needn't show every extreme that they name: Each value appears once; the rows of one ctx index hold two runs of 128 consecutive positions, runs number b and 15 - b, with b differing between indices.
All inputs are finite; a program needn't handle non-finite values.
Results may differ from the reference program's by a relative error of at most 0.019.
Values may be sent and summed in bfloat16 or wider, within the bound.
A program may use at most 256 MiB of HBM per device.

```python
import jax
import jax.numpy as jnp
from jax import lax

D = 2048
HEADS = 32
HD = 64
FF = 8192
TOK_DEV = 256
TOKENS = 2048
N_CTX = 8


def draw_positions(key, part):
    order = jax.random.permutation(key, N_CTX)
    half_run = TOK_DEV // 2
    offsets = jnp.arange(half_run, dtype=jnp.int32)
    first_run = order[:, None] * half_run + offsets[None, :]
    second_run = (2 * N_CTX - 1 - order)[:, None] * half_run + offsets[None, :]
    return jnp.concatenate([first_run, second_run], axis=1).reshape(N_CTX * TOK_DEV).astype(jnp.int32)


def draw_qkv_weight(key, part):
    key_common = jax.random.fold_in(key, 11)
    stacked = jax.random.normal(key_common, (3, D, D), jnp.float32) * D ** (-0.5)
    return jnp.clip(stacked, -1.0, 1.0).astype(jnp.bfloat16)


def block_levels(stream_key, shape, split, low, top_value):
    def one(dim, blocks):
        draws = jax.random.uniform(jax.random.fold_in(jax.random.fold_in(stream_key, 6), dim), (blocks,), jnp.float32, low / len(split), top_value / len(split))
        return jnp.repeat(jnp.exp(draws), shape[dim] // blocks).reshape((-1,) + (1,) * (len(shape) - dim - 1))

    factor_of = one(*split[0])
    for cut in split[1:]:
        factor_of = factor_of * one(*cut)
    return factor_of


def centred(stream_key, shape, spread, reach, pieces=(), held_as=jnp.bfloat16):
    array = spread * jax.random.normal(stream_key, shape, jnp.float32)
    if pieces:
        array = array * block_levels(stream_key, shape, pieces, -0.22, 0.18)
    return jnp.clip(array, -reach, reach).astype(held_as)


def setup_inputs(seed: int = 0) -> dict:
    key_list = jax.random.split(jax.random.key(seed), 9)
    block_input = centred(key_list[0], (TOKENS, D), 1.0, 6.0, ((0, 32),))
    qkv_weight = draw_qkv_weight(jax.random.fold_in(key_list[8], 71), 0)
    out_weight = centred(key_list[2], (D, D), (max(1, 2 * D // TOKENS)) ** -0.5, 4.0, ((0, 4), (1, 8)))
    gate_up_weight = centred(key_list[3], (2, D, FF), D ** -0.5, 0.125, ((1, 8), (2, 4)))
    down_weight = centred(key_list[4], (FF, D), FF ** -0.5, 0.0625, ((0, 4), (1, 8)))
    norm_gains = jnp.clip(1.0 + 0.1 * jax.random.normal(key_list[5], (2, D), jnp.float32), 0.5, 1.5).astype(jnp.bfloat16)
    positions = draw_positions(jax.random.fold_in(key_list[8], 71), 0)
    layer_output_gradient = centred(key_list[7], (TOKENS, D), 1.0, 6.0, ((0, 32),))
    return {"block_input": block_input, "qkv_weight": qkv_weight, "out_weight": out_weight, "gate_up_weight": gate_up_weight, "down_weight": down_weight, "norm_gains": norm_gains, "positions": positions, "layer_output_gradient": layer_output_gradient}


norm_eps = 1e-05
rope_base = 130000.0

def inv_rms(values):
    return lax.rsqrt(lax.optimization_barrier(jnp.mean(values * values, axis=-1, keepdims=True)) + norm_eps)

def rope_tables(where_at, head_dim):
    half_dim = head_dim // 2
    inv_freq = rope_base ** (-(jnp.arange(half_dim, dtype=jnp.float32) * 2.0 / head_dim))
    angles = where_at.astype(jnp.float32)[:, None] * inv_freq[None, :]
    return (jnp.cos(angles)[:, None, :], jnp.sin(angles)[:, None, :])

def rotate(values, cos_tab, sin_tab, n_heads, head_dim):
    shaped = values.reshape(values.shape[0], n_heads, head_dim)
    half_dim = head_dim // 2
    lower_half, upper_half = (shaped[..., :half_dim], shaped[..., half_dim:])
    turned = jnp.concatenate([lower_half * cos_tab - upper_half * sin_tab, upper_half * cos_tab + lower_half * sin_tab], axis=-1)
    return turned.reshape(values.shape[0], n_heads * head_dim)

def unrotate(values, cos_tab, sin_tab, n_heads, head_dim):
    shaped = values.reshape(values.shape[0], n_heads, head_dim)
    half_dim = head_dim // 2
    lower_half, upper_half = (shaped[..., :half_dim], shaped[..., half_dim:])
    turned = jnp.concatenate([lower_half * cos_tab + upper_half * sin_tab, upper_half * cos_tab - lower_half * sin_tab], axis=-1)
    return turned.reshape(values.shape[0], n_heads * head_dim)

def ref_scores(query_rows, key_rows, query_pos, key_pos, head_dim):
    scores = jnp.einsum('qhd,khd->hqk', query_rows, key_rows) * head_dim ** (-0.5)
    visible = key_pos[None, None, :] <= query_pos[None, :, None]
    return (jnp.where(visible, scores, -1e+30), visible)

def attend(query_bf, key_bf, value_bf, where_at, n_heads, head_dim):
    n_rows = query_bf.shape[0]
    q_size = min(n_rows, 256)
    key_all = key_bf.astype(jnp.float32).reshape(n_rows, n_heads, head_dim)
    value_all = value_bf.astype(jnp.float32).reshape(n_rows, n_heads, head_dim)

    def one_block(block_index):
        start_row = (block_index * q_size).astype(jnp.int32)
        queries = lax.dynamic_slice_in_dim(query_bf, start_row, q_size, 0).astype(jnp.float32).reshape(q_size, n_heads, head_dim)
        query_pos = lax.dynamic_slice_in_dim(where_at, start_row, q_size, 0)
        scores, visible = ref_scores(queries, key_all, query_pos, where_at, head_dim)
        row_peak = lax.optimization_barrier(jnp.max(scores, axis=-1, keepdims=True))
        log_total = row_peak + jnp.log(lax.optimization_barrier(jnp.sum(jnp.exp(scores - row_peak), axis=-1, keepdims=True)))
        weights = jnp.where(visible, jnp.exp(scores - log_total), 0.0).astype(jnp.bfloat16)
        weights = lax.optimization_barrier(weights)
        mixed_heads = jnp.einsum('hqk,khd->qhd', weights.astype(jnp.float32), value_all)
        return (mixed_heads.reshape(q_size, n_heads * head_dim).astype(jnp.bfloat16), log_total[..., 0])
    outputs, log_totals = lax.map(one_block, jnp.arange(n_rows // q_size, dtype=jnp.int32))
    return (outputs.reshape(n_rows, n_heads * head_dim), log_totals)

def attend_back(query_bf, key_bf, value_bf, attn_bf, attn_grad_bf, log_totals, where_at, n_heads, head_dim):
    n_rows = query_bf.shape[0]
    q_size = min(n_rows, 256)
    score_scale = head_dim ** (-0.5)
    key_all = key_bf.astype(jnp.float32).reshape(n_rows, n_heads, head_dim)
    value_all = value_bf.astype(jnp.float32).reshape(n_rows, n_heads, head_dim)

    def one_step(key_value, block_index):
        key_grad, value_grad = key_value
        start_row = (block_index * q_size).astype(jnp.int32)
        queries = lax.dynamic_slice_in_dim(query_bf, start_row, q_size, 0).astype(jnp.float32).reshape(q_size, n_heads, head_dim)
        out_rows = lax.dynamic_slice_in_dim(attn_bf, start_row, q_size, 0).astype(jnp.float32).reshape(q_size, n_heads, head_dim)
        grad_rows = lax.dynamic_slice_in_dim(attn_grad_bf, start_row, q_size, 0).astype(jnp.float32).reshape(q_size, n_heads, head_dim)
        query_pos = lax.dynamic_slice_in_dim(where_at, start_row, q_size, 0)
        scores, visible = ref_scores(queries, key_all, query_pos, where_at, head_dim)
        prob_rows = jnp.where(visible, jnp.exp(scores - log_totals[block_index][..., None]), 0.0)
        probs_bf = lax.optimization_barrier(prob_rows.astype(jnp.bfloat16)).astype(jnp.float32)
        deltas = lax.optimization_barrier(jnp.sum(grad_rows * out_rows, axis=-1)).T
        prob_grad = jnp.einsum('qhd,khd->hqk', grad_rows, value_all)
        score_grad = (prob_rows * (prob_grad - deltas[..., None]) * score_scale).astype(jnp.bfloat16)
        score_grad = lax.optimization_barrier(score_grad).astype(jnp.float32)
        query_grad = jnp.einsum('hqk,khd->qhd', score_grad, key_all)
        key_grad = key_grad + jnp.einsum('hqk,qhd->khd', score_grad, queries)
        value_grad = value_grad + jnp.einsum('hqk,qhd->khd', probs_bf, grad_rows)
        return ((key_grad, value_grad), query_grad.reshape(q_size, n_heads * head_dim))
    zero_heads = jnp.zeros((n_rows, n_heads, head_dim), jnp.float32)
    (key_grad, value_grad), query_grads = lax.scan(one_step, (zero_heads, zero_heads), jnp.arange(n_rows // q_size, dtype=jnp.int32))
    width = n_heads * head_dim
    return (query_grads.reshape(n_rows, width), key_grad.reshape(n_rows, width), value_grad.reshape(n_rows, width))

def reference(block_input, qkv_weight, out_weight, gate_up_weight, down_weight, norm_gains, positions, layer_output_gradient):
    attention_norm_gain = norm_gains[0].astype(jnp.float32)
    perceptron_norm_gain = norm_gains[1].astype(jnp.float32)
    input_single_precision = block_input.astype(jnp.float32)
    attention_root_mean_square = inv_rms(input_single_precision)
    attention_unit_rows = input_single_precision * attention_root_mean_square
    attention_normed_rows = (attention_unit_rows * attention_norm_gain).astype(jnp.bfloat16)
    cos_tab, sin_tab = rope_tables(positions, HD)
    query_f = jnp.dot(attention_normed_rows, qkv_weight[0], preferred_element_type=jnp.float32)
    key_f = jnp.dot(attention_normed_rows, qkv_weight[1], preferred_element_type=jnp.float32)
    value_f = jnp.dot(attention_normed_rows, qkv_weight[2], preferred_element_type=jnp.float32)
    query_bf = rotate(query_f, cos_tab, sin_tab, HEADS, HD).astype(jnp.bfloat16)
    key_bf = rotate(key_f, cos_tab, sin_tab, HEADS, HD).astype(jnp.bfloat16)
    value_bf = value_f.astype(jnp.bfloat16)
    attn_bf, log_totals = attend(query_bf, key_bf, value_bf, positions, HEADS, HD)
    hidden_residual = input_single_precision + jnp.dot(attn_bf, out_weight, preferred_element_type=jnp.float32)
    perceptron_root_mean_square = inv_rms(hidden_residual)
    perceptron_unit_rows = hidden_residual * perceptron_root_mean_square
    perceptron_normed_rows = (perceptron_unit_rows * perceptron_norm_gain).astype(jnp.bfloat16)
    gate_pre = jnp.dot(perceptron_normed_rows, gate_up_weight[0], preferred_element_type=jnp.float32)
    up_pre = jnp.dot(perceptron_normed_rows, gate_up_weight[1], preferred_element_type=jnp.float32)
    sigmoid_gate = jax.nn.sigmoid(gate_pre)
    activated = gate_pre * sigmoid_gate
    hidden_bf = (activated * up_pre).astype(jnp.bfloat16)
    block_output = (hidden_residual + jnp.dot(hidden_bf, down_weight, preferred_element_type=jnp.float32)).astype(jnp.bfloat16)
    down_grad = jnp.dot(hidden_bf.T, layer_output_gradient, preferred_element_type=jnp.float32)
    hidden_grad = jnp.dot(layer_output_gradient, down_weight.T, preferred_element_type=jnp.float32)
    gate_grad_bf = (hidden_grad * up_pre * (sigmoid_gate * (1.0 + gate_pre * (1.0 - sigmoid_gate)))).astype(jnp.bfloat16)
    up_grad_bf = (hidden_grad * activated).astype(jnp.bfloat16)
    gate_up_grad = jnp.stack([jnp.dot(perceptron_normed_rows.T, gate_grad_bf, preferred_element_type=jnp.float32), jnp.dot(perceptron_normed_rows.T, up_grad_bf, preferred_element_type=jnp.float32)])
    perceptron_normed_gradient = jnp.dot(gate_grad_bf, gate_up_weight[0].T, preferred_element_type=jnp.float32) + jnp.dot(up_grad_bf, gate_up_weight[1].T, preferred_element_type=jnp.float32)
    perceptron_unit_gradient = perceptron_normed_gradient * perceptron_norm_gain
    perceptron_gain_gradient = lax.optimization_barrier(jnp.sum(perceptron_normed_gradient * perceptron_unit_rows, axis=0))
    residual_stream_gradient = layer_output_gradient.astype(jnp.float32) + perceptron_root_mean_square * (perceptron_unit_gradient - perceptron_unit_rows * lax.optimization_barrier(jnp.mean(perceptron_unit_gradient * perceptron_unit_rows, axis=-1, keepdims=True)))
    residual_bf = residual_stream_gradient.astype(jnp.bfloat16)
    out_weight_grad = jnp.dot(attn_bf.T, residual_bf, preferred_element_type=jnp.float32)
    attn_grad_bf = jnp.dot(residual_bf, out_weight.T, preferred_element_type=jnp.float32).astype(jnp.bfloat16)
    query_grad, key_grad, value_grad = attend_back(query_bf, key_bf, value_bf, attn_bf, attn_grad_bf, log_totals, positions, HEADS, HD)
    query_raw = unrotate(query_grad, cos_tab, sin_tab, HEADS, HD).astype(jnp.bfloat16)
    key_raw = unrotate(key_grad, cos_tab, sin_tab, HEADS, HD).astype(jnp.bfloat16)
    value_raw = value_grad.astype(jnp.bfloat16)
    qkv_grad = jnp.stack([jnp.dot(attention_normed_rows.T, query_raw, preferred_element_type=jnp.float32), jnp.dot(attention_normed_rows.T, key_raw, preferred_element_type=jnp.float32), jnp.dot(attention_normed_rows.T, value_raw, preferred_element_type=jnp.float32)])
    attention_normed_gradient = jnp.dot(query_raw, qkv_weight[0].T, preferred_element_type=jnp.float32) + jnp.dot(key_raw, qkv_weight[1].T, preferred_element_type=jnp.float32) + jnp.dot(value_raw, qkv_weight[2].T, preferred_element_type=jnp.float32)
    attention_unit_gradient = attention_normed_gradient * attention_norm_gain
    attention_gain_gradient = lax.optimization_barrier(jnp.sum(attention_normed_gradient * attention_unit_rows, axis=0))
    layer_input_gradient = residual_stream_gradient + attention_root_mean_square * (attention_unit_gradient - attention_unit_rows * lax.optimization_barrier(jnp.mean(attention_unit_gradient * attention_unit_rows, axis=-1, keepdims=True)))
    gain_grad = jnp.stack([attention_gain_gradient, perceptron_gain_gradient])
    return (block_output, layer_input_gradient, qkv_grad, out_weight_grad, gate_up_grad, down_grad, gain_grad)
```

```python
import functools
import math

import jax
import jax.numpy as jnp
from jax import lax
from jax.experimental import pallas as pl
from jax.experimental.pallas import tpu as pltpu
from jax.sharding import PartitionSpec as P

HD = 64
MESH = pl.DeviceIdType.MESH
DMA = pltpu.SemaphoreType.DMA
ANY = pl.BlockSpec(memory_space=pl.ANY)
VMEM = pl.BlockSpec(memory_space=pltpu.VMEM)
bf16 = jnp.bfloat16
f32 = jnp.float32

norm_eps = 1e-05
rope_base = 130000.0


def inv_rms(values):
    return lax.rsqrt(jnp.mean(values * values, axis=-1, keepdims=True) + norm_eps)


def rope_tables(where_at, head_dim):
    half_dim = head_dim // 2
    inv_freq = rope_base ** (-(jnp.arange(half_dim, dtype=f32) * 2.0 / head_dim))
    angles = where_at.astype(f32)[:, None] * inv_freq[None, :]
    return (jnp.cos(angles)[:, None, :], jnp.sin(angles)[:, None, :])


def rotate(values, cos_tab, sin_tab, n_heads, head_dim):
    shaped = values.reshape(values.shape[0], n_heads, head_dim)
    half_dim = head_dim // 2
    lower_half, upper_half = (shaped[..., :half_dim], shaped[..., half_dim:])
    turned = jnp.concatenate(
        [lower_half * cos_tab - upper_half * sin_tab, upper_half * cos_tab + lower_half * sin_tab],
        axis=-1,
    )
    return turned.reshape(values.shape[0], n_heads * head_dim)


def unrotate(values, cos_tab, sin_tab, n_heads, head_dim):
    return rotate(values, cos_tab, -sin_tab, n_heads, head_dim)


class Place:
    def __init__(self, nz):
        ctx, tp = lax.axis_index("ctx"), lax.axis_index("tp")
        self.nz = nz
        self.first = ctx // (2 * nz) * (2 * nz)
        self.z, self.y = (ctx - self.first) // 2, (ctx - self.first) % 2
        self.x, self.k = tp // 2, tp % 2

    def device(self, z, y, x, k):
        return {"ctx": self.first + 2 * z + y, "tp": 2 * x + k}


def slot_of(z, x, k):
    return (z * 2 + x) * 2 + k


class Comm:
    def __init__(self, at, pool):
        self.at, self.pool, self.used, self.ends, self.late = at, pool, 0, [], []
        z, y, x, k, nz = at.z, at.y, at.x, at.k, at.nz
        self.to_x = at.device(z, y, 1 - x, k)
        self.to_k = at.device(z, y, x, 1 - k)
        self.to_y = at.device(z, 1 - y, x, k)
        self.to_xk = at.device(z, y, 1 - x, 1 - k)
        peers = [self.to_x, self.to_k, self.to_y, self.to_xk]
        peers += [at.device((z + d) % nz, y, x, k) for d in range(1, nz)]
        barrier = pltpu.get_barrier_semaphore()
        for peer in peers:
            pl.semaphore_signal(barrier, inc=1, device_id=peer, device_id_type=MESH)
        pl.semaphore_wait(barrier, len(peers))

    def sem(self):
        self.used += 1
        return self.pool.at[self.used - 1]

    def sems(self, n):
        return [self.sem() for _ in range(n)]

    def step(self, arrivals, copies, cond=None, then=None):
        sems = self.sems(len(copies))

        def copy(i):
            src, dst, recv_sem, device = copies[i]
            return pltpu.make_async_remote_copy(
                src_ref=src,
                dst_ref=dst,
                send_sem=sems[i],
                recv_sem=recv_sem,
                device_id=device,
                device_id_type=MESH,
            )

        def go():
            for buf, sem in arrivals:
                self.arrive(buf, sem)
            if then is not None:
                then()
            for i in range(len(copies)):
                copy(i).start()

        def end():
            for i in range(len(copies)):
                copy(i).wait_send()

        if cond is None:
            go()
        else:
            pl.when(cond)(go)
        if copies:
            self.ends.append((cond, end))

    def keep(self, src, dst):
        copy = pltpu.make_async_copy(src, dst, self.sem())
        copy.start()
        self.ends.append((None, copy.wait))

    def arrive(self, buf, recv_sem):
        pltpu.make_async_remote_copy(
            src_ref=buf,
            dst_ref=buf,
            send_sem=recv_sem,
            recv_sem=recv_sem,
            device_id=self.to_k,
            device_id_type=MESH,
        ).wait_recv()

    def finish(self):
        for buf, sem in self.late:
            self.arrive(buf, sem)
        for cond, end in self.ends:
            if cond is None:
                end()
            else:
                pl.when(cond)(end)


def take_turns(*steps):
    steps = list(steps)
    while steps:
        for one in list(steps):
            if next(one, steps) is steps:
                steps.remove(one)


def advance(steps, n):
    for _ in range(n):
        next(steps, None)


def exhaust(*many):
    for steps in many:
        for _ in steps:
            pass


def line(at):
    places = []
    for d in range(1, at.nz):
        places.append((d, -1, (at.z + at.nz - d) % at.nz, at.z >= d))
        places.append((d, 1, (at.z + d) % at.nz, at.z + d < at.nz))
    return places


def z_steps(at):
    return 2 * at.nz - 1


def gather_steps(comm, own, o_ref, lo, size):
    at = comm.at
    z, x, k, nz = at.z, at.x, at.k, at.nz
    rows = own.shape[0]
    places = [(0, 0, z, None)] + line(at)
    n = len(places)
    sem_z, sem_x, sem_k = (comm.sems(m * n) for m in (1, 1, 2))

    def part(slot):
        return o_ref.at[pl.ds(pl.multiple_of(slot * rows + lo, size), size), :]

    for i, (d, side, zi, cond) in enumerate(places):
        slot = slot_of(zi, x, k)
        here = own.at[pl.ds(lo, size), :] if d == 0 else part(slot)
        if d:
            comm.step([(part(slot), sem_z[i])], [], cond)
        for way in (1, -1):
            if d < nz - 1 and side != way:
                on = (z < nz - 1) if way == 1 else (z > 0)
                if cond is not None:
                    on = on & cond
                to = at.device((z + nz + way) % nz, at.y, x, k)
                j = next(j for j, p in enumerate(places) if p[0] == d + 1 and p[1] == -way)
                comm.step([], [(here, part(slot), sem_z[j], to)], on)
        comm.step(
            [],
            [
                (here, part(slot), sem_x[i], comm.to_x),
                (here, part(slot), sem_k[i], comm.to_k),
            ],
            cond,
        )
        if d == 0:
            comm.keep(here, part(slot))
        yield
    for i, (d, side, zi, cond) in enumerate(places):
        slot = slot_of(zi, 1 - x, k)
        comm.step(
            [(part(slot), sem_x[i])], [(part(slot), part(slot), sem_k[n + i], comm.to_k)], cond
        )
        yield
    for h, xh in enumerate((x, 1 - x)):
        for i, (d, side, zi, cond) in enumerate(places):
            comm.step([(part(slot_of(zi, xh, 1 - k)), sem_k[h * n + i])], [], cond)


def add_rows(dst, terms):
    rows = dst.shape[0]
    step = math.gcd(rows, 16)

    def some_rows(i, _):
        r = pl.ds(pl.multiple_of(i * step, step), step)
        total = terms[0][r, :].astype(f32)
        for term in terms[1:]:
            total = total + term[r, :].astype(f32)
        dst[r, :] = total.astype(dst.dtype)
        return 0

    lax.fori_loop(0, rows // step, some_rows, 0)


def far_first(at):
    nz = at.nz
    orders = []
    for z in range(nz):
        others = sorted((c for c in range(nz) if c != z), key=lambda c: (-abs(c - z), c))
        orders.append([(abs(c - z), 1 if c > z else -1, c) for c in others] + [(0, 0, z)])
    here = [1 - ((at.z - c) * (at.z - c) + nz * nz - 1) // (nz * nz) for c in range(nz)]
    return [
        tuple(sum(here[c] * orders[c][t][i] for c in range(nz)) for i in range(3))
        for t in range(nz)
    ]


class Scatter:
    def __init__(self, comm, p_ref, bufs, total):
        nz = comm.at.nz
        self.comm, self.p_ref, self.bufs, self.total = comm, p_ref, bufs, total
        self.targets = far_first(comm.at)
        self.sem_k, self.sem_x = comm.sems(2 * nz), comm.sems(nz)
        self.sem_z = comm.used
        comm.sems(2 * nz)

    def mine(self, zi, flip, core):
        x = self.comm.at.x
        return self.p_ref.at[slot_of(zi, 1 - x if flip else x, core)]

    def passing(self, side, d):
        i = (side + 1) // 2 * self.comm.at.nz + d
        return self.bufs[2].at[i], self.comm.pool.at[self.sem_z + i]

    def first(self, t):
        comm, nz, k = self.comm, self.comm.at.nz, self.comm.at.k
        zi = self.targets[t][2]
        comm.step(
            [],
            [
                (self.mine(zi, flip, 1 - k), self.bufs[0].at[flip * nz + zi],
                 self.sem_k[flip * nz + t], comm.to_k)
                for flip in (1, 0)
            ],
        )

    def second(self, t):
        comm, nz, k = self.comm, self.comm.at.nz, self.comm.at.k
        zi = self.targets[t][2]
        b = self.bufs[0].at[nz + zi]
        comm.step(
            [(b, self.sem_k[nz + t])],
            [(b, self.bufs[1].at[zi], self.sem_x[t], comm.to_x)],
            None,
            lambda: add_rows(b, [b, self.mine(zi, 1, k)]),
        )

    def third(self, t):
        comm, at = self.comm, self.comm.at
        z, nz, k = at.z, at.nz, at.k
        d, side, zi = self.targets[t]
        b, landed = self.bufs[0].at[zi], self.bufs[1].at[zi]
        terms = [b, self.mine(zi, 0, k), landed]
        comm.arrive(b, self.sem_k[t])
        comm.arrive(landed, self.sem_x[t])
        if t == nz - 1:
            add_rows(self.total, terms)
            for way, on in ((1, z > 0), (-1, z < nz - 1)):
                buf, sem = self.passing(way, 0)

                @pl.when(on)
                def _():
                    comm.arrive(buf, sem)
                    add_rows(self.total, [self.total, buf])

            return
        add_rows(b, terms)
        buf, sem = self.passing(side, d)
        behind = z - side

        @pl.when((behind >= 0) & (behind < nz))
        def _():
            comm.arrive(buf, sem)
            add_rows(b, [b, buf])

        dst, sem = self.passing(side, d - 1)
        comm.step([], [(b, dst, sem, at.device(z + side, at.y, at.x, k))])

    def steps(self, produce=None):
        nz = self.comm.at.nz
        for i in range(nz + 2):
            if i < nz:
                if produce is not None:
                    produce(self.targets[i][2])
                self.first(i)
            yield
            for stage, lag in ((self.second, 1), (self.third, 2)):
                if 0 <= i - lag < nz:
                    stage(i - lag)
                    yield


def scatter_bufs(nz, rows, width):
    return [pltpu.VMEM((n * nz, rows, width), bf16) for n in (2, 1, 2)]


def along(ref, axis, i, size):
    r = pl.ds(pl.multiple_of(i * size, size), size)
    before = (slice(None),) * (len(ref.shape) - axis)
    return ref.at[before + (r,) + (slice(None),) * (axis - 1)]


class Swap:
    def __init__(self, array, unit_axis, feature_axis, units, depth, shape, plane=None):
        self.array, self.shape, self.plane = array, shape, plane
        self.unit_axis, self.feature_axis, self.units, self.depth = unit_axis, feature_axis, units, depth
        self.out = jax.ShapeDtypeStruct(shape, bf16)

    def of_units(self, ref, z):
        if self.plane is not None:
            ref = ref.at[self.plane]
        return along(ref, self.unit_axis, z, self.units)

    def of_features(self, ref, z, y):
        return along(ref, self.feature_axis, 2 * z + y, self.depth)


def swap_in(comm, swaps, srcs, dsts):
    at = comm.at
    z, y, x, k, nz = at.z, at.y, at.x, at.k, at.nz
    sem_z = [comm.sems(nz) for _ in swaps]
    sem_y = [comm.sems(nz) for _ in swaps]

    def sends():
        for i, one in enumerate(swaps):
            mine = one.of_features(dsts[i], z, y)
            for d in range(1, nz):
                zi = (z + d) % nz
                comm.step([], [(one.of_units(srcs[i], zi), mine, sem_z[i][d], at.device(zi, y, x, k))])
                yield
            own = one.of_units(srcs[i], z)
            comm.step([], [(own, mine, sem_y[i][0], comm.to_y)])
            comm.keep(own, mine)
            yield

    def passes():
        for i, one in enumerate(swaps):
            for d in range(1, nz):
                come = one.of_features(dsts[i], (z + nz - d) % nz, y)
                comm.step([(come, sem_z[i][d])], [(come, come, sem_y[i][d], comm.to_y)])
                yield
        for i, one in enumerate(swaps):
            for d in range(nz):
                zi = (z + nz - d) % nz
                comm.late.append((one.of_features(dsts[i], zi, 1 - y), sem_y[i][d]))

    return sends(), passes()


def add_piece(dst, src):
    if len(dst.shape) == 3:
        for p in range(dst.shape[0]):
            add_rows(dst.at[p], [dst.at[p], src.at[p]])
    else:
        add_rows(dst, [dst, src])


def swap_out(comm, swaps, srcs, dsts, landed):
    at = comm.at
    z, y, x, k, nz = at.z, at.y, at.x, at.k, at.nz
    sem_y = [comm.sems(nz) for _ in swaps]
    sem_z = [comm.sems(nz) for _ in swaps]

    def sends():
        for i, one in enumerate(swaps):
            for d in list(range(1, nz)) + [0]:
                zi = (z + d) % nz
                comm.step(
                    [], [(one.of_features(srcs[i], zi, 1 - y), landed[i].at[zi], sem_y[i][d], comm.to_y)]
                )
                yield

    def passes():
        for i, one in enumerate(swaps):
            mine = one.of_units(dsts[i], z)
            for d in list(range(1, nz)) + [0]:
                zi = (z + d) % nz
                buf = landed[i].at[zi]
                comm.arrive(buf, sem_y[i][d])
                add_piece(buf, one.of_features(srcs[i], zi, y))
                if d:
                    comm.step([], [(buf, mine, sem_z[i][d], at.device(zi, y, x, k))])
                else:
                    comm.keep(buf, mine)
                yield
        for i, one in enumerate(swaps):
            for d in range(1, nz):
                comm.late.append((one.of_units(dsts[i], (z + nz - d) % nz), sem_z[i][d]))

    return sends(), passes()


def landing(nz, one, user_shape):
    shape = list(user_shape)
    shape[len(shape) - one.feature_axis] = one.depth
    return pltpu.VMEM((nz, *shape), bf16)


def comm_kernel(nz, work, swaps, n_in, n_out, *refs):
    given = [one for one in swaps if one.array is not None]
    m, g = len(swaps), len(given)
    ins, srcs = refs[:n_in], refs[n_in : n_in + g]
    outs = refs[n_in + g : n_in + g + n_out]
    dsts = refs[n_in + g + n_out : n_in + g + n_out + m]
    scratch = refs[n_in + g + n_out + m :]
    comm = Comm(Place(nz), scratch[-1])
    work(comm, (swaps, srcs, dsts), ins, outs, scratch[:-1])
    comm.finish()


def comm_call(name, nz, collective, work, ins, outs, scratch, swaps, swap_spec=ANY, vmem=48):
    given = [one.array for one in swaps if one.array is not None]
    return pl.pallas_call(
        functools.partial(comm_kernel, nz, work, swaps, len(ins), len(outs)),
        out_shape=[jax.ShapeDtypeStruct(s, d) for s, d, _ in outs] + [one.out for one in swaps],
        in_specs=[s for _, s in ins] + [swap_spec] * len(given),
        out_specs=[s for _, _, s in outs] + [ANY] * len(swaps),
        scratch_shapes=scratch + [DMA((600,))],
        compiler_params=pltpu.CompilerParams(
            collective_id=collective, has_side_effects=True, vmem_limit_bytes=vmem * 2**20
        ),
        name=name,
    )(*[v for v, _ in ins], *given)


def by_rows(lo, size, do):
    step = math.gcd(size, 16)

    def some_rows(i, _):
        do(pl.ds(pl.multiple_of(lo + i * step, step), step))
        return 0

    lax.fori_loop(0, size // step, some_rows, 0)


def halves(rows):
    return [(0, rows // 2), (rows // 2, rows // 2)] if rows % 32 == 0 else [(0, rows)]


def feature_pieces(nz, groups, d_model):
    a = 2 * nz
    r = d_model // a // groups
    return [(c, i * r, (i * a + c) * r, r) for c in range(a) for i in range(groups)]


def sum_gains(comm, groups, sums, sorted_sums, landed, total):
    at = comm.at
    z, y, x, k, nz = at.z, at.y, at.x, at.k, at.nz
    for c, lo, col, r in feature_pieces(nz, groups, sums.shape[1]):
        sorted_sums[c % 2, c // 2, :, lo : lo + r] = sums[:, col : col + r]
    sem = comm.sems(4 + nz)
    comm.step([], [(sorted_sums.at[1 - y], landed.at[pl.ds(0, nz)], sem[0], comm.to_y)])
    comm.arrive(landed.at[pl.ds(0, nz)], sem[0])
    sorted_sums[y] += landed[0:nz]
    for d in range(1, nz):
        zi = (z + d) % nz
        comm.step([], [(sorted_sums.at[y, zi], landed.at[nz + d], sem[d], at.device(zi, y, x, k))])
    total[...] = sorted_sums[y, z]
    for d in range(1, nz):
        comm.arrive(landed.at[nz + d], sem[d])
        total[...] += landed[nz + d]
    landed[nz] = total[...]
    for i, to in enumerate((comm.to_k, comm.to_x, comm.to_xk)):
        comm.step([], [(landed.at[nz], landed.at[2 * nz + i], sem[nz + i], to)])
    for i in range(3):
        comm.arrive(landed.at[2 * nz + i], sem[nz + i])
        total[...] += landed[2 * nz + i]


def gains_of_group(comm, groups, gain_ref, landed, gains):
    at = comm.at
    z, y, x, k, nz = at.z, at.y, at.x, at.k, at.nz
    sem = comm.sems(nz + 1)
    for d in range(1, nz):
        to = at.device((z + d) % nz, y, x, k)
        comm.step([], [(gain_ref, landed.at[y, z], sem[d], to)])
    landed[y, z] = gain_ref[...]
    for d in range(1, nz):
        comm.arrive(landed.at[y, (z + nz - d) % nz], sem[d])
    comm.step([], [(landed.at[y], landed.at[y], sem[0], comm.to_y)])
    comm.arrive(landed.at[1 - y], sem[0])
    for c, lo, col, r in feature_pieces(nz, groups, gains.shape[1]):
        gains[:, col : col + r] = landed[c % 2, c // 2, :, lo : lo + r].astype(f32)


def start_work(groups, comm, swap, ins, outs, scratch):
    x_ref, gain_ref = ins
    rows_attn, gains = outs
    normed, landed = scratch
    at = comm.at
    gains_of_group(comm, groups, gain_ref, landed, gains)

    def norm(r):
        x = x_ref[r, :].astype(f32)
        normed[r, :] = (x * inv_rms(x) * gains[0:1, :]).astype(bf16)

    rows = x_ref.shape[0]
    by_rows(0, rows, norm)
    shards = gather_steps(comm, normed, rows_attn, 0, rows)
    sends, passes = swap_in(comm, *swap)
    advance(shards, 1)
    advance(sends, at.nz)
    take_turns(shards, sends)
    exhaust(passes)


def product_into(p_ref, rows, at_slot, lhs, rhs, rhs_dims):
    n = p_ref.shape[2]
    wide = math.gcd(n, 512)
    count = lhs[0].shape[0] // rows
    for j in range(n // wide):
        cols = slice(j * wide, (j + 1) * wide)
        total = None
        for one, right, dims in zip(lhs, rhs, rhs_dims):
            block = right[:, cols] if dims == 0 else right[cols, :]
            term = lax.dot_general(one, block, (((1,), (dims,)), ((), ())), preferred_element_type=f32)
            total = term if total is None else total + term
        p_ref[pl.ds(at_slot, count), :, cols] = total.astype(bf16).reshape(count, rows, wide)


def row_blocks(rows, keys, do):
    step = math.gcd(rows, 128)
    fine = max(16, min(128, 128 * 2048 // keys))
    for i in range(rows // step):

        def some(j, _):
            do(pl.ds(pl.multiple_of(i * step + j * fine, fine), fine))
            return 0

        lax.fori_loop(0, step // fine, some, 0)
        yield


def attend(heads, q_ref, k_ref, v_ref, at_q, at_k, o_ref, lse_ref):
    def block(r):
        visible = at_k[...] <= at_q[r, :]
        for h in range(heads):
            c = slice(h * HD, (h + 1) * HD)
            scores = lax.dot_general(
                q_ref[r, c], k_ref[:, c], (((1,), (1,)), ((), ())), preferred_element_type=f32
            )
            scores = jnp.where(visible, scores, -1e30)
            peak = jnp.max(scores, axis=-1, keepdims=True)
            weights = jnp.exp(scores - peak)
            total = jnp.sum(weights, axis=-1, keepdims=True)
            probs = (weights * (1.0 / total)).astype(bf16)
            o_ref[r, c] = jnp.dot(probs, v_ref[:, c], preferred_element_type=f32).astype(bf16)
            lse_ref[r, h : h + 1] = peak + jnp.log(total)

    yield from row_blocks(q_ref.shape[0], k_ref.shape[0], block)


def attend_back(heads, q_ref, k_ref, v_ref, at_q, at_k, o_ref, lse_ref, do_ref, dq_ref, dk_ref, dv_ref):
    over_rows = (((0,), (0,)), ((), ()))
    over_cols = (((1,), (1,)), ((), ()))
    dk_ref[...] = jnp.zeros_like(dk_ref)
    dv_ref[...] = jnp.zeros_like(dv_ref)

    def block(r):
        visible = at_k[...] <= at_q[r, :]
        for h in range(heads):
            c = slice(h * HD, (h + 1) * HD)
            q, grad = q_ref[r, c], do_ref[r, c]
            scores = lax.dot_general(q, k_ref[:, c], over_cols, preferred_element_type=f32)
            scores = jnp.where(visible, scores, -1e30)
            probs = jnp.exp(scores - lse_ref[r, h : h + 1])
            delta = jnp.sum(
                grad.astype(f32) * o_ref[r, c].astype(f32), axis=-1, keepdims=True
            )
            prob_grad = lax.dot_general(grad, v_ref[:, c], over_cols, preferred_element_type=f32)
            score_grad = (probs * (prob_grad - delta)).astype(bf16)
            dq_ref[r, c] = jnp.dot(score_grad, k_ref[:, c], preferred_element_type=f32) * HD ** (-0.5)
            dk_ref[c, :] += lax.dot_general(q, score_grad, over_rows, preferred_element_type=f32)
            dv_ref[c, :] += lax.dot_general(
                grad, probs.astype(bf16), over_rows, preferred_element_type=f32
            )

    yield from row_blocks(q_ref.shape[0], k_ref.shape[0], block)


def attend_work(heads, comm, swap, ins, outs, scratch):
    q_ref, k_ref, v_ref, at_q, at_k, dy_ref = ins
    o_ref, lse_ref, k_out, v_out, grad_rows = outs
    k_all, v_all = scratch
    at = comm.at
    y, keys = at.y, k_ref.shape[0]

    def half(ref, yy):
        return ref.at[pl.ds(pl.multiple_of(yy * keys, keys), keys), :]

    sem = comm.sems(2)
    for i, (mine, both) in enumerate(((k_ref, k_all), (v_ref, v_all))):
        comm.step([], [(mine, half(both, y), sem[i], comm.to_y)])
        half(both, y)[...] = mine[...]
    grads = gather_steps(comm, dy_ref, grad_rows, 0, dy_ref.shape[0])
    sends, passes = swap_in(comm, *swap)
    advance(grads, 1)
    advance(sends, 4)
    advance(grads, 2)
    for i, (both, out) in enumerate(((k_all, k_out), (v_all, v_out))):
        comm.arrive(half(both, 1 - y), sem[i])
        comm.keep(both, out)
    compute = attend(heads, q_ref, k_all, v_all, at_q, at_k, o_ref, lse_ref)
    take_turns(grads, sends, compute)
    exhaust(passes)


def attend_back_work(heads, comm, swap, ins, outs, scratch):
    q_ref, k_ref, v_ref, at_q, at_k, o_ref, lse_ref, do_ref, p_ref, hidden = ins
    dq_ref, dk_out, dv_out, block_out = outs
    total, dk_ref, dv_ref, going, come, gu_landed = scratch[:6]
    bufs = scratch[6:]
    at = comm.at
    y, keys = at.y, k_ref.shape[0] // 2

    def half(ref, yy):
        return ref.at[:, pl.ds(pl.multiple_of(yy * keys, keys), keys)]

    def out(r):
        block_out[r, :] = (hidden[r, :] + total[r, :]).astype(bf16)

    sends, passes = swap_out(comm, *swap, [gu_landed])
    exhaust(sends)
    steps = Scatter(comm, p_ref, bufs, total).steps()
    compute = attend_back(
        heads, q_ref, k_ref, v_ref, at_q, at_k, o_ref, lse_ref, do_ref, dq_ref, dk_ref, dv_ref
    )
    advance(steps, 2)
    take_turns(compute, steps, passes)
    by_rows(0, hidden.shape[0], out)
    sem = comm.sems(2)
    for i, ref in enumerate((dk_ref, dv_ref)):
        going[i] = half(ref, 1 - y)[...].astype(bf16)
        comm.step([], [(going.at[i], come.at[i], sem[i], comm.to_y)])
    for i, (ref, dst) in enumerate(((dk_ref, dk_out), (dv_ref, dv_out))):
        comm.arrive(come.at[i], sem[i])
        dst[...] = half(ref, y)[...] + come[i].astype(f32)


def middle_work(comm, swap, ins, outs, scratch):
    attn, out_w, x_ref, gains = ins
    hidden, rows_mlp = outs
    normed, p_ref, bufs = scratch[0], scratch[1], scratch[2:]
    rows = x_ref.shape[0]

    def norm(r):
        h = hidden[r, :] + x_ref[r, :].astype(f32)
        hidden[r, :] = h
        normed[r, :] = (h * inv_rms(h) * gains[1:2, :]).astype(bf16)

    def produce(zi):
        r = pl.ds(pl.multiple_of(zi * 4 * rows, 4 * rows), 4 * rows)
        product_into(p_ref, rows, zi * 4, [attn[r, :]], [out_w], [0])

    sends, passes = swap_in(comm, *swap)
    advance(sends, comm.at.nz)
    steps = Scatter(comm, p_ref, bufs, hidden).steps(produce)
    exhaust(steps)
    by_rows(0, rows, norm)
    shards = gather_steps(comm, normed, rows_mlp, 0, rows)
    advance(shards, z_steps(comm.at))
    take_turns(shards, sends, passes)


def norm_back(grad, unit, rms, gain):
    unit_grad = grad * gain
    return rms * (unit_grad - unit * jnp.mean(unit_grad * unit, axis=-1, keepdims=True))


def back_work(groups, comm, swap, ins, outs, scratch):
    rows_mlp, grad_rows, gate_w, up_w, dn_w, hidden, dy_ref, gains = ins
    residual, branch_rows, gain_sum, q_out, gu_out = outs
    total, rounded, p_ref, q_ref, gates, n2, dy, gu_g, dn_g, dn_landed = scratch[:10]
    bufs = scratch[10:]
    at = comm.at
    nz = at.nz
    rows = hidden.shape[0]
    tall = 4 * rows
    gain_sum[...] = jnp.zeros_like(gain_sum)
    sems = comm.sems(2 * nz)

    def load(t, zi):
        r = pl.ds(pl.multiple_of(zi * tall, tall), tall)
        return [
            pltpu.make_async_copy(rows_mlp.at[r, :], n2.at[r, :], sems[2 * t]),
            pltpu.make_async_copy(grad_rows.at[r, :], dy.at[r, :], sems[2 * t + 1]),
        ]

    main = Scatter(comm, p_ref, bufs, total)
    for t in range(nz):
        for copy in load(t, main.targets[t][2]):
            copy.start()
    turn = iter(range(nz))

    def produce(zi):
        for copy in load(next(turn), zi):
            copy.wait()
        r = pl.ds(pl.multiple_of(zi * tall, tall), tall)
        x, g = n2[r, :], dy[r, :]
        gate = jnp.dot(x, gate_w[...], preferred_element_type=f32)
        up = jnp.dot(x, up_w[...], preferred_element_type=f32)
        grad = lax.dot_general(g, dn_w[...], (((1,), (1,)), ((), ())), preferred_element_type=f32)
        sig = jax.nn.sigmoid(gate)
        act = gate * sig
        hid = (act * up).astype(bf16)
        gate_grad = (grad * up * (sig * (1.0 + gate * (1.0 - sig)))).astype(bf16)
        up_grad = (grad * act).astype(bf16)
        gates[0, r, :] = gate_grad
        gates[1, r, :] = up_grad
        gates[2, r, :] = hid
        product_into(p_ref, rows, zi * 4, [gate_grad, up_grad], [gate_w, up_w], [1, 1])
        product_into(q_ref, rows, zi * 4, [hid], [dn_w], [0])

    def back(r):
        h = hidden[r, :]
        rms = inv_rms(h)
        unit, grad = h * rms, total[r, :]
        gain_sum[...] += jnp.sum(grad * unit, axis=0, keepdims=True)
        dh = dy_ref[r, :].astype(f32) + norm_back(grad, unit, rms, gains[1:2, :])
        residual[r, :] = dh
        rounded[r, :] = dh.astype(bf16)

    def gradients():
        d_model = n2.shape[1]
        depth = d_model // (2 * nz)
        over_rows = (((0,), (0,)), ((), ()))
        pieces = feature_pieces(nz, groups, d_model)
        per = max(1, len(pieces) // 8)
        for j in range(0, len(pieces), per):
            for c, lo, col, r in pieces[j : j + per]:
                f, to = slice(col, col + r), slice(c * depth + lo, c * depth + lo + r)
                for p in (0, 1):
                    gu_g[p, to, :] = lax.dot_general(
                        n2[:, f], gates[p], over_rows, preferred_element_type=f32
                    ).astype(bf16)
                dn_g[:, to] = lax.dot_general(
                    gates[2], dy[:, f], over_rows, preferred_element_type=f32
                ).astype(bf16)
            yield

    steps = main.steps(produce)
    others = gradients()
    advance(steps, 3 * nz - 2)
    comm.keep(q_ref, q_out)
    take_turns(steps, others)
    comm.keep(gu_g, gu_out)
    by_rows(0, rows, back)
    shards = gather_steps(comm, rounded, branch_rows, 0, rows)
    sends, passes = swap_out(comm, swap[0], (dn_g,), swap[2], [dn_landed])
    advance(shards, 1)
    exhaust(sends)
    advance(shards, z_steps(at) - 1)
    take_turns(shards, passes)


def last_work(groups, comm, swap, ins, outs, scratch):
    proj_grads, qkv_w, residual, x_ref, gains, gain_sum_2 = ins
    grad_in, gain_out = outs
    total, gain_sums, sorted_sums, landed, qkv_landed, out_landed, p_ref = scratch[:7]
    bufs = scratch[7:]
    rows = x_ref.shape[0]
    gain_sums[0:1, :] = jnp.zeros_like(gain_sum_2)
    gain_sums[1:2, :] = gain_sum_2[...]

    def back(r):
        x = x_ref[r, :].astype(f32)
        rms = inv_rms(x)
        unit, grad = x * rms, total[r, :]
        gain_sums[0:1, :] += jnp.sum(grad * unit, axis=0, keepdims=True)
        grad_in[r, :] = residual[r, :] + norm_back(grad, unit, rms, gains[0:1, :])

    width = qkv_w.shape[2]

    def produce(zi):
        r = pl.ds(pl.multiple_of(zi * 4 * rows, 4 * rows), 4 * rows)
        lhs = [proj_grads[r, p * width : (p + 1) * width] for p in range(3)]
        product_into(p_ref, rows, zi * 4, lhs, [qkv_w.at[p] for p in range(3)], [1] * 3)

    sends, passes = swap_out(comm, *swap, [qkv_landed, out_landed])
    exhaust(sends)
    take_turns(Scatter(comm, p_ref, bufs, total).steps(produce), passes)
    by_rows(0, rows, back)
    sum_gains(comm, groups, gain_sums, sorted_sums, landed, gain_out)


def body(
    block_input,
    qkv_weight,
    out_weight,
    gate_up_weight,
    down_weight,
    norm_gains,
    positions,
    layer_output_gradient,
):
    n_ctx, n_tp = lax.axis_size("ctx"), lax.axis_size("tp")
    nz = math.gcd(qkv_weight.shape[2] // HD, n_ctx // 2)
    nz = math.gcd(nz, 4)
    a = 2 * nz
    b = n_ctx // a
    assert n_tp == 4
    depth = qkv_weight.shape[1] * b
    d_model = depth * a
    width = qkv_weight.shape[2] // nz
    heads = width // HD
    units = down_weight.shape[0] // nz
    rows = block_input.shape[0]
    across = [[i * a + j for i in range(b)] for j in range(a)]

    def over_groups(v, axis):
        return lax.all_gather(v, "ctx", axis=axis, tiled=True, axis_index_groups=across) if b > 1 else v

    def to_groups(v, axis):
        if b == 1:
            return v
        return lax.psum_scatter(
            v, "ctx", scatter_dimension=axis, tiled=True, axis_index_groups=across
        )

    def model_order(v, axis):
        if b == 1:
            return v
        s = v.shape
        w = v.reshape(s[:axis] + (a, b, depth // b) + s[axis + 1 :])
        return jnp.swapaxes(w, axis, axis + 1).reshape(s)

    def swap_order(v, axis):
        if b == 1:
            return v
        s = v.shape
        w = v.reshape(s[:axis] + (b, a, depth // b) + s[axis + 1 :])
        return jnp.swapaxes(w, axis, axis + 1).reshape(s)

    my_gains = over_groups(norm_gains, 1)
    group_rows = 4 * nz * rows
    rows_attn, gains, qkv_w, out_w = comm_call(
        "start", nz, 0, functools.partial(start_work, b),
        [(block_input, VMEM), (my_gains, VMEM)],
        [((group_rows, d_model), bf16, ANY), ((2, d_model), f32, VMEM)],
        [pltpu.VMEM((rows, d_model), bf16), pltpu.VMEM((2, nz) + my_gains.shape, bf16)],
        [Swap(over_groups(qkv_weight, 1), 1, 2, width, depth, (3, d_model, width)),
         Swap(over_groups(out_weight, 1), 2, 1, width, depth, (width, d_model))],
    )
    qkv_w, out_w = model_order(qkv_w, 1), model_order(out_w, 1)

    score_scale = HD ** (-0.5)
    y, group = lax.axis_index("ctx") % 2, lax.axis_index("ctx") // a
    by_place = positions.reshape(b, nz, 2, n_tp * rows)
    key_pos = by_place.transpose(2, 0, 1, 3).reshape(2 * b, group_rows)
    own_pos = lax.dynamic_index_in_dim(key_pos, y * b + group, 0, keepdims=False)
    cos_tab, sin_tab = rope_tables(own_pos, HD)
    projected = jnp.einsum("td,kde->kte", rows_attn, qkv_w, preferred_element_type=f32)
    query_bf = rotate(projected[0], cos_tab, sin_tab, heads, HD).astype(bf16)
    query_bf = query_bf * jnp.asarray(score_scale, bf16)
    key_bf = rotate(projected[1], cos_tab, sin_tab, heads, HD).astype(bf16)
    value_bf = projected[2].astype(bf16)
    places = [(own_pos[:, None], VMEM), (key_pos.reshape(1, -1), VMEM)]
    n_keys = 2 * b * group_rows
    attn_bf, log_total, key_all, value_all, grad_rows, dn_w = comm_call(
        "attend", nz, 1, functools.partial(attend_work, heads),
        [(query_bf, VMEM), (over_groups(key_bf, 0), VMEM), (over_groups(value_bf, 0), VMEM)]
        + places + [(layer_output_gradient, VMEM)],
        [((group_rows, width), bf16, VMEM), ((group_rows, heads), f32, VMEM),
         ((n_keys, width), bf16, ANY), ((n_keys, width), bf16, ANY),
         ((group_rows, d_model), bf16, ANY)],
        [pltpu.VMEM((n_keys, width), bf16), pltpu.VMEM((n_keys, width), bf16)],
        [Swap(over_groups(down_weight, 1), 2, 1, units, depth, (units, d_model))],
    )
    dn_w = model_order(dn_w, 1)
    gu_all = over_groups(gate_up_weight, 1)
    partials = pltpu.VMEM((4 * nz, rows, d_model), bf16)
    hidden, rows_mlp, gate_w, up_w = comm_call(
        "middle", nz, 2, middle_work,
        [(attn_bf, VMEM), (out_w, VMEM), (block_input, VMEM), (gains, VMEM)],
        [((rows, d_model), f32, VMEM), ((group_rows, d_model), bf16, ANY)],
        [pltpu.VMEM((rows, d_model), bf16), partials] + scatter_bufs(nz, rows, d_model),
        [Swap(gu_all, 1, 2, units, depth, (d_model, units), p) for p in (0, 1)],
    )
    gate_w, up_w = model_order(gate_w, 0), model_order(up_w, 0)
    down_swap = Swap(None, 2, 1, units, depth, (nz * units, depth))
    residual_grad, branch_rows, gain_sum_2, mlp_part, gu_grad, dn_back = comm_call(
        "back", nz, 3, functools.partial(back_work, b),
        [(rows_mlp, ANY), (grad_rows, ANY), (gate_w, VMEM), (up_w, VMEM), (dn_w, VMEM),
         (hidden, VMEM), (layer_output_gradient, VMEM), (gains, VMEM)],
        [((rows, d_model), f32, VMEM), ((group_rows, d_model), bf16, ANY),
         ((1, d_model), f32, VMEM), ((4 * nz, rows, d_model), bf16, ANY),
         ((2, d_model, units), bf16, ANY)],
        [pltpu.VMEM((rows, d_model), f32), pltpu.VMEM((rows, d_model), bf16), partials, partials,
         pltpu.VMEM((3, group_rows, units), bf16),
         pltpu.VMEM((group_rows, d_model), bf16), pltpu.VMEM((group_rows, d_model), bf16),
         pltpu.VMEM((2, d_model, units), bf16), pltpu.VMEM((units, d_model), bf16),
         landing(nz, down_swap, (units, d_model))]
        + scatter_bufs(nz, rows, d_model),
        [down_swap],
        vmem=60,
    )
    out_weight_grad = jnp.einsum("te,td->ed", attn_bf, branch_rows, preferred_element_type=f32)
    attn_grad_bf = jnp.einsum("td,ed->te", branch_rows, out_w, preferred_element_type=f32).astype(bf16)
    gu_swap = Swap(gu_grad, 1, 2, units, depth, (2, depth, nz * units))
    query_grad, key_terms, value_terms, block_output, gu_back = comm_call(
        "attend_back", nz, 4, functools.partial(attend_back_work, heads),
        [(query_bf, VMEM), (key_all, VMEM), (value_all, VMEM)] + places
        + [(attn_bf, VMEM), (log_total, VMEM), (attn_grad_bf, VMEM), (mlp_part, VMEM),
           (hidden, VMEM)],
        [((group_rows, width), f32, VMEM), ((width, n_keys // 2), f32, VMEM),
         ((width, n_keys // 2), f32, VMEM), ((rows, d_model), bf16, VMEM)],
        [pltpu.VMEM((rows, d_model), f32), pltpu.VMEM((width, n_keys), f32),
         pltpu.VMEM((width, n_keys), f32), pltpu.VMEM((2, width, n_keys // 2), bf16),
         pltpu.VMEM((2, width, n_keys // 2), bf16), landing(nz, gu_swap, (2, d_model, units))]
        + scatter_bufs(nz, rows, d_model),
        [gu_swap],
        swap_spec=VMEM,
    )
    key_grad, value_grad = key_terms.T, value_terms.T
    if b > 1:
        key_grad = to_groups(key_grad.astype(bf16), 0).astype(f32)
        value_grad = to_groups(value_grad.astype(bf16), 0).astype(f32)
    query_raw = unrotate(query_grad, cos_tab, sin_tab, heads, HD).astype(bf16)
    key_raw = unrotate(key_grad, cos_tab, sin_tab, heads, HD).astype(bf16)
    value_raw = value_grad.astype(bf16)
    proj_grads = jnp.concatenate([query_raw, key_raw, value_raw], axis=1)
    qkv_grad = jnp.einsum(
        "td,kte->kde", rows_attn, jnp.stack([query_raw, key_raw, value_raw]),
        preferred_element_type=f32,
    )
    qkv_swap = Swap(
        swap_order(qkv_grad.astype(bf16), 1), 1, 2, width, depth, (3, depth, nz * width)
    )
    out_swap = Swap(
        swap_order(out_weight_grad.astype(bf16), 1), 2, 1, width, depth, (nz * width, depth)
    )
    layer_input_gradient, gain_sums, qkv_back, out_back = comm_call(
        "last", nz, 5, functools.partial(last_work, b),
        [(proj_grads, VMEM), (qkv_w, VMEM), (residual_grad, VMEM), (block_input, VMEM),
         (gains, VMEM), (gain_sum_2, VMEM)],
        [((rows, d_model), f32, VMEM), ((2, depth), f32, VMEM)],
        [pltpu.VMEM((rows, d_model), f32), pltpu.VMEM((2, d_model), f32),
         pltpu.VMEM((2, nz, 2, depth), f32), pltpu.VMEM((2 * nz + 3, 2, depth), f32),
         landing(nz, qkv_swap, (3, d_model, width)), landing(nz, out_swap, (width, d_model)),
         partials] + scatter_bufs(nz, rows, d_model),
        [qkv_swap, out_swap],
        swap_spec=VMEM,
    )
    if b > 1:
        gain_sums = lax.psum(gain_sums, "ctx", axis_index_groups=across)
    gain_cols = d_model // (n_ctx * n_tp)
    gain_part = lax.dynamic_slice_in_dim(
        gain_sums, (group * n_tp + lax.axis_index("tp")) * gain_cols, gain_cols, 1
    )
    return (
        block_output,
        layer_input_gradient,
        to_groups(qkv_back, 1).astype(f32),
        to_groups(out_back, 1).astype(f32),
        to_groups(gu_back, 1).astype(f32),
        to_groups(dn_back, 1).astype(f32),
        gain_part,
    )


def solution(mesh):
    placed = (
        P(("ctx", "tp"), None),
        P(None, "ctx", "tp"),
        P("tp", "ctx"),
        P(None, "ctx", "tp"),
        P("tp", "ctx"),
        P(None, "ctx"),
        P(),
        P(("ctx", "tp"), None),
    )
    return jax.shard_map(
        body,
        mesh=mesh,
        in_specs=placed,
        out_specs=(
            P(("ctx", "tp"), None),
            P(("ctx", "tp"), None),
            P(None, "ctx", "tp"),
            P("tp", "ctx"),
            P(None, "ctx", "tp"),
            P("tp", "ctx"),
            P(None, ("ctx", "tp")),
        ),
        check_vma=False,
    )
```

```python
import functools
import math

import jax
import jax.numpy as jnp
from jax import lax
from jax.experimental import pallas as pl
from jax.experimental.pallas import tpu as pltpu
from jax.sharding import PartitionSpec as P

HD = 64
MESH = pl.DeviceIdType.MESH
DMA = pltpu.SemaphoreType.DMA
ANY = pl.BlockSpec(memory_space=pl.ANY)
VMEM = pl.BlockSpec(memory_space=pltpu.VMEM)
bf16 = jnp.bfloat16
f32 = jnp.float32

norm_eps = 1e-05
rope_base = 130000.0


def inv_rms(values):
    return lax.rsqrt(jnp.mean(values * values, axis=-1, keepdims=True) + norm_eps)


def rope_tables(where_at, head_dim):
    half_dim = head_dim // 2
    inv_freq = rope_base ** (-(jnp.arange(half_dim, dtype=f32) * 2.0 / head_dim))
    angles = where_at.astype(f32)[:, None] * inv_freq[None, :]
    return (jnp.cos(angles)[:, None, :], jnp.sin(angles)[:, None, :])


def rotate(values, cos_tab, sin_tab, n_heads, head_dim):
    shaped = values.reshape(values.shape[0], n_heads, head_dim)
    half_dim = head_dim // 2
    lower_half, upper_half = (shaped[..., :half_dim], shaped[..., half_dim:])
    turned = jnp.concatenate(
        [lower_half * cos_tab - upper_half * sin_tab, upper_half * cos_tab + lower_half * sin_tab],
        axis=-1,
    )
    return turned.reshape(values.shape[0], n_heads * head_dim)


def unrotate(values, cos_tab, sin_tab, n_heads, head_dim):
    return rotate(values, cos_tab, -sin_tab, n_heads, head_dim)


class Place:
    def __init__(self, nz):
        ctx, tp = lax.axis_index("ctx"), lax.axis_index("tp")
        self.nz = nz
        self.first = ctx // (2 * nz) * (2 * nz)
        self.z, self.y = (ctx - self.first) // 2, (ctx - self.first) % 2
        self.x, self.k = tp // 2, tp % 2

    def device(self, z, y, x, k):
        return {"ctx": self.first + 2 * z + y, "tp": 2 * x + k}

    def elsewhere(self, g, flip):
        n = lax.axis_size("ctx")
        y = self.y + flip * (1 - 2 * self.y)
        return {"ctx": (self.first + g * 2 * self.nz) % n + 2 * self.z + y}


def slot_of(z, x, k):
    return (z * 2 + x) * 2 + k


class Comm:
    def __init__(self, at, pool, groups=1):
        self.at, self.pool, self.used, self.ends, self.late = at, pool, 0, [], []
        z, y, x, k, nz = at.z, at.y, at.x, at.k, at.nz
        self.to_x = at.device(z, y, 1 - x, k)
        self.to_k = at.device(z, y, x, 1 - k)
        self.to_y = at.device(z, 1 - y, x, k)
        self.to_xk = at.device(z, y, 1 - x, 1 - k)
        peers = [self.to_x, self.to_k, self.to_y, self.to_xk]
        self.afar = [(g, f, at.elsewhere(g, f)) for g in range(1, groups) for f in (0, 1)]
        peers += [device for _, _, device in self.afar]
        peers += [at.device((z + d) % nz, y, x, k) for d in range(1, nz)]
        barrier = pltpu.get_barrier_semaphore()
        for peer in peers:
            pl.semaphore_signal(barrier, inc=1, device_id=peer, device_id_type=MESH)
        pl.semaphore_wait(barrier, len(peers))

    def sem(self):
        self.used += 1
        return self.pool.at[self.used - 1]

    def sems(self, n):
        return [self.sem() for _ in range(n)]

    def step(self, arrivals, copies, cond=None, then=None):
        sems = self.sems(len(copies))

        def copy(i):
            src, dst, recv_sem, device = copies[i]
            return pltpu.make_async_remote_copy(
                src_ref=src,
                dst_ref=dst,
                send_sem=sems[i],
                recv_sem=recv_sem,
                device_id=device,
                device_id_type=MESH,
            )

        def go():
            for buf, sem in arrivals:
                self.arrive(buf, sem)
            if then is not None:
                then()
            for i in range(len(copies)):
                copy(i).start()

        def end():
            for i in range(len(copies)):
                copy(i).wait_send()

        if cond is None:
            go()
        else:
            pl.when(cond)(go)
        if copies:
            self.ends.append((cond, end))

    def move(self, src, dst):
        copy = pltpu.make_async_copy(src, dst, self.sem())
        copy.start()
        return copy.wait

    def keep(self, src, dst):
        self.ends.append((None, self.move(src, dst)))

    def arrive(self, buf, recv_sem):
        pltpu.make_async_remote_copy(
            src_ref=buf,
            dst_ref=buf,
            send_sem=recv_sem,
            recv_sem=recv_sem,
            device_id=self.to_k,
            device_id_type=MESH,
        ).wait_recv()

    def finish(self):
        for buf, sem in self.late:
            self.arrive(buf, sem)
        for cond, end in self.ends:
            if cond is None:
                end()
            else:
                pl.when(cond)(end)


def take_turns(*steps):
    steps = list(steps)
    while steps:
        for one in list(steps):
            if next(one, steps) is steps:
                steps.remove(one)


def advance(steps, n):
    for _ in range(n):
        next(steps, None)


def exhaust(*many):
    for steps in many:
        for _ in steps:
            pass


def line(at):
    places = []
    for d in range(1, at.nz):
        places.append((d, -1, (at.z + at.nz - d) % at.nz, at.z >= d))
        places.append((d, 1, (at.z + d) % at.nz, at.z + d < at.nz))
    return places


def z_steps(at):
    return 2 * at.nz - 1


def gather_steps(comm, own, o_ref, lo, size):
    at = comm.at
    z, x, k, nz = at.z, at.x, at.k, at.nz
    rows = own.shape[0]
    places = [(0, 0, z, None)] + line(at)
    n = len(places)
    sem_z, sem_x, sem_k = (comm.sems(m * n) for m in (1, 1, 2))

    def part(slot):
        return o_ref.at[pl.ds(pl.multiple_of(slot * rows + lo, size), size), :]

    for i, (d, side, zi, cond) in enumerate(places):
        slot = slot_of(zi, x, k)
        here = own.at[pl.ds(lo, size), :] if d == 0 else part(slot)
        if d:
            comm.step([(part(slot), sem_z[i])], [], cond)
        for way in (1, -1):
            if d < nz - 1 and side != way:
                on = (z < nz - 1) if way == 1 else (z > 0)
                if cond is not None:
                    on = on & cond
                to = at.device((z + nz + way) % nz, at.y, x, k)
                j = next(j for j, p in enumerate(places) if p[0] == d + 1 and p[1] == -way)
                comm.step([], [(here, part(slot), sem_z[j], to)], on)
        comm.step(
            [],
            [
                (here, part(slot), sem_x[i], comm.to_x),
                (here, part(slot), sem_k[i], comm.to_k),
            ],
            cond,
        )
        if d == 0:
            moved = comm.move(here, part(slot))
        yield
    for i, (d, side, zi, cond) in enumerate(places):
        slot = slot_of(zi, 1 - x, k)
        comm.step(
            [(part(slot), sem_x[i])], [(part(slot), part(slot), sem_k[n + i], comm.to_k)], cond
        )
        yield
    for h, xh in enumerate((x, 1 - x)):
        for i, (d, side, zi, cond) in enumerate(places):
            comm.step([(part(slot_of(zi, xh, 1 - k)), sem_k[h * n + i])], [], cond)
    moved()


def add_rows(dst, terms):
    rows = dst.shape[0]
    step = math.gcd(rows, 16)

    def some_rows(i, _):
        r = pl.ds(pl.multiple_of(i * step, step), step)
        total = terms[0][r, :].astype(f32)
        for term in terms[1:]:
            total = total + term[r, :].astype(f32)
        dst[r, :] = total.astype(dst.dtype)
        return 0

    lax.fori_loop(0, rows // step, some_rows, 0)


def far_first(at):
    nz = at.nz
    orders = []
    for z in range(nz):
        others = sorted((c for c in range(nz) if c != z), key=lambda c: (-abs(c - z), c))
        orders.append([(abs(c - z), 1 if c > z else -1, c) for c in others] + [(0, 0, z)])
    here = [1 - ((at.z - c) * (at.z - c) + nz * nz - 1) // (nz * nz) for c in range(nz)]
    return [
        tuple(sum(here[c] * orders[c][t][i] for c in range(nz)) for i in range(3))
        for t in range(nz)
    ]


class Scatter:
    def __init__(self, comm, p_ref, bufs, total):
        nz = comm.at.nz
        self.comm, self.p_ref, self.bufs, self.total = comm, p_ref, bufs, total
        self.targets = far_first(comm.at)
        self.sem_k, self.sem_x = comm.sems(2 * nz), comm.sems(nz)
        self.sem_z = comm.used
        comm.sems(2 * nz)

    def mine(self, zi, flip, core):
        x = self.comm.at.x
        return self.p_ref.at[slot_of(zi, 1 - x if flip else x, core)]

    def passing(self, side, d):
        i = (side + 1) // 2 * self.comm.at.nz + d
        return self.bufs[2].at[i], self.comm.pool.at[self.sem_z + i]

    def first(self, t):
        comm, nz, k = self.comm, self.comm.at.nz, self.comm.at.k
        zi = self.targets[t][2]
        comm.step(
            [],
            [
                (self.mine(zi, flip, 1 - k), self.bufs[0].at[flip * nz + zi],
                 self.sem_k[flip * nz + t], comm.to_k)
                for flip in (1, 0)
            ],
        )

    def second(self, t):
        comm, nz, k = self.comm, self.comm.at.nz, self.comm.at.k
        zi = self.targets[t][2]
        b = self.bufs[0].at[nz + zi]
        comm.step(
            [(b, self.sem_k[nz + t])],
            [(b, self.bufs[1].at[zi], self.sem_x[t], comm.to_x)],
            None,
            lambda: add_rows(b, [b, self.mine(zi, 1, k)]),
        )

    def third(self, t):
        comm, at = self.comm, self.comm.at
        z, nz, k = at.z, at.nz, at.k
        d, side, zi = self.targets[t]
        b, landed = self.bufs[0].at[zi], self.bufs[1].at[zi]
        terms = [b, self.mine(zi, 0, k), landed]
        comm.arrive(b, self.sem_k[t])
        comm.arrive(landed, self.sem_x[t])
        if t == nz - 1:
            add_rows(self.total, terms)
            for way, on in ((1, z > 0), (-1, z < nz - 1)):
                buf, sem = self.passing(way, 0)

                @pl.when(on)
                def _():
                    comm.arrive(buf, sem)
                    add_rows(self.total, [self.total, buf])

            return
        add_rows(b, terms)
        buf, sem = self.passing(side, d)
        behind = z - side

        @pl.when((behind >= 0) & (behind < nz))
        def _():
            comm.arrive(buf, sem)
            add_rows(b, [b, buf])

        dst, sem = self.passing(side, d - 1)
        comm.step([], [(b, dst, sem, at.device(z + side, at.y, at.x, k))])

    def steps(self, produce=None):
        nz = self.comm.at.nz
        for i in range(nz + 2):
            if i < nz:
                if produce is not None:
                    produce(self.targets[i][2])
                self.first(i)
            yield
            for stage, lag in ((self.second, 1), (self.third, 2)):
                if 0 <= i - lag < nz:
                    stage(i - lag)
                    yield


def scatter_bufs(nz, rows, width):
    return [pltpu.VMEM((n * nz, rows, width), bf16) for n in (2, 1, 2)]


def along(ref, axis, i, size):
    r = pl.ds(pl.multiple_of(i * size, size), size)
    before = (slice(None),) * (len(ref.shape) - axis)
    return ref.at[before + (r,) + (slice(None),) * (axis - 1)]


class Swap:
    def __init__(self, array, unit_axis, feature_axis, units, depth, shape, plane=None, groups=1):
        self.array, self.shape, self.plane = array, shape, plane
        self.unit_axis, self.feature_axis, self.units, self.depth = unit_axis, feature_axis, units, depth
        self.groups = groups if feature_axis == 2 else 1
        self.out = jax.ShapeDtypeStruct(shape, bf16)

    def of_units(self, ref, z):
        if self.plane is not None:
            ref = ref.at[self.plane]
        return along(ref, self.unit_axis, z, self.units)

    def of_features(self, ref, z, y):
        return along(ref, self.feature_axis, 2 * z + y, self.depth)

    def runs(self, ref, nz, z, y):
        if self.groups == 1:
            return [self.of_features(ref, z, y)]
        r = self.depth // self.groups
        return [along(ref, 2, i * 2 * nz + 2 * z + y, r) for i in range(self.groups)]

    def cuts(self, piece):
        if self.groups == 1:
            return [piece]
        r = self.depth // self.groups
        return [along(piece, 2, i, r) for i in range(self.groups)]


def swap_in(comm, one, src, dst):
    at = comm.at
    z, y, x, k, nz = at.z, at.y, at.x, at.k, at.nz
    sem_z = [comm.sems(one.groups) for _ in range(nz)]
    sem_y = [comm.sems(one.groups) for _ in range(nz)]
    moved = []

    def sends():
        mine = one.runs(dst, nz, z, y)
        for d in range(1, nz):
            zi = (z + d) % nz
            parts = one.cuts(one.of_units(src, zi))
            for part, to, sem in zip(parts, mine, sem_z[d]):
                comm.step([], [(part, to, sem, at.device(zi, y, x, k))])
            yield
        for part, to, sem in zip(one.cuts(one.of_units(src, z)), mine, sem_y[0]):
            comm.step([], [(part, to, sem, comm.to_y)])
            moved.append(comm.move(part, to))
        yield

    def passes():
        for d in range(1, nz):
            for run, sem, on in zip(one.runs(dst, nz, (z + nz - d) % nz, y), sem_z[d], sem_y[d]):
                comm.step([(run, sem)], [(run, run, on, comm.to_y)])
            yield

    def arrivals():
        for d in range(nz):
            for run, sem in zip(one.runs(dst, nz, (z + nz - d) % nz, 1 - y), sem_y[d]):
                comm.arrive(run, sem)
        for wait in moved:
            wait()

    return sends(), passes(), arrivals


def add_piece(dst, src):
    if len(dst.shape) == 3:
        for p in range(dst.shape[0]):
            add_rows(dst.at[p], [dst.at[p], src.at[p]])
    else:
        add_rows(dst, [dst, src])


def swap_out_y(comm, one, src, landed):
    at = comm.at
    z, y, nz = at.z, at.y, at.nz
    order = list(range(1, nz)) + [0]
    sems = comm.sems(nz)

    def sends():
        for d in order:
            zi = (z + d) % nz
            comm.step([], [(one.of_features(src, zi, 1 - y), landed.at[zi], sems[d], comm.to_y)])
            yield

    def sums():
        for d in order:
            zi = (z + d) % nz
            comm.arrive(landed.at[zi], sems[d])
            add_piece(landed.at[zi], one.of_features(src, zi, y))
            yield

    return sends(), sums()


def swap_out_z(comm, one, summed, dst):
    at = comm.at
    z, y, x, k, nz = at.z, at.y, at.x, at.k, at.nz
    mine = one.of_units(dst, z)
    sems = comm.sems(nz)
    for d in list(range(1, nz)) + [0]:
        zi = (z + d) % nz
        if d:
            comm.step([], [(summed.at[zi], mine, sems[d], at.device(zi, y, x, k))])
            comm.late.append((one.of_units(dst, (z + nz - d) % nz), sems[d]))
        else:
            comm.keep(summed.at[zi], mine)
        yield


def paired(first, second):
    for _ in first:
        next(second, None)
        yield
    yield from second


def chain(*many):
    for steps in many:
        yield from steps


def landing(nz, one, user_shape):
    shape = list(user_shape)
    shape[len(shape) - one.feature_axis] = one.depth
    return pltpu.VMEM((nz, *shape), bf16)


def comm_kernel(nz, groups, work, swaps, extra, n_in, n_out, *refs):
    given = [one for one in swaps if one.array is not None]
    m, g = len(swaps), len(given)
    ins, srcs = refs[:n_in], refs[n_in : n_in + g]
    outs = refs[n_in + g : n_in + g + n_out]
    dsts = refs[n_in + g + n_out : n_in + g + n_out + m]
    scratch = refs[n_in + g + n_out + m :]
    comm = Comm(Place(nz), scratch[-1], groups)
    work(comm, (swaps + extra, srcs, dsts), ins, outs, scratch[:-1])
    comm.finish()


def comm_call(name, nz, collective, work, ins, outs, scratch, swaps, swap_spec=ANY, vmem=48, groups=1, extra=()):
    given = [one.array for one in swaps if one.array is not None]
    return pl.pallas_call(
        functools.partial(comm_kernel, nz, groups, work, swaps, list(extra), len(ins), len(outs)),
        out_shape=[jax.ShapeDtypeStruct(s, d) for s, d, _ in outs] + [one.out for one in swaps],
        in_specs=[s for _, s in ins] + [swap_spec] * len(given),
        out_specs=[s for _, _, s in outs] + [ANY] * len(swaps),
        scratch_shapes=scratch + [DMA((700,))],
        compiler_params=pltpu.CompilerParams(
            collective_id=collective, has_side_effects=True, vmem_limit_bytes=vmem * 2**20
        ),
        name=name,
    )(*[v for v, _ in ins], *given)


def by_rows(lo, size, do):
    step = math.gcd(size, 16)

    def some_rows(i, _):
        do(pl.ds(pl.multiple_of(lo + i * step, step), step))
        return 0

    lax.fori_loop(0, size // step, some_rows, 0)


def halves(rows):
    return [(0, rows // 2), (rows // 2, rows // 2)] if rows % 32 == 0 else [(0, rows)]


def feature_pieces(nz, groups, d_model):
    a = 2 * nz
    r = d_model // a // groups
    return [(c, i * r, (i * a + c) * r, r) for c in range(a) for i in range(groups)]


def sum_gains(comm, groups, sums, sorted_sums, landed, total):
    at = comm.at
    z, y, x, k, nz = at.z, at.y, at.x, at.k, at.nz
    for c, lo, col, r in feature_pieces(nz, groups, sums.shape[1]):
        sorted_sums[c % 2, c // 2, :, lo : lo + r] = sums[:, col : col + r]
    sem = comm.sems(4 + nz)
    comm.step([], [(sorted_sums.at[1 - y], landed.at[pl.ds(0, nz)], sem[0], comm.to_y)])
    comm.arrive(landed.at[pl.ds(0, nz)], sem[0])
    sorted_sums[y] += landed[0:nz]
    for d in range(1, nz):
        zi = (z + d) % nz
        comm.step([], [(sorted_sums.at[y, zi], landed.at[nz + d], sem[d], at.device(zi, y, x, k))])
    total[...] = sorted_sums[y, z]
    for d in range(1, nz):
        comm.arrive(landed.at[nz + d], sem[d])
        total[...] += landed[nz + d]
    landed[nz] = total[...]
    for i, to in enumerate((comm.to_k, comm.to_x, comm.to_xk)):
        comm.step([], [(landed.at[nz], landed.at[2 * nz + i], sem[nz + i], to)])
    for i in range(3):
        comm.arrive(landed.at[2 * nz + i], sem[nz + i])
        total[...] += landed[2 * nz + i]


def gains_of_group(comm, groups, gain_ref, landed, gains):
    at = comm.at
    z, y, x, k, nz = at.z, at.y, at.x, at.k, at.nz
    sem = comm.sems(nz + 1)
    for d in range(1, nz):
        to = at.device((z + d) % nz, y, x, k)
        comm.step([], [(gain_ref, landed.at[y, z], sem[d], to)])
    landed[y, z] = gain_ref[...]
    for d in range(1, nz):
        comm.arrive(landed.at[y, (z + nz - d) % nz], sem[d])
    comm.step([], [(landed.at[y], landed.at[y], sem[0], comm.to_y)])
    comm.arrive(landed.at[1 - y], sem[0])
    for c, lo, col, r in feature_pieces(nz, groups, gains.shape[1]):
        gains[:, col : col + r] = landed[c % 2, c // 2, :, lo : lo + r].astype(f32)


def product_into(p_ref, rows, at_slot, lhs, rhs, rhs_dims):
    n = p_ref.shape[2]
    wide = math.gcd(n, 512)
    count = lhs[0].shape[0] // rows
    for j in range(n // wide):
        cols = slice(j * wide, (j + 1) * wide)
        total = None
        for one, right, dims in zip(lhs, rhs, rhs_dims):
            block = right[:, cols] if dims == 0 else right[cols, :]
            term = lax.dot_general(one, block, (((1,), (dims,)), ((), ())), preferred_element_type=f32)
            total = term if total is None else total + term
        p_ref[pl.ds(at_slot, count), :, cols] = total.astype(bf16).reshape(count, rows, wide)


def row_blocks(rows, keys, do):
    step = math.gcd(rows, 128)
    fine = max(16, min(128, 128 * 2048 // keys))
    for i in range(rows // step):

        def some(j, _):
            do(pl.ds(pl.multiple_of(i * step + j * fine, fine), fine))
            return 0

        lax.fori_loop(0, step // fine, some, 0)
        yield


def attend(heads, q_ref, k_ref, v_ref, at_q, at_k, o_ref, lse_ref):
    def block(r):
        visible = at_k[...] <= at_q[r, :]
        for h in range(heads):
            c = slice(h * HD, (h + 1) * HD)
            scores = lax.dot_general(
                q_ref[r, c], k_ref[:, c], (((1,), (1,)), ((), ())), preferred_element_type=f32
            )
            scores = jnp.where(visible, scores, -1e30)
            peak = jnp.max(scores, axis=-1, keepdims=True)
            weights = jnp.exp(scores - peak)
            total = jnp.sum(weights, axis=-1, keepdims=True)
            probs = (weights * (1.0 / total)).astype(bf16)
            o_ref[r, c] = jnp.dot(probs, v_ref[:, c], preferred_element_type=f32).astype(bf16)
            lse_ref[r, h : h + 1] = peak + jnp.log(total)

    yield from row_blocks(q_ref.shape[0], k_ref.shape[0], block)


def attend_back(heads, q_ref, k_ref, v_ref, at_q, at_k, o_ref, lse_ref, do_ref, dq_ref, dk_ref, dv_ref):
    over_rows = (((0,), (0,)), ((), ()))
    over_cols = (((1,), (1,)), ((), ()))
    dk_ref[...] = jnp.zeros_like(dk_ref)
    dv_ref[...] = jnp.zeros_like(dv_ref)

    def block(r):
        visible = at_k[...] <= at_q[r, :]
        for h in range(heads):
            c = slice(h * HD, (h + 1) * HD)
            q, grad = q_ref[r, c], do_ref[r, c]
            scores = lax.dot_general(q, k_ref[:, c], over_cols, preferred_element_type=f32)
            scores = jnp.where(visible, scores, -1e30)
            probs = jnp.exp(scores - lse_ref[r, h : h + 1])
            delta = jnp.sum(
                grad.astype(f32) * o_ref[r, c].astype(f32), axis=-1, keepdims=True
            )
            prob_grad = lax.dot_general(grad, v_ref[:, c], over_cols, preferred_element_type=f32)
            score_grad = (probs * (prob_grad - delta)).astype(bf16)
            dq_ref[r, c] = jnp.dot(score_grad, k_ref[:, c], preferred_element_type=f32) * HD ** (-0.5)
            dk_ref[c, :] += lax.dot_general(q, score_grad, over_rows, preferred_element_type=f32)
            dv_ref[c, :] += lax.dot_general(
                grad, probs.astype(bf16), over_rows, preferred_element_type=f32
            )

    yield from row_blocks(q_ref.shape[0], k_ref.shape[0], block)


def forward_work(heads, groups, comm, swap, ins, outs, scratch):
    x_ref, gain_ref, cos, sin, at_q, at_k = ins
    gains, q_ref, o_ref, lse_ref, hidden, rows_attn, k_out, v_out, rows_mlp = outs
    normed, landed, rows_v, qkv_v, out_v, k_all, v_all, p_ref = scratch[:8]
    bufs = scratch[8:]
    swaps, srcs, dsts = swap
    at = comm.at
    y, nz = at.y, at.nz
    rows, d_model = x_ref.shape
    tall = 4 * rows
    keys = q_ref.shape[0]
    width = q_ref.shape[1]

    places = (qkv_v, out_v) + tuple(dsts[2:])
    qkv, out, down, gate, up = [swap_in(comm, *v) for v in zip(swaps, srcs, places)]
    exhaust(qkv[0])
    gains_of_group(comm, groups, gain_ref, landed, gains)

    def norm_1(r):
        x = x_ref[r, :].astype(f32)
        normed[r, :] = (x * inv_rms(x) * gains[0:1, :]).astype(bf16)

    by_rows(0, rows, norm_1)
    shards = gather_steps(comm, normed, rows_v, 0, rows)
    advance(shards, z_steps(at))
    take_turns(shards, chain(out[0], qkv[1]))
    exhaust(down[0])
    qkv[2]()
    comm.keep(qkv_v, dsts[0])
    comm.keep(rows_v, rows_attn)

    def half(ref, g, yy):
        return ref.at[pl.ds(pl.multiple_of((yy * groups + g) * keys, keys), keys), :]

    group = at.first // (2 * nz)
    mine = [half(ref, group, y) for ref in (k_all, v_all)]
    low = lax.broadcasted_iota(jnp.int32, (1, width), 1) % HD < HD // 2

    def project(i, _):
        r = pl.ds(pl.multiple_of(i * tall, tall), tall)
        block = rows_v[r, :]

        def turned(p):
            u = jnp.dot(block, qkv_v[p], preferred_element_type=f32)
            other = jnp.where(
                low, pltpu.roll(u, width - HD // 2, 1), pltpu.roll(u, HD // 2, 1)
            )
            return (u * cos[r, :] + other * sin[r, :]).astype(bf16)

        q_ref[r, :] = turned(0) * jnp.asarray(HD ** (-0.5), bf16)
        mine[0][r, :] = turned(1)
        mine[1][r, :] = jnp.dot(block, qkv_v[2], preferred_element_type=f32).astype(bf16)
        return 0

    lax.fori_loop(0, nz, project, 0)
    sem = comm.sems(4 * groups)
    for i, ref in enumerate(mine):
        comm.step([], [(ref, ref, sem[i], comm.to_y)])
        for g, f, device in comm.afar:
            comm.step([], [(ref, ref, sem[2 + (2 * g + f) * 2 + i - 2], device)])
    exhaust(gate[0])
    exhaust(out[1])
    out[2]()
    comm.keep(out_v, dsts[1])
    for i, (ref, dst) in enumerate(((k_all, k_out), (v_all, v_out))):
        comm.arrive(half(ref, group, 1 - y), sem[i])
        for g, f, device in comm.afar:
            come = half(ref, (group + groups - g) % groups, y + f * (1 - 2 * y))
            comm.arrive(come, sem[2 + (2 * g + f) * 2 + i - 2])
        comm.keep(ref, dst)
    take_turns(
        attend(heads, q_ref, k_all, v_all, at_q, at_k, o_ref, lse_ref), chain(down[1], gate[1])
    )

    def norm_2(r):
        h = hidden[r, :] + x_ref[r, :].astype(f32)
        hidden[r, :] = h
        normed_2[r, :] = (h * inv_rms(h) * gains[1:2, :]).astype(bf16)

    def produce(zi):
        r = pl.ds(pl.multiple_of(zi * tall, tall), tall)
        product_into(p_ref, rows, zi * 4, [o_ref[r, :]], [out_v], [0])

    normed_2, total = bufs[3], bufs[4]
    steps = Scatter(comm, p_ref, bufs[:3], total).steps(produce)
    advance(up[0], 1)
    exhaust(steps)
    for c, lo, col, r in feature_pieces(nz, groups, d_model) if groups > 1 else [(0, 0, 0, d_model)]:
        frm = c * (d_model // (2 * nz)) + lo
        hidden[:, col : col + r] = total[:, frm : frm + r]
    by_rows(0, rows, norm_2)
    shards = gather_steps(comm, normed_2, rows_mlp, 0, rows)
    advance(shards, z_steps(at))
    take_turns(shards, up[0])
    exhaust(up[1])
    for one in (down, gate, up):
        one[2]()


def attend_back_work(heads, comm, swap, ins, outs, scratch):
    q_ref, k_ref, v_ref, at_q, at_k, o_ref, lse_ref, do_ref, gate_sum, up_grad = ins
    dq_ref, dk_out, dv_out = outs
    dk_ref, dv_ref, going, come, up_landed = scratch
    (gate, up), _, dsts = swap
    at = comm.at
    y, keys = at.y, k_ref.shape[0] // 2

    def half(ref, yy):
        return ref.at[:, pl.ds(pl.multiple_of(yy * keys, keys), keys)]

    sends, sums = swap_out_y(comm, up, up_grad, up_landed)
    exhaust(sends)
    exhaust(swap_out_z(comm, gate, gate_sum, dsts[0]))
    compute = attend_back(
        heads, q_ref, k_ref, v_ref, at_q, at_k, o_ref, lse_ref, do_ref, dq_ref, dk_ref, dv_ref
    )
    take_turns(compute, paired(sums, swap_out_z(comm, up, up_landed, dsts[1])))
    sem = comm.sems(2)
    for i, ref in enumerate((dk_ref, dv_ref)):
        going[i] = half(ref, 1 - y)[...].astype(bf16)
        comm.step([], [(going.at[i], come.at[i], sem[i], comm.to_y)])
    for i, (ref, dst) in enumerate(((dk_ref, dk_out), (dv_ref, dv_out))):
        comm.arrive(come.at[i], sem[i])
        dst[...] = half(ref, y)[...] + come[i].astype(f32)


def norm_back(grad, unit, rms, gain):
    unit_grad = grad * gain
    return rms * (unit_grad - unit * jnp.mean(unit_grad * unit, axis=-1, keepdims=True))


def back_work(groups, comm, swap, ins, outs, scratch):
    rows_mlp, gate_w, up_w, dn_w, hidden, dy_ref, gains = ins
    residual, branch_rows, gain_sum, block_out, gate_out, up_out = outs
    total, rounded, p_ref, q_ref, pre, gates, n2, dy, gate_g, up_g, dn_g, dn_landed, gate_landed = scratch[:13]
    bufs, bufs_q = scratch[13:16], scratch[16:19]
    (down, gate_swap), _, dsts = swap
    at = comm.at
    nz = at.nz
    rows = hidden.shape[0]
    tall = 4 * rows
    gain_sum[...] = jnp.zeros_like(gain_sum)
    sems = comm.sems(nz)

    def load(t, zi):
        r = pl.ds(pl.multiple_of(zi * tall, tall), tall)
        return pltpu.make_async_copy(rows_mlp.at[r, :], n2.at[r, :], sems[t])

    main = Scatter(comm, p_ref, bufs, total)
    for t in range(nz):
        load(t, main.targets[t][2]).start()
    turn = iter(range(nz))

    def forward(zi):
        load(next(turn), zi).wait()
        r = pl.ds(pl.multiple_of(zi * tall, tall), tall)
        x = n2[r, :]
        gate = jnp.dot(x, gate_w[...], preferred_element_type=f32)
        up = jnp.dot(x, up_w[...], preferred_element_type=f32)
        pre[0, r, :] = gate
        pre[1, r, :] = up
        hid = (gate * jax.nn.sigmoid(gate) * up).astype(bf16)
        gates[2, r, :] = hid
        product_into(q_ref, rows, zi * 4, [hid], [dn_w], [0])

    def backward(zi):
        r = pl.ds(pl.multiple_of(zi * tall, tall), tall)
        grad = lax.dot_general(
            dy[r, :], dn_w[...], (((1,), (1,)), ((), ())), preferred_element_type=f32
        )
        gate, up = pre[0, r, :], pre[1, r, :]
        sig = jax.nn.sigmoid(gate)
        gate_grad = (grad * up * (sig * (1.0 + gate * (1.0 - sig)))).astype(bf16)
        up_grad = (grad * (gate * sig)).astype(bf16)
        gates[0, r, :] = gate_grad
        gates[1, r, :] = up_grad
        product_into(p_ref, rows, zi * 4, [gate_grad, up_grad], [gate_w, up_w], [1, 1])

    def back(r):
        h = hidden[r, :]
        rms = inv_rms(h)
        unit, grad = h * rms, total[r, :]
        gain_sum[...] += jnp.sum(grad * unit, axis=0, keepdims=True)
        dh = dy_ref[r, :].astype(f32) + norm_back(grad, unit, rms, gains[1:2, :])
        residual[r, :] = dh
        rounded[r, :] = dh.astype(bf16)

    def out(r):
        block_out[r, :] = (hidden[r, :] + residual[r, :]).astype(bf16)

    def gradients(which):
        d_model = n2.shape[1]
        depth = d_model // (2 * nz)
        over_rows = (((0,), (0,)), ((), ()))
        pieces = feature_pieces(nz, groups, d_model)
        per = max(1, len(pieces) // 4)
        for j in range(0, len(pieces), per):
            for c, lo, col, r in pieces[j : j + per]:
                f, to = slice(col, col + r), slice(c * depth + lo, c * depth + lo + r)
                if which == 2:
                    dn_g[:, to] = lax.dot_general(
                        gates[2], dy[:, f], over_rows, preferred_element_type=f32
                    ).astype(bf16)
                else:
                    (gate_g, up_g)[which][to, :] = lax.dot_general(
                        n2[:, f], gates[which], over_rows, preferred_element_type=f32
                    ).astype(bf16)
            yield

    shards = gather_steps(comm, dy_ref, dy, 0, rows)
    side = Scatter(comm, q_ref, bufs_q, residual).steps(forward)
    advance(shards, 1)
    for _ in range(3 * nz - 3):
        next(side)
        advance(shards, 1)
    take_turns(shards, side)
    by_rows(0, rows, out)
    steps = main.steps(backward)
    down_sends, down_sums = swap_out_y(comm, down, dn_g, dn_landed)
    gate_sends, gate_sums = swap_out_y(comm, gate_swap, gate_g, gate_landed)
    advance(steps, 3 * nz - 3)
    take_turns(
        steps,
        chain(gradients(2), down_sends, gradients(0), gate_sends, gradients(1)),
    )
    comm.keep(up_g, up_out)
    by_rows(0, rows, back)
    shards = gather_steps(comm, rounded, branch_rows, 0, rows)
    advance(shards, z_steps(at))
    take_turns(shards, paired(down_sums, swap_out_z(comm, down, dn_landed, dsts[0])))
    exhaust(gate_sums)
    comm.keep(gate_landed, gate_out)


def last_work(groups, comm, swap, ins, outs, scratch):
    proj_grads, qkv_w, residual, x_ref, gains, gain_sum_2 = ins
    grad_in, gain_out = outs
    total, gain_sums, sorted_sums, landed, qkv_landed, out_landed, p_ref = scratch[:7]
    bufs = scratch[7:]
    rows = x_ref.shape[0]
    gain_sums[0:1, :] = jnp.zeros_like(gain_sum_2)
    gain_sums[1:2, :] = gain_sum_2[...]

    def back(r):
        x = x_ref[r, :].astype(f32)
        rms = inv_rms(x)
        unit, grad = x * rms, total[r, :]
        gain_sums[0:1, :] += jnp.sum(grad * unit, axis=0, keepdims=True)
        grad_in[r, :] = residual[r, :] + norm_back(grad, unit, rms, gains[0:1, :])

    width = qkv_w.shape[2]

    def produce(zi):
        r = pl.ds(pl.multiple_of(zi * 4 * rows, 4 * rows), 4 * rows)
        lhs = [proj_grads[r, p * width : (p + 1) * width] for p in range(3)]
        product_into(p_ref, rows, zi * 4, lhs, [qkv_w.at[p] for p in range(3)], [1] * 3)

    (qkv, out), srcs, dsts = swap
    qkv_sends, qkv_sums = swap_out_y(comm, qkv, srcs[0], qkv_landed)
    out_sends, out_sums = swap_out_y(comm, out, srcs[1], out_landed)
    exhaust(out_sends, qkv_sends)
    take_turns(
        Scatter(comm, p_ref, bufs, total).steps(produce),
        chain(
            paired(out_sums, swap_out_z(comm, out, out_landed, dsts[1])),
            paired(qkv_sums, swap_out_z(comm, qkv, qkv_landed, dsts[0])),
        ),
    )
    by_rows(0, rows, back)
    sum_gains(comm, groups, gain_sums, sorted_sums, landed, gain_out)


def body(
    block_input,
    qkv_weight,
    out_weight,
    gate_up_weight,
    down_weight,
    norm_gains,
    positions,
    layer_output_gradient,
):
    n_ctx, n_tp = lax.axis_size("ctx"), lax.axis_size("tp")
    nz = math.gcd(qkv_weight.shape[2] // HD, n_ctx // 2)
    nz = math.gcd(nz, 4)
    a = 2 * nz
    b = n_ctx // a
    assert n_tp == 4
    depth = qkv_weight.shape[1] * b
    d_model = depth * a
    width = qkv_weight.shape[2] // nz
    heads = width // HD
    units = down_weight.shape[0] // nz
    rows = block_input.shape[0]
    across = [[i * a + j for i in range(b)] for j in range(a)]

    def over_groups(v, axis):
        return lax.all_gather(v, "ctx", axis=axis, tiled=True, axis_index_groups=across) if b > 1 else v

    def to_groups(v, axis):
        if b == 1:
            return v
        return lax.psum_scatter(
            v, "ctx", scatter_dimension=axis, tiled=True, axis_index_groups=across
        )

    def model_order(v, axis):
        if b == 1:
            return v
        s = v.shape
        w = v.reshape(s[:axis] + (a, b, depth // b) + s[axis + 1 :])
        return jnp.swapaxes(w, axis, axis + 1).reshape(s)

    def swap_order(v, axis):
        if b == 1:
            return v
        s = v.shape
        w = v.reshape(s[:axis] + (b, a, depth // b) + s[axis + 1 :])
        return jnp.swapaxes(w, axis, axis + 1).reshape(s)

    my_gains = over_groups(norm_gains, 1)
    group_rows = 4 * nz * rows
    n_keys = 2 * b * group_rows
    y, group = lax.axis_index("ctx") % 2, lax.axis_index("ctx") // a
    by_place = positions.reshape(b, nz, 2, n_tp * rows)
    key_pos = by_place.transpose(2, 0, 1, 3).reshape(2 * b, group_rows)
    own_pos = lax.dynamic_index_in_dim(key_pos, y * b + group, 0, keepdims=False)
    cos_tab, sin_tab = rope_tables(own_pos, HD)
    cos_wide = jnp.tile(cos_tab[:, 0, :], (1, 2 * heads))
    sin_wide = jnp.tile(jnp.concatenate([-sin_tab, sin_tab], axis=-1)[:, 0, :], (1, heads))
    places = [(own_pos[:, None], VMEM), (key_pos.reshape(1, -1), VMEM)]
    gu_all = over_groups(gate_up_weight, 1)
    partials = pltpu.VMEM((4 * nz, rows, d_model), bf16)
    (gains, query_bf, attn_bf, log_total, hidden, rows_attn, key_all, value_all, rows_mlp,
     qkv_w, out_w, dn_w, gate_w, up_w) = comm_call(
        "forward", nz, 0, functools.partial(forward_work, heads, b),
        [(block_input, VMEM), (my_gains, VMEM), (cos_wide, VMEM), (sin_wide, VMEM)] + places,
        [((2, d_model), f32, VMEM), ((group_rows, width), bf16, VMEM),
         ((group_rows, width), bf16, VMEM), ((group_rows, heads), f32, VMEM),
         ((rows, d_model), f32, VMEM), ((group_rows, d_model), bf16, ANY),
         ((n_keys, width), bf16, ANY), ((n_keys, width), bf16, ANY),
         ((group_rows, d_model), bf16, ANY)],
        [pltpu.VMEM((rows, d_model), bf16), pltpu.VMEM((2, nz) + my_gains.shape, bf16),
         pltpu.VMEM((group_rows, d_model), bf16), pltpu.VMEM((3, d_model, width), bf16),
         pltpu.VMEM((width, d_model), bf16), pltpu.VMEM((n_keys, width), bf16),
         pltpu.VMEM((n_keys, width), bf16), partials]
        + scatter_bufs(nz, rows, d_model)
        + [pltpu.VMEM((rows, d_model), bf16), pltpu.VMEM((rows, d_model), f32)],
        [Swap(over_groups(qkv_weight, 1), 1, 2, width, depth, (3, d_model, width), None, b),
         Swap(over_groups(out_weight, 1), 2, 1, width, depth, (width, d_model)),
         Swap(over_groups(down_weight, 1), 2, 1, units, depth, (units, d_model))]
        + [Swap(gu_all, 1, 2, units, depth, (d_model, units), p, b) for p in (0, 1)],
        groups=b,
    )
    out_w, dn_w = model_order(out_w, 1), model_order(dn_w, 1)
    down_swap = Swap(None, 2, 1, units, depth, (nz * units, depth))
    half_swap = Swap(None, 1, 2, units, depth, (depth, nz * units))
    residual_grad, branch_rows, gain_sum_2, block_output, gate_sum, up_grad, dn_back = comm_call(
        "back", nz, 3, functools.partial(back_work, b),
        [(rows_mlp, ANY), (gate_w, VMEM), (up_w, VMEM), (dn_w, VMEM),
         (hidden, VMEM), (layer_output_gradient, VMEM), (gains, VMEM)],
        [((rows, d_model), f32, VMEM), ((group_rows, d_model), bf16, ANY),
         ((1, d_model), f32, VMEM), ((rows, d_model), bf16, VMEM),
         ((nz, depth, units), bf16, ANY), ((d_model, units), bf16, ANY)],
        [pltpu.VMEM((rows, d_model), f32), pltpu.VMEM((rows, d_model), bf16), partials, partials,
         pltpu.VMEM((2, group_rows, units), f32), pltpu.VMEM((3, group_rows, units), bf16),
         pltpu.VMEM((group_rows, d_model), bf16), pltpu.VMEM((group_rows, d_model), bf16),
         pltpu.VMEM((d_model, units), bf16), pltpu.VMEM((d_model, units), bf16),
         pltpu.VMEM((units, d_model), bf16),
         landing(nz, down_swap, (units, d_model)), landing(nz, half_swap, (d_model, units))]
        + scatter_bufs(nz, rows, d_model) + scatter_bufs(nz, rows, d_model),
        [down_swap],
        vmem=60,
        extra=[half_swap],
    )
    out_weight_grad = jnp.einsum("te,td->ed", attn_bf, branch_rows, preferred_element_type=f32)
    attn_grad_bf = jnp.einsum("td,ed->te", branch_rows, out_w, preferred_element_type=f32).astype(bf16)
    query_grad, key_terms, value_terms, gate_back, up_back = comm_call(
        "attend_back", nz, 4, functools.partial(attend_back_work, heads),
        [(query_bf, VMEM), (key_all, VMEM), (value_all, VMEM)] + places
        + [(attn_bf, VMEM), (log_total, VMEM), (attn_grad_bf, VMEM), (gate_sum, VMEM),
           (up_grad, VMEM)],
        [((group_rows, width), f32, VMEM), ((width, n_keys // 2), f32, VMEM),
         ((width, n_keys // 2), f32, VMEM)],
        [pltpu.VMEM((width, n_keys), f32), pltpu.VMEM((width, n_keys), f32),
         pltpu.VMEM((2, width, n_keys // 2), bf16), pltpu.VMEM((2, width, n_keys // 2), bf16),
         landing(nz, half_swap, (d_model, units))],
        [half_swap, half_swap],
    )
    gu_back = jnp.stack([gate_back, up_back])
    key_grad, value_grad = key_terms.T, value_terms.T
    if b > 1:
        key_grad = to_groups(key_grad.astype(bf16), 0).astype(f32)
        value_grad = to_groups(value_grad.astype(bf16), 0).astype(f32)
    query_raw = unrotate(query_grad, cos_tab, sin_tab, heads, HD).astype(bf16)
    key_raw = unrotate(key_grad, cos_tab, sin_tab, heads, HD).astype(bf16)
    value_raw = value_grad.astype(bf16)
    proj_grads = jnp.concatenate([query_raw, key_raw, value_raw], axis=1)
    qkv_grad = jnp.einsum(
        "td,kte->kde", rows_attn, jnp.stack([query_raw, key_raw, value_raw]),
        preferred_element_type=f32,
    )
    qkv_swap = Swap(
        swap_order(qkv_grad.astype(bf16), 1), 1, 2, width, depth, (3, depth, nz * width)
    )
    out_swap = Swap(
        swap_order(out_weight_grad.astype(bf16), 1), 2, 1, width, depth, (nz * width, depth)
    )
    layer_input_gradient, gain_sums, qkv_back, out_back = comm_call(
        "last", nz, 5, functools.partial(last_work, b),
        [(proj_grads, VMEM), (qkv_w, VMEM), (residual_grad, VMEM), (block_input, VMEM),
         (gains, VMEM), (gain_sum_2, VMEM)],
        [((rows, d_model), f32, VMEM), ((2, depth), f32, VMEM)],
        [pltpu.VMEM((rows, d_model), f32), pltpu.VMEM((2, d_model), f32),
         pltpu.VMEM((2, nz, 2, depth), f32), pltpu.VMEM((2 * nz + 3, 2, depth), f32),
         landing(nz, qkv_swap, (3, d_model, width)), landing(nz, out_swap, (width, d_model)),
         partials] + scatter_bufs(nz, rows, d_model),
        [qkv_swap, out_swap],
        swap_spec=VMEM,
    )
    if b > 1:
        gain_sums = lax.psum(gain_sums, "ctx", axis_index_groups=across)
    gain_cols = d_model // (n_ctx * n_tp)
    gain_part = lax.dynamic_slice_in_dim(
        gain_sums, (group * n_tp + lax.axis_index("tp")) * gain_cols, gain_cols, 1
    )
    return (
        block_output,
        layer_input_gradient,
        to_groups(qkv_back, 1).astype(f32),
        to_groups(out_back, 1).astype(f32),
        to_groups(gu_back, 1).astype(f32),
        to_groups(dn_back, 1).astype(f32),
        gain_part,
    )


def solution(mesh):
    placed = (
        P(("ctx", "tp"), None),
        P(None, "ctx", "tp"),
        P("tp", "ctx"),
        P(None, "ctx", "tp"),
        P("tp", "ctx"),
        P(None, "ctx"),
        P(),
        P(("ctx", "tp"), None),
    )
    return jax.shard_map(
        body,
        mesh=mesh,
        in_specs=placed,
        out_specs=(
            P(("ctx", "tp"), None),
            P(("ctx", "tp"), None),
            P(None, "ctx", "tp"),
            P("tp", "ctx"),
            P(None, "ctx", "tp"),
            P("tp", "ctx"),
            P(None, ("ctx", "tp")),
        ),
        check_vma=False,
    )
```

```python
import functools
import math

import jax
import jax.numpy as jnp
from jax import lax
from jax.experimental import pallas as pl
from jax.experimental.pallas import tpu as pltpu
from jax.sharding import PartitionSpec as P

HD = 64
MESH = pl.DeviceIdType.MESH
DMA = pltpu.SemaphoreType.DMA
ANY = pl.BlockSpec(memory_space=pl.ANY)
VMEM = pl.BlockSpec(memory_space=pltpu.VMEM)
bf16 = jnp.bfloat16
f32 = jnp.float32

norm_eps = 1e-05
rope_base = 130000.0


def inv_rms(values):
    return lax.rsqrt(jnp.mean(values * values, axis=-1, keepdims=True) + norm_eps)


def rope_tables(where_at, head_dim):
    half_dim = head_dim // 2
    inv_freq = rope_base ** (-(jnp.arange(half_dim, dtype=f32) * 2.0 / head_dim))
    angles = where_at.astype(f32)[:, None] * inv_freq[None, :]
    return (jnp.cos(angles)[:, None, :], jnp.sin(angles)[:, None, :])


def rotate(values, cos_tab, sin_tab, n_heads, head_dim):
    shaped = values.reshape(values.shape[0], n_heads, head_dim)
    half_dim = head_dim // 2
    lower_half, upper_half = (shaped[..., :half_dim], shaped[..., half_dim:])
    turned = jnp.concatenate(
        [lower_half * cos_tab - upper_half * sin_tab, upper_half * cos_tab + lower_half * sin_tab],
        axis=-1,
    )
    return turned.reshape(values.shape[0], n_heads * head_dim)


def unrotate(values, cos_tab, sin_tab, n_heads, head_dim):
    return rotate(values, cos_tab, -sin_tab, n_heads, head_dim)


class Place:
    def __init__(self, nz):
        ctx, tp = lax.axis_index("ctx"), lax.axis_index("tp")
        self.nz = nz
        self.first = ctx // (2 * nz) * (2 * nz)
        self.z, self.y = (ctx - self.first) // 2, (ctx - self.first) % 2
        self.x, self.k = tp // 2, tp % 2

    def device(self, z, y, x, k):
        return {"ctx": self.first + 2 * z + y, "tp": 2 * x + k}

    def elsewhere(self, g, flip):
        n = lax.axis_size("ctx")
        y = self.y + flip * (1 - 2 * self.y)
        return {"ctx": (self.first + g * 2 * self.nz) % n + 2 * self.z + y}


def slot_of(z, x, k):
    return (z * 2 + x) * 2 + k


class Comm:
    def __init__(self, at, pool, groups=1):
        self.at, self.pool, self.used, self.ends, self.late = at, pool, 0, [], []
        z, y, x, k, nz = at.z, at.y, at.x, at.k, at.nz
        self.to_x = at.device(z, y, 1 - x, k)
        self.to_k = at.device(z, y, x, 1 - k)
        self.to_y = at.device(z, 1 - y, x, k)
        self.to_xk = at.device(z, y, 1 - x, 1 - k)
        peers = [self.to_x, self.to_k, self.to_y, self.to_xk]
        self.afar = [(g, f, at.elsewhere(g, f)) for g in range(1, groups) for f in (0, 1)]
        peers += [device for _, _, device in self.afar]
        peers += [at.device((z + d) % nz, y, x, k) for d in range(1, nz)]
        barrier = pltpu.get_barrier_semaphore()
        for peer in peers:
            pl.semaphore_signal(barrier, inc=1, device_id=peer, device_id_type=MESH)
        pl.semaphore_wait(barrier, len(peers))

    def sem(self):
        self.used += 1
        return self.pool.at[self.used - 1]

    def sems(self, n):
        return [self.sem() for _ in range(n)]

    def step(self, arrivals, copies, cond=None, then=None):
        sems = self.sems(len(copies))

        def copy(i):
            src, dst, recv_sem, device = copies[i]
            return pltpu.make_async_remote_copy(
                src_ref=src,
                dst_ref=dst,
                send_sem=sems[i],
                recv_sem=recv_sem,
                device_id=device,
                device_id_type=MESH,
            )

        def go():
            for buf, sem in arrivals:
                self.arrive(buf, sem)
            if then is not None:
                then()
            for i in range(len(copies)):
                copy(i).start()

        def end():
            for i in range(len(copies)):
                copy(i).wait_send()

        if cond is None:
            go()
        else:
            pl.when(cond)(go)
        if copies:
            self.ends.append((cond, end))

    def move(self, src, dst):
        copy = pltpu.make_async_copy(src, dst, self.sem())
        copy.start()
        return copy.wait

    def keep(self, src, dst):
        self.ends.append((None, self.move(src, dst)))

    def arrive(self, buf, recv_sem):
        pltpu.make_async_remote_copy(
            src_ref=buf,
            dst_ref=buf,
            send_sem=recv_sem,
            recv_sem=recv_sem,
            device_id=self.to_k,
            device_id_type=MESH,
        ).wait_recv()

    def finish(self):
        for buf, sem in self.late:
            self.arrive(buf, sem)
        for cond, end in self.ends:
            if cond is None:
                end()
            else:
                pl.when(cond)(end)


def take_turns(*steps):
    steps = list(steps)
    while steps:
        for one in list(steps):
            if next(one, steps) is steps:
                steps.remove(one)


def advance(steps, n):
    for _ in range(n):
        next(steps, None)


def exhaust(*many):
    for steps in many:
        for _ in steps:
            pass


def line(at):
    places = []
    for d in range(1, at.nz):
        places.append((d, -1, (at.z + at.nz - d) % at.nz, at.z >= d))
        places.append((d, 1, (at.z + d) % at.nz, at.z + d < at.nz))
    return places


def z_steps(at):
    return 2 * at.nz - 1


def gather_steps(comm, own, o_ref, lo, size):
    at = comm.at
    z, x, k, nz = at.z, at.x, at.k, at.nz
    rows = own.shape[0]
    places = [(0, 0, z, None)] + line(at)
    n = len(places)
    sem_z, sem_x, sem_k = (comm.sems(m * n) for m in (1, 1, 2))

    def part(slot):
        return o_ref.at[pl.ds(pl.multiple_of(slot * rows + lo, size), size), :]

    for i, (d, side, zi, cond) in enumerate(places):
        slot = slot_of(zi, x, k)
        here = own.at[pl.ds(lo, size), :] if d == 0 else part(slot)
        if d:
            comm.step([(part(slot), sem_z[i])], [], cond)
        for way in (1, -1):
            if d < nz - 1 and side != way:
                on = (z < nz - 1) if way == 1 else (z > 0)
                if cond is not None:
                    on = on & cond
                to = at.device((z + nz + way) % nz, at.y, x, k)
                j = next(j for j, p in enumerate(places) if p[0] == d + 1 and p[1] == -way)
                comm.step([], [(here, part(slot), sem_z[j], to)], on)
        comm.step(
            [],
            [
                (here, part(slot), sem_x[i], comm.to_x),
                (here, part(slot), sem_k[i], comm.to_k),
            ],
            cond,
        )
        if d == 0:
            moved = comm.move(here, part(slot))
        yield
    for i, (d, side, zi, cond) in enumerate(places):
        slot = slot_of(zi, 1 - x, k)
        comm.step(
            [(part(slot), sem_x[i])], [(part(slot), part(slot), sem_k[n + i], comm.to_k)], cond
        )
        yield
    for h, xh in enumerate((x, 1 - x)):
        for i, (d, side, zi, cond) in enumerate(places):
            comm.step([(part(slot_of(zi, xh, 1 - k)), sem_k[h * n + i])], [], cond)
    moved()


def add_rows(dst, terms):
    rows = dst.shape[0]
    step = math.gcd(rows, 16)

    def some_rows(i, _):
        r = pl.ds(pl.multiple_of(i * step, step), step)
        total = terms[0][r, :].astype(f32)
        for term in terms[1:]:
            total = total + term[r, :].astype(f32)
        dst[r, :] = total.astype(dst.dtype)
        return 0

    lax.fori_loop(0, rows // step, some_rows, 0)


def far_first(at):
    nz = at.nz
    orders = []
    for z in range(nz):
        others = sorted((c for c in range(nz) if c != z), key=lambda c: (-abs(c - z), c))
        orders.append([(abs(c - z), 1 if c > z else -1, c) for c in others] + [(0, 0, z)])
    here = [1 - ((at.z - c) * (at.z - c) + nz * nz - 1) // (nz * nz) for c in range(nz)]
    return [
        tuple(sum(here[c] * orders[c][t][i] for c in range(nz)) for i in range(3))
        for t in range(nz)
    ]


class Scatter:
    def __init__(self, comm, p_ref, bufs, total, lo, size):
        nz = comm.at.nz
        self.comm, self.p_ref, self.bufs = comm, p_ref, bufs
        self.range = pl.ds(lo, size)
        self.total = total.at[self.range, :]
        self.targets = far_first(comm.at)
        self.sem_k, self.sem_x = comm.sems(2 * nz), comm.sems(nz)
        self.sem_z = comm.used
        comm.sems(2 * nz)

    def buf(self, b, j):
        return self.bufs[b].at[j, self.range, :]

    def mine(self, zi, flip, core):
        x = self.comm.at.x
        return self.p_ref.at[slot_of(zi, 1 - x if flip else x, core), self.range, :]

    def passing(self, side, d):
        i = (side + 1) // 2 * self.comm.at.nz + d
        return self.buf(2, i), self.comm.pool.at[self.sem_z + i]

    def first(self, t):
        comm, nz, k = self.comm, self.comm.at.nz, self.comm.at.k
        zi = self.targets[t][2]
        comm.step(
            [],
            [
                (self.mine(zi, flip, 1 - k), self.buf(0, flip * nz + zi),
                 self.sem_k[flip * nz + t], comm.to_k)
                for flip in (1, 0)
            ],
        )

    def second(self, t):
        comm, nz, k = self.comm, self.comm.at.nz, self.comm.at.k
        zi = self.targets[t][2]
        b = self.buf(0, nz + zi)
        comm.step(
            [(b, self.sem_k[nz + t])],
            [(b, self.buf(1, zi), self.sem_x[t], comm.to_x)],
            None,
            lambda: add_rows(b, [b, self.mine(zi, 1, k)]),
        )

    def third(self, t):
        comm, at = self.comm, self.comm.at
        z, nz, k = at.z, at.nz, at.k
        d, side, zi = self.targets[t]
        b, landed = self.buf(0, zi), self.buf(1, zi)
        terms = [b, self.mine(zi, 0, k), landed]
        comm.arrive(b, self.sem_k[t])
        comm.arrive(landed, self.sem_x[t])
        if t == nz - 1:
            add_rows(self.total, terms)
            for way, on in ((1, z > 0), (-1, z < nz - 1)):
                buf, sem = self.passing(way, 0)

                @pl.when(on)
                def _():
                    comm.arrive(buf, sem)
                    add_rows(self.total, [self.total, buf])

            return
        add_rows(b, terms)
        buf, sem = self.passing(side, d)
        behind = z - side

        @pl.when((behind >= 0) & (behind < nz))
        def _():
            comm.arrive(buf, sem)
            add_rows(b, [b, buf])

        dst, sem = self.passing(side, d - 1)
        comm.step([], [(b, dst, sem, at.device(z + side, at.y, at.x, k))])

    def steps(self, produce=None):
        nz = self.comm.at.nz
        for i in range(nz + 2):
            if i < nz:
                if produce is not None:
                    produce(self.targets[i][2])
                self.first(i)
            yield
            for stage, lag in ((self.second, 1), (self.third, 2)):
                if 0 <= i - lag < nz:
                    stage(i - lag)
                    yield


def scatter_bufs(nz, rows, width):
    return [pltpu.VMEM((n * nz, rows, width), bf16) for n in (2, 1, 2)]


def along(ref, axis, i, size):
    r = pl.ds(pl.multiple_of(i * size, size), size)
    before = (slice(None),) * (len(ref.shape) - axis)
    return ref.at[before + (r,) + (slice(None),) * (axis - 1)]


class Swap:
    def __init__(self, array, unit_axis, feature_axis, units, depth, shape, plane=None, groups=1):
        self.array, self.shape, self.plane = array, shape, plane
        self.unit_axis, self.feature_axis, self.units, self.depth = unit_axis, feature_axis, units, depth
        self.groups = groups if feature_axis == 2 else 1
        self.out = jax.ShapeDtypeStruct(shape, bf16)

    def of_units(self, ref, z):
        if self.plane is not None:
            ref = ref.at[self.plane]
        return along(ref, self.unit_axis, z, self.units)

    def of_features(self, ref, z, y):
        return along(ref, self.feature_axis, 2 * z + y, self.depth)

    def runs(self, ref, nz, z, y):
        if self.groups == 1:
            return [self.of_features(ref, z, y)]
        r = self.depth // self.groups
        return [along(ref, 2, i * 2 * nz + 2 * z + y, r) for i in range(self.groups)]

    def cuts(self, piece):
        if self.groups == 1:
            return [piece]
        r = self.depth // self.groups
        return [along(piece, 2, i, r) for i in range(self.groups)]


def swap_in(comm, one, src, dst):
    at = comm.at
    z, y, x, k, nz = at.z, at.y, at.x, at.k, at.nz
    sem_z = [comm.sems(one.groups) for _ in range(nz)]
    sem_y = [comm.sems(one.groups) for _ in range(nz)]
    moved = []

    def sends():
        mine = one.runs(dst, nz, z, y)
        for d in range(1, nz):
            zi = (z + d) % nz
            parts = one.cuts(one.of_units(src, zi))
            for part, to, sem in zip(parts, mine, sem_z[d]):
                comm.step([], [(part, to, sem, at.device(zi, y, x, k))])
            yield
        for part, to, sem in zip(one.cuts(one.of_units(src, z)), mine, sem_y[0]):
            comm.step([], [(part, to, sem, comm.to_y)])
            moved.append(comm.move(part, to))
        yield

    def passes():
        for d in range(1, nz):
            for run, sem, on in zip(one.runs(dst, nz, (z + nz - d) % nz, y), sem_z[d], sem_y[d]):
                comm.step([(run, sem)], [(run, run, on, comm.to_y)])
            yield

    def arrivals():
        for d in range(nz):
            for run, sem in zip(one.runs(dst, nz, (z + nz - d) % nz, 1 - y), sem_y[d]):
                comm.arrive(run, sem)
        for wait in moved:
            wait()

    return sends(), passes(), arrivals


def add_piece(dst, src):
    if len(dst.shape) == 3:
        for p in range(dst.shape[0]):
            add_rows(dst.at[p], [dst.at[p], src.at[p]])
    else:
        add_rows(dst, [dst, src])


def swap_out_y(comm, one, src, landed):
    at = comm.at
    z, y, nz = at.z, at.y, at.nz
    order = list(range(1, nz)) + [0]
    sems = comm.sems(nz)

    def sends():
        for d in order:
            zi = (z + d) % nz
            comm.step([], [(one.of_features(src, zi, 1 - y), landed.at[zi], sems[d], comm.to_y)])
            yield

    def sums():
        for d in order:
            zi = (z + d) % nz
            comm.arrive(landed.at[zi], sems[d])
            add_piece(landed.at[zi], one.of_features(src, zi, y))
            yield

    return sends(), sums()


def swap_out_z(comm, one, summed, dst):
    at = comm.at
    z, y, x, k, nz = at.z, at.y, at.x, at.k, at.nz
    mine = one.of_units(dst, z)
    sems = comm.sems(nz)
    for d in list(range(1, nz)) + [0]:
        zi = (z + d) % nz
        if d:
            comm.step([], [(summed.at[zi], mine, sems[d], at.device(zi, y, x, k))])
            comm.late.append((one.of_units(dst, (z + nz - d) % nz), sems[d]))
        else:
            comm.keep(summed.at[zi], mine)
        yield


def paired(first, second):
    for _ in first:
        next(second, None)
        yield
    yield from second


def lagged(first, second, lag):
    n = 0
    for _ in first:
        n += 1
        if n > lag:
            next(second, None)
        yield
    yield from second


def chain(*many):
    for steps in many:
        yield from steps


def landing(nz, one, user_shape):
    shape = list(user_shape)
    shape[len(shape) - one.feature_axis] = one.depth
    return pltpu.VMEM((nz, *shape), bf16)


def comm_kernel(nz, groups, work, swaps, extra, n_in, n_out, *refs):
    given = [one for one in swaps if one.array is not None]
    m, g = len(swaps), len(given)
    ins, srcs = refs[:n_in], refs[n_in : n_in + g]
    outs = refs[n_in + g : n_in + g + n_out]
    dsts = refs[n_in + g + n_out : n_in + g + n_out + m]
    scratch = refs[n_in + g + n_out + m :]
    comm = Comm(Place(nz), scratch[-1], groups)
    work(comm, (swaps + extra, srcs, dsts), ins, outs, scratch[:-1])
    comm.finish()


def comm_call(name, nz, collective, work, ins, outs, scratch, swaps, swap_spec=ANY, vmem=48, groups=1, extra=()):
    given = [one.array for one in swaps if one.array is not None]
    return pl.pallas_call(
        functools.partial(comm_kernel, nz, groups, work, swaps, list(extra), len(ins), len(outs)),
        out_shape=[jax.ShapeDtypeStruct(s, d) for s, d, _ in outs] + [one.out for one in swaps],
        in_specs=[s for _, s in ins] + [swap_spec] * len(given),
        out_specs=[s for _, _, s in outs] + [ANY] * len(swaps),
        scratch_shapes=scratch + [DMA((700,))],
        compiler_params=pltpu.CompilerParams(
            collective_id=collective, has_side_effects=True, vmem_limit_bytes=vmem * 2**20
        ),
        name=name,
    )(*[v for v, _ in ins], *given)


def by_rows(lo, size, do):
    step = math.gcd(size, 16)

    def some_rows(i, _):
        do(pl.ds(pl.multiple_of(lo + i * step, step), step))
        return 0

    lax.fori_loop(0, size // step, some_rows, 0)


def two_parts(rows):
    return [(0, rows // 2), (rows // 2, rows // 2)]


def making_steps(nz):
    return 3 * nz - 5


def feature_pieces(nz, groups, d_model):
    a = 2 * nz
    r = d_model // a // groups
    return [(c, i * r, (i * a + c) * r, r) for c in range(a) for i in range(groups)]


def sum_gains(comm, groups, sums, sorted_sums, landed, total):
    at = comm.at
    z, y, x, k, nz = at.z, at.y, at.x, at.k, at.nz
    for c, lo, col, r in feature_pieces(nz, groups, sums.shape[1]):
        sorted_sums[c % 2, c // 2, :, lo : lo + r] = sums[:, col : col + r]
    sem = comm.sems(4 + nz)
    comm.step([], [(sorted_sums.at[1 - y], landed.at[pl.ds(0, nz)], sem[0], comm.to_y)])
    comm.arrive(landed.at[pl.ds(0, nz)], sem[0])
    sorted_sums[y] += landed[0:nz]
    for d in range(1, nz):
        zi = (z + d) % nz
        comm.step([], [(sorted_sums.at[y, zi], landed.at[nz + d], sem[d], at.device(zi, y, x, k))])
    total[...] = sorted_sums[y, z]
    for d in range(1, nz):
        comm.arrive(landed.at[nz + d], sem[d])
        total[...] += landed[nz + d]
    landed[nz] = total[...]
    for i, to in enumerate((comm.to_k, comm.to_x, comm.to_xk)):
        comm.step([], [(landed.at[nz], landed.at[2 * nz + i], sem[nz + i], to)])
    for i in range(3):
        comm.arrive(landed.at[2 * nz + i], sem[nz + i])
        total[...] += landed[2 * nz + i]


def gains_of_group(comm, groups, gain_ref, landed, gains):
    at = comm.at
    z, y, x, k, nz = at.z, at.y, at.x, at.k, at.nz
    sem = comm.sems(nz + 1)
    for d in range(1, nz):
        to = at.device((z + d) % nz, y, x, k)
        comm.step([], [(gain_ref, landed.at[y, z], sem[d], to)])
    landed[y, z] = gain_ref[...]
    for d in range(1, nz):
        comm.arrive(landed.at[y, (z + nz - d) % nz], sem[d])
    comm.step([], [(landed.at[y], landed.at[y], sem[0], comm.to_y)])
    comm.arrive(landed.at[1 - y], sem[0])
    for c, lo, col, r in feature_pieces(nz, groups, gains.shape[1]):
        gains[:, col : col + r] = landed[c % 2, c // 2, :, lo : lo + r].astype(f32)


def product_into(p_ref, rows, at_slot, lhs, rhs, rhs_dims):
    n = p_ref.shape[2]
    wide = math.gcd(n, 512)
    count = lhs[0].shape[0] // rows
    for j in range(n // wide):
        cols = slice(j * wide, (j + 1) * wide)
        total = None
        for one, right, dims in zip(lhs, rhs, rhs_dims):
            block = right[:, cols] if dims == 0 else right[cols, :]
            term = lax.dot_general(one, block, (((1,), (dims,)), ((), ())), preferred_element_type=f32)
            total = term if total is None else total + term
        p_ref[pl.ds(at_slot, count), :, cols] = total.astype(bf16).reshape(count, rows, wide)


def row_blocks(rows, keys, do):
    step = math.gcd(rows, 128)
    fine = max(16, min(128, 128 * 2048 // keys))
    for i in range(rows // step):

        def some(j, _):
            do(pl.ds(pl.multiple_of(i * step + j * fine, fine), fine))
            return 0

        lax.fori_loop(0, step // fine, some, 0)
        yield


def attend(heads, q_ref, k_ref, v_ref, at_q, at_k, o_ref, lse_ref):
    def block(r):
        visible = at_k[...] <= at_q[r, :]
        for h in range(heads):
            c = slice(h * HD, (h + 1) * HD)
            scores = lax.dot_general(
                q_ref[r, c], k_ref[:, c], (((1,), (1,)), ((), ())), preferred_element_type=f32
            )
            scores = jnp.where(visible, scores, -1e30)
            peak = jnp.max(scores, axis=-1, keepdims=True)
            weights = jnp.exp(scores - peak)
            total = jnp.sum(weights, axis=-1, keepdims=True)
            probs = (weights * (1.0 / total)).astype(bf16)
            o_ref[r, c] = jnp.dot(probs, v_ref[:, c], preferred_element_type=f32).astype(bf16)
            lse_ref[r, h : h + 1] = peak + jnp.log(total)

    yield from row_blocks(q_ref.shape[0], k_ref.shape[0], block)


def attend_back(heads, q_ref, k_ref, v_ref, at_q, at_k, o_ref, lse_ref, do_ref, dq_ref, dk_ref, dv_ref):
    over_rows = (((0,), (0,)), ((), ()))
    over_cols = (((1,), (1,)), ((), ()))
    dk_ref[...] = jnp.zeros_like(dk_ref)
    dv_ref[...] = jnp.zeros_like(dv_ref)

    def block(r):
        visible = at_k[...] <= at_q[r, :]
        for h in range(heads):
            c = slice(h * HD, (h + 1) * HD)
            q, grad = q_ref[r, c], do_ref[r, c]
            scores = lax.dot_general(q, k_ref[:, c], over_cols, preferred_element_type=f32)
            scores = jnp.where(visible, scores, -1e30)
            probs = jnp.exp(scores - lse_ref[r, h : h + 1])
            delta = jnp.sum(
                grad.astype(f32) * o_ref[r, c].astype(f32), axis=-1, keepdims=True
            )
            prob_grad = lax.dot_general(grad, v_ref[:, c], over_cols, preferred_element_type=f32)
            score_grad = (probs * (prob_grad - delta)).astype(bf16)
            dq_ref[r, c] = jnp.dot(score_grad, k_ref[:, c], preferred_element_type=f32) * HD ** (-0.5)
            dk_ref[c, :] += lax.dot_general(q, score_grad, over_rows, preferred_element_type=f32)
            dv_ref[c, :] += lax.dot_general(
                grad, probs.astype(bf16), over_rows, preferred_element_type=f32
            )

    yield from row_blocks(q_ref.shape[0], k_ref.shape[0], block)


def other_halves(u):
    width = u.shape[1]
    low = lax.broadcasted_iota(jnp.int32, (1, width), 1) % HD < HD // 2
    return jnp.where(low, pltpu.roll(u, width - HD // 2, 1), pltpu.roll(u, HD // 2, 1))


def forward_work(heads, groups, comm, swap, ins, outs, scratch):
    x_ref, gain_ref, cos, sin, at_q, at_k = ins
    gains, q_ref, o_ref, lse_ref, hidden, rows_attn, k_out, v_out, rows_mlp = outs
    normed, landed, rows_v, qkv_v, out_v, k_all, v_all, p_ref = scratch[:8]
    bufs = scratch[8:]
    swaps, srcs, dsts = swap
    at = comm.at
    y, nz = at.y, at.nz
    rows, d_model = x_ref.shape
    tall = 4 * rows
    keys = q_ref.shape[0]
    width = q_ref.shape[1]

    places = (qkv_v, out_v) + tuple(dsts[2:])
    qkv, out, down, gate, up = [swap_in(comm, *v) for v in zip(swaps, srcs, places)]
    exhaust(qkv[0])
    gains_of_group(comm, groups, gain_ref, landed, gains)

    def norm_1(r):
        x = x_ref[r, :].astype(f32)
        normed[r, :] = (x * inv_rms(x) * gains[0:1, :]).astype(bf16)

    by_rows(0, rows, norm_1)
    shards = gather_steps(comm, normed, rows_v, 0, rows)
    advance(shards, z_steps(at))
    take_turns(shards, chain(out[0], qkv[1], down[0]))
    qkv[2]()
    comm.keep(qkv_v, dsts[0])
    comm.keep(rows_v, rows_attn)

    def half(ref, g, yy):
        return ref.at[pl.ds(pl.multiple_of((yy * groups + g) * keys, keys), keys), :]

    group = at.first // (2 * nz)
    mine = [half(ref, group, y) for ref in (k_all, v_all)]

    def project(i, _):
        r = pl.ds(pl.multiple_of(i * tall, tall), tall)
        block = rows_v[r, :]

        def turned(p):
            u = jnp.dot(block, qkv_v[p], preferred_element_type=f32)
            return (u * cos[r, :] + other_halves(u) * sin[r, :]).astype(bf16)

        q_ref[r, :] = turned(0) * jnp.asarray(HD ** (-0.5), bf16)
        mine[0][r, :] = turned(1)
        mine[1][r, :] = jnp.dot(block, qkv_v[2], preferred_element_type=f32).astype(bf16)
        return 0

    lax.fori_loop(0, nz, project, 0)
    sem = comm.sems(4 * groups)
    for i, ref in enumerate(mine):
        comm.step([], [(ref, ref, sem[i], comm.to_y)])
        for g, f, device in comm.afar:
            comm.step([], [(ref, ref, sem[2 + (2 * g + f) * 2 + i - 2], device)])
    exhaust(gate[0], out[1])
    out[2]()
    comm.keep(out_v, dsts[1])
    for i, (ref, dst) in enumerate(((k_all, k_out), (v_all, v_out))):
        comm.arrive(half(ref, group, 1 - y), sem[i])
        for g, f, device in comm.afar:
            come = half(ref, (group + groups - g) % groups, y + f * (1 - 2 * y))
            comm.arrive(come, sem[2 + (2 * g + f) * 2 + i - 2])
        comm.keep(ref, dst)
    take_turns(
        attend(heads, q_ref, k_all, v_all, at_q, at_k, o_ref, lse_ref), chain(down[1], up[0], gate[1])
    )

    def norm_2(r):
        h = hidden[r, :] + x_ref[r, :].astype(f32)
        hidden[r, :] = h
        normed_2[r, :] = (h * inv_rms(h) * gains[1:2, :]).astype(bf16)

    def produce(zi):
        r = pl.ds(pl.multiple_of(zi * tall, tall), tall)
        product_into(p_ref, rows, zi * 4, [o_ref[r, :]], [out_v], [0])

    normed_2, total = bufs[3], bufs[4]

    def part(lo, size, making):
        yield from Scatter(comm, p_ref, bufs[:3], total, lo, size).steps(making)
        r = pl.ds(lo, size)
        for c, piece, col, n in feature_pieces(nz, groups, d_model) if groups > 1 else [(0, 0, 0, d_model)]:
            frm = c * (d_model // (2 * nz)) + piece
            hidden[r, col : col + n] = total[r, frm : frm + n]
        by_rows(lo, size, norm_2)
        yield
        yield from gather_steps(comm, normed_2, rows_mlp, lo, size)

    front, rear = [part(lo, size, None if lo else produce) for lo, size in two_parts(rows)]
    advance(front, making_steps(nz))
    take_turns(lagged(front, rear, 1), up[1])
    for one in (down, gate, up):
        one[2]()


def norm_back(grad, unit, rms, gain):
    unit_grad = grad * gain
    return rms * (unit_grad - unit * jnp.mean(unit_grad * unit, axis=-1, keepdims=True))


def back_work(groups, comm, swap, ins, outs, scratch):
    rows_mlp, gate_w, up_w, dn_w, hidden, dy_ref, gains = ins
    residual, branch_rows, gain_sum, block_out, gate_out, up_out = outs
    total, rounded, p_ref, q_ref, pre, gates, n2, dy, gate_g, up_g, dn_g, dn_landed, gate_landed = scratch[:13]
    bufs, bufs_q, total_q = scratch[13:16], scratch[16:19], scratch[19]
    (down, gate_swap), _, dsts = swap
    at = comm.at
    nz = at.nz
    rows = hidden.shape[0]
    tall = 4 * rows
    gain_sum[...] = jnp.zeros_like(gain_sum)
    sems = comm.sems(nz)

    def load(t, zi):
        r = pl.ds(pl.multiple_of(zi * tall, tall), tall)
        return pltpu.make_async_copy(rows_mlp.at[r, :], n2.at[r, :], sems[t])

    for t, target in enumerate(far_first(at)):
        load(t, target[2]).start()
    turn = iter(range(nz))

    def forward(zi):
        load(next(turn), zi).wait()
        r = pl.ds(pl.multiple_of(zi * tall, tall), tall)
        x = n2[r, :]
        gate = jnp.dot(x, gate_w[...], preferred_element_type=f32)
        up = jnp.dot(x, up_w[...], preferred_element_type=f32)
        pre[0, r, :] = gate
        pre[1, r, :] = up
        hid = (gate * jax.nn.sigmoid(gate) * up).astype(bf16)
        gates[2, r, :] = hid
        product_into(q_ref, rows, zi * 4, [hid], [dn_w], [0])

    def backward(zi):
        r = pl.ds(pl.multiple_of(zi * tall, tall), tall)
        grad = lax.dot_general(
            dy[r, :], dn_w[...], (((1,), (1,)), ((), ())), preferred_element_type=f32
        )
        gate, up = pre[0, r, :], pre[1, r, :]
        sig = jax.nn.sigmoid(gate)
        gate_grad = (grad * up * (sig * (1.0 + gate * (1.0 - sig)))).astype(bf16)
        up_grad = (grad * (gate * sig)).astype(bf16)
        gates[0, r, :] = gate_grad
        gates[1, r, :] = up_grad
        product_into(p_ref, rows, zi * 4, [gate_grad, up_grad], [gate_w, up_w], [1, 1])

    def back(r):
        h = hidden[r, :]
        rms = inv_rms(h)
        unit, grad = h * rms, total[r, :]
        gain_sum[...] += jnp.sum(grad * unit, axis=0, keepdims=True)
        dh = dy_ref[r, :].astype(f32) + norm_back(grad, unit, rms, gains[1:2, :])
        residual[r, :] = dh
        rounded[r, :] = dh.astype(bf16)

    def out(r):
        block_out[r, :] = (hidden[r, :] + total_q[r, :]).astype(bf16)

    def gradients(which):
        d_model = n2.shape[1]
        depth = d_model // (2 * nz)
        over_rows = (((0,), (0,)), ((), ()))
        pieces = feature_pieces(nz, groups, d_model)
        per = max(1, len(pieces) // 4)
        for j in range(0, len(pieces), per):
            for c, lo, col, r in pieces[j : j + per]:
                f, to = slice(col, col + r), slice(c * depth + lo, c * depth + lo + r)
                if which == 2:
                    dn_g[:, to] = lax.dot_general(
                        gates[2], dy[:, f], over_rows, preferred_element_type=f32
                    ).astype(bf16)
                else:
                    (gate_g, up_g)[which][to, :] = lax.dot_general(
                        n2[:, f], gates[which], over_rows, preferred_element_type=f32
                    ).astype(bf16)
            yield

    def output():
        yield from Scatter(comm, q_ref, bufs_q, total_q, 0, rows).steps(forward)
        by_rows(0, rows, out)

    def part(lo, size, making):
        yield from Scatter(comm, p_ref, bufs, total, lo, size).steps(making)
        by_rows(lo, size, back)
        yield
        yield from gather_steps(comm, rounded, branch_rows, lo, size)

    shards = gather_steps(comm, dy_ref, dy, 0, rows)
    side = output()
    advance(shards, 1)
    for _ in range(making_steps(nz)):
        next(side)
        advance(shards, 1)
    for _ in shards:
        next(side, None)
    front, rear = [part(lo, size, None if lo else backward) for lo, size in two_parts(rows)]
    for _ in range(making_steps(nz)):
        next(front)
        advance(side, 1)
    down_sends, down_sums = swap_out_y(comm, down, dn_g, dn_landed)
    gate_sends, gate_sums = swap_out_y(comm, gate_swap, gate_g, gate_landed)

    def weights():
        yield from gradients(2)
        yield from down_sends
        yield from gradients(0)
        yield from gate_sends
        yield from gradients(1)
        comm.keep(up_g, up_out)
        yield from paired(down_sums, swap_out_z(comm, down, dn_landed, dsts[0]))
        yield from gate_sums

    take_turns(lagged(front, rear, 1), side, weights())
    comm.keep(gate_landed, gate_out)


def tail_work(heads, groups, comm, swap, ins, outs, scratch):
    (q_ref, k_ref, v_ref, at_q, at_k, o_ref, lse_ref, do_ref, gate_sum, up_grad, out_grad,
     rows_attn, cos, sin, qkv_w, residual, x_ref, gains, gain_sum_2) = ins
    grad_in, gain_out = outs
    (dq_ref, dk_ref, dv_ref, going, come, up_landed, out_landed, qkv_landed, proj, qkv_g,
     total, gain_sums, sorted_sums, landed, p_ref) = scratch[:15]
    bufs = scratch[15:]
    (gate, up, out, qkv), _, dsts = swap
    at = comm.at
    y, nz = at.y, at.nz
    keys, width = q_ref.shape
    rows, d_model = x_ref.shape
    tall = 4 * rows
    gain_sums[0:1, :] = jnp.zeros_like(gain_sum_2)
    gain_sums[1:2, :] = gain_sum_2[...]

    up_sends, up_sums = swap_out_y(comm, up, up_grad, up_landed)
    out_sends, out_sums = swap_out_y(comm, out, out_grad, out_landed)
    exhaust(up_sends, out_sends, swap_out_z(comm, gate, gate_sum, dsts[0]))
    more = chain(
        paired(up_sums, swap_out_z(comm, up, up_landed, dsts[1])),
        paired(out_sums, swap_out_z(comm, out, out_landed, dsts[2])),
    )
    compute = attend_back(
        heads, q_ref, k_ref, v_ref, at_q, at_k, o_ref, lse_ref, do_ref, dq_ref, dk_ref, dv_ref
    )
    take_turns(compute, more)

    group = at.first // (2 * nz)

    def share(ref, g, yy):
        return ref.at[:, pl.ds(pl.multiple_of((yy * groups + g) * keys, keys), keys)]

    others = [(0, 1, comm.to_y)] + comm.afar
    sem = comm.sems(2 * len(others))
    for j, (g, f, device) in enumerate(others):
        for i, ref in enumerate((dk_ref, dv_ref)):
            theirs = share(ref, (group + g) % groups, y + f * (1 - 2 * y))
            going[j, i] = theirs[...].astype(bf16)
            comm.step([], [(going.at[j, i], come.at[j, i], sem[2 * j + i], device)])

    def unturned(u, r):
        return (u * cos[r, :] - other_halves(u) * sin[r, :]).astype(bf16)

    every = pl.ds(0, keys)
    proj[:, 0:width] = unturned(dq_ref[...], every)
    for i, ref in enumerate((dk_ref, dv_ref)):
        grad = share(ref, group, y)[...]
        for j in range(len(others)):
            comm.arrive(come.at[j, i], sem[2 * j + i])
            grad = grad + come[j, i].astype(f32)
        grad = grad.T
        cols = slice((i + 1) * width, (i + 2) * width)
        proj[:, cols] = unturned(grad, every) if i == 0 else grad.astype(bf16)

    def back(r):
        x = x_ref[r, :].astype(f32)
        rms = inv_rms(x)
        unit, grad = x * rms, total[r, :]
        gain_sums[0:1, :] += jnp.sum(grad * unit, axis=0, keepdims=True)
        grad_in[r, :] = residual[r, :] + norm_back(grad, unit, rms, gains[0:1, :])

    def produce(zi):
        r = pl.ds(pl.multiple_of(zi * tall, tall), tall)
        lhs = [proj[r, p * width : (p + 1) * width] for p in range(3)]
        product_into(p_ref, rows, zi * 4, lhs, [qkv_w.at[p] for p in range(3)], [1] * 3)

    qkv_sends, qkv_sums = swap_out_y(comm, qkv, qkv_g, qkv_landed)

    def weights():
        depth = d_model // (2 * nz)
        pieces = feature_pieces(nz, groups, d_model)
        per = max(1, len(pieces) // 4)
        for j in range(0, len(pieces), per):
            for c, lo, col, n in pieces[j : j + per]:
                grad = lax.dot_general(
                    rows_attn[:, col : col + n], proj[...], (((0,), (0,)), ((), ())),
                    preferred_element_type=f32,
                ).astype(bf16)
                for p in range(3):
                    qkv_g[p, c * depth + lo : c * depth + lo + n, :] = grad[:, p * width : (p + 1) * width]
            yield
        yield from qkv_sends
        yield from paired(qkv_sums, swap_out_z(comm, qkv, qkv_landed, dsts[3]))

    steps = Scatter(comm, p_ref, bufs, total, 0, rows).steps(produce)
    advance(steps, making_steps(nz))
    take_turns(weights(), steps)
    by_rows(0, rows, back)
    sum_gains(comm, groups, gain_sums, sorted_sums, landed, gain_out)


def body(
    block_input,
    qkv_weight,
    out_weight,
    gate_up_weight,
    down_weight,
    norm_gains,
    positions,
    layer_output_gradient,
):
    n_ctx, n_tp = lax.axis_size("ctx"), lax.axis_size("tp")
    nz = math.gcd(qkv_weight.shape[2] // HD, n_ctx // 2)
    nz = math.gcd(nz, 4)
    a = 2 * nz
    b = n_ctx // a
    assert n_tp == 4
    depth = qkv_weight.shape[1] * b
    d_model = depth * a
    width = qkv_weight.shape[2] // nz
    heads = width // HD
    units = down_weight.shape[0] // nz
    rows = block_input.shape[0]
    across = [[i * a + j for i in range(b)] for j in range(a)]

    def over_groups(v, axis):
        return lax.all_gather(v, "ctx", axis=axis, tiled=True, axis_index_groups=across) if b > 1 else v

    def to_groups(v, axis):
        if b == 1:
            return v
        return lax.psum_scatter(
            v, "ctx", scatter_dimension=axis, tiled=True, axis_index_groups=across
        )

    def model_order(v, axis):
        if b == 1:
            return v
        s = v.shape
        w = v.reshape(s[:axis] + (a, b, depth // b) + s[axis + 1 :])
        return jnp.swapaxes(w, axis, axis + 1).reshape(s)

    def swap_order(v, axis):
        if b == 1:
            return v
        s = v.shape
        w = v.reshape(s[:axis] + (b, a, depth // b) + s[axis + 1 :])
        return jnp.swapaxes(w, axis, axis + 1).reshape(s)

    my_gains = over_groups(norm_gains, 1)
    group_rows = 4 * nz * rows
    n_keys = 2 * b * group_rows
    y, group = lax.axis_index("ctx") % 2, lax.axis_index("ctx") // a
    by_place = positions.reshape(b, nz, 2, n_tp * rows)
    key_pos = by_place.transpose(2, 0, 1, 3).reshape(2 * b, group_rows)
    own_pos = lax.dynamic_index_in_dim(key_pos, y * b + group, 0, keepdims=False)
    cos_tab, sin_tab = rope_tables(own_pos, HD)
    cos_wide = jnp.tile(cos_tab[:, 0, :], (1, 2 * heads))
    sin_wide = jnp.tile(jnp.concatenate([-sin_tab, sin_tab], axis=-1)[:, 0, :], (1, heads))
    places = [(own_pos[:, None], VMEM), (key_pos.reshape(1, -1), VMEM)]
    gu_all = over_groups(gate_up_weight, 1)
    partials = pltpu.VMEM((4 * nz, rows, d_model), bf16)
    (gains, query_bf, attn_bf, log_total, hidden, rows_attn, key_all, value_all, rows_mlp,
     qkv_w, out_w, dn_w, gate_w, up_w) = comm_call(
        "forward", nz, 0, functools.partial(forward_work, heads, b),
        [(block_input, VMEM), (my_gains, VMEM), (cos_wide, VMEM), (sin_wide, VMEM)] + places,
        [((2, d_model), f32, VMEM), ((group_rows, width), bf16, VMEM),
         ((group_rows, width), bf16, VMEM), ((group_rows, heads), f32, VMEM),
         ((rows, d_model), f32, VMEM), ((group_rows, d_model), bf16, ANY),
         ((n_keys, width), bf16, ANY), ((n_keys, width), bf16, ANY),
         ((group_rows, d_model), bf16, ANY)],
        [pltpu.VMEM((rows, d_model), bf16), pltpu.VMEM((2, nz) + my_gains.shape, bf16),
         pltpu.VMEM((group_rows, d_model), bf16), pltpu.VMEM((3, d_model, width), bf16),
         pltpu.VMEM((width, d_model), bf16), pltpu.VMEM((n_keys, width), bf16),
         pltpu.VMEM((n_keys, width), bf16), partials]
        + scatter_bufs(nz, rows, d_model)
        + [pltpu.VMEM((rows, d_model), bf16), pltpu.VMEM((rows, d_model), f32)],
        [Swap(over_groups(qkv_weight, 1), 1, 2, width, depth, (3, d_model, width), None, b),
         Swap(over_groups(out_weight, 1), 2, 1, width, depth, (width, d_model)),
         Swap(over_groups(down_weight, 1), 2, 1, units, depth, (units, d_model))]
        + [Swap(gu_all, 1, 2, units, depth, (d_model, units), p, b) for p in (0, 1)],
        groups=b,
    )
    out_w, dn_w = model_order(out_w, 1), model_order(dn_w, 1)
    down_swap = Swap(None, 2, 1, units, depth, (nz * units, depth))
    half_swap = Swap(None, 1, 2, units, depth, (depth, nz * units))
    residual_grad, branch_rows, gain_sum_2, block_output, gate_sum, up_grad, dn_back = comm_call(
        "back", nz, 3, functools.partial(back_work, b),
        [(rows_mlp, ANY), (gate_w, VMEM), (up_w, VMEM), (dn_w, VMEM),
         (hidden, VMEM), (layer_output_gradient, VMEM), (gains, VMEM)],
        [((rows, d_model), f32, VMEM), ((group_rows, d_model), bf16, ANY),
         ((1, d_model), f32, VMEM), ((rows, d_model), bf16, VMEM),
         ((nz, depth, units), bf16, ANY), ((d_model, units), bf16, ANY)],
        [pltpu.VMEM((rows, d_model), f32), pltpu.VMEM((rows, d_model), bf16), partials, partials,
         pltpu.VMEM((2, group_rows, units), f32), pltpu.VMEM((3, group_rows, units), bf16),
         pltpu.VMEM((group_rows, d_model), bf16), pltpu.VMEM((group_rows, d_model), bf16),
         pltpu.VMEM((d_model, units), bf16), pltpu.VMEM((d_model, units), bf16),
         pltpu.VMEM((units, d_model), bf16),
         landing(nz, down_swap, (units, d_model)), landing(nz, half_swap, (d_model, units))]
        + scatter_bufs(nz, rows, d_model) + scatter_bufs(nz, rows, d_model)
        + [pltpu.VMEM((rows, d_model), f32)],
        [down_swap],
        vmem=60,
        extra=[half_swap],
    )
    out_weight_grad = jnp.einsum("te,td->ed", attn_bf, branch_rows, preferred_element_type=f32)
    attn_grad_bf = jnp.einsum("td,ed->te", branch_rows, out_w, preferred_element_type=f32).astype(bf16)
    out_swap = Swap(None, 2, 1, width, depth, (nz * width, depth))
    qkv_swap = Swap(None, 1, 2, width, depth, (3, depth, nz * width))
    others = 2 * b - 1
    layer_input_gradient, gain_sums, gate_back, up_back, out_back, qkv_back = comm_call(
        "tail", nz, 4, functools.partial(tail_work, heads, b),
        [(query_bf, VMEM), (key_all, VMEM), (value_all, VMEM)] + places
        + [(attn_bf, VMEM), (log_total, VMEM), (attn_grad_bf, VMEM), (gate_sum, VMEM),
           (up_grad, VMEM), (swap_order(out_weight_grad.astype(bf16), 1), VMEM),
           (rows_attn, VMEM), (cos_wide, VMEM), (sin_wide, VMEM), (qkv_w, VMEM),
           (residual_grad, VMEM), (block_input, VMEM), (gains, VMEM), (gain_sum_2, VMEM)],
        [((rows, d_model), f32, VMEM), ((2, depth), f32, VMEM)],
        [pltpu.VMEM((group_rows, width), f32),
         pltpu.VMEM((width, n_keys), f32), pltpu.VMEM((width, n_keys), f32),
         pltpu.VMEM((others, 2, width, group_rows), bf16),
         pltpu.VMEM((others, 2, width, group_rows), bf16),
         landing(nz, half_swap, (d_model, units)), landing(nz, out_swap, (width, d_model)),
         landing(nz, qkv_swap, (3, d_model, width)),
         pltpu.VMEM((group_rows, 3 * width), bf16), pltpu.VMEM((3, d_model, width), bf16),
         pltpu.VMEM((rows, d_model), f32), pltpu.VMEM((2, d_model), f32),
         pltpu.VMEM((2, nz, 2, depth), f32), pltpu.VMEM((2 * nz + 3, 2, depth), f32), partials]
        + scatter_bufs(nz, rows, d_model),
        [half_swap, half_swap, out_swap, qkv_swap],
        vmem=56,
        groups=b,
    )
    gu_back = jnp.stack([gate_back, up_back])
    if b > 1:
        gain_sums = lax.psum(gain_sums, "ctx", axis_index_groups=across)
    gain_cols = d_model // (n_ctx * n_tp)
    gain_part = lax.dynamic_slice_in_dim(
        gain_sums, (group * n_tp + lax.axis_index("tp")) * gain_cols, gain_cols, 1
    )
    return (
        block_output,
        layer_input_gradient,
        to_groups(qkv_back, 1).astype(f32),
        to_groups(out_back, 1).astype(f32),
        to_groups(gu_back, 1).astype(f32),
        to_groups(dn_back, 1).astype(f32),
        gain_part,
    )


def solution(mesh):
    placed = (
        P(("ctx", "tp"), None),
        P(None, "ctx", "tp"),
        P("tp", "ctx"),
        P(None, "ctx", "tp"),
        P("tp", "ctx"),
        P(None, "ctx"),
        P(),
        P(("ctx", "tp"), None),
    )
    return jax.shard_map(
        body,
        mesh=mesh,
        in_specs=placed,
        out_specs=(
            P(("ctx", "tp"), None),
            P(("ctx", "tp"), None),
            P(None, "ctx", "tp"),
            P("tp", "ctx"),
            P(None, "ctx", "tp"),
            P("tp", "ctx"),
            P(None, ("ctx", "tp")),
        ),
        check_vma=False,
    )
```

```python
import functools
import math

import jax
import jax.numpy as jnp
from jax import lax
from jax.experimental import pallas as pl
from jax.experimental.pallas import tpu as pltpu
from jax.sharding import PartitionSpec as P

HD = 64
MESH = pl.DeviceIdType.MESH
DMA = pltpu.SemaphoreType.DMA
ANY = pl.BlockSpec(memory_space=pl.ANY)
VMEM = pl.BlockSpec(memory_space=pltpu.VMEM)
bf16 = jnp.bfloat16
f32 = jnp.float32

norm_eps = 1e-05
rope_base = 130000.0


def inv_rms(values):
    return lax.rsqrt(jnp.mean(values * values, axis=-1, keepdims=True) + norm_eps)


def rope_tables(where_at, head_dim):
    half_dim = head_dim // 2
    inv_freq = rope_base ** (-(jnp.arange(half_dim, dtype=f32) * 2.0 / head_dim))
    angles = where_at.astype(f32)[:, None] * inv_freq[None, :]
    return (jnp.cos(angles)[:, None, :], jnp.sin(angles)[:, None, :])


def rotate(values, cos_tab, sin_tab, n_heads, head_dim):
    shaped = values.reshape(values.shape[0], n_heads, head_dim)
    half_dim = head_dim // 2
    lower_half, upper_half = (shaped[..., :half_dim], shaped[..., half_dim:])
    turned = jnp.concatenate(
        [lower_half * cos_tab - upper_half * sin_tab, upper_half * cos_tab + lower_half * sin_tab],
        axis=-1,
    )
    return turned.reshape(values.shape[0], n_heads * head_dim)


def unrotate(values, cos_tab, sin_tab, n_heads, head_dim):
    return rotate(values, cos_tab, -sin_tab, n_heads, head_dim)


class Place:
    def __init__(self, nz):
        ctx, tp = lax.axis_index("ctx"), lax.axis_index("tp")
        self.nz = nz
        self.first = ctx // (2 * nz) * (2 * nz)
        self.z, self.y = (ctx - self.first) // 2, (ctx - self.first) % 2
        self.x, self.k = tp // 2, tp % 2

    def device(self, z, y, x, k):
        return {"ctx": self.first + 2 * z + y, "tp": 2 * x + k}

    def elsewhere(self, g, flip):
        n = lax.axis_size("ctx")
        y = self.y + flip * (1 - 2 * self.y)
        return {"ctx": (self.first + g * 2 * self.nz) % n + 2 * self.z + y}


def slot_of(z, x, k):
    return (z * 2 + x) * 2 + k


class Comm:
    def __init__(self, at, pool, groups=1):
        self.at, self.pool, self.used, self.ends, self.late = at, pool, 0, [], []
        z, y, x, k, nz = at.z, at.y, at.x, at.k, at.nz
        self.to_x = at.device(z, y, 1 - x, k)
        self.to_k = at.device(z, y, x, 1 - k)
        self.to_y = at.device(z, 1 - y, x, k)
        self.to_xk = at.device(z, y, 1 - x, 1 - k)
        peers = [self.to_x, self.to_k, self.to_y, self.to_xk]
        self.afar = [(g, f, at.elsewhere(g, f)) for g in range(1, groups) for f in (0, 1)]
        peers += [device for _, _, device in self.afar]
        peers += [at.device((z + d) % nz, y, x, k) for d in range(1, nz)]
        barrier = pltpu.get_barrier_semaphore()
        for peer in peers:
            pl.semaphore_signal(barrier, inc=1, device_id=peer, device_id_type=MESH)
        pl.semaphore_wait(barrier, len(peers))

    def sem(self):
        self.used += 1
        return self.pool.at[self.used - 1]

    def sems(self, n):
        return [self.sem() for _ in range(n)]

    def step(self, arrivals, copies, cond=None, then=None):
        sems = self.sems(len(copies))

        def copy(i):
            src, dst, recv_sem, device = copies[i]
            return pltpu.make_async_remote_copy(
                src_ref=src,
                dst_ref=dst,
                send_sem=sems[i],
                recv_sem=recv_sem,
                device_id=device,
                device_id_type=MESH,
            )

        def go():
            for buf, sem in arrivals:
                self.arrive(buf, sem)
            if then is not None:
                then()
            for i in range(len(copies)):
                copy(i).start()

        def end():
            for i in range(len(copies)):
                copy(i).wait_send()

        if cond is None:
            go()
        else:
            pl.when(cond)(go)
        if copies:
            self.ends.append((cond, end))

    def move(self, src, dst):
        copy = pltpu.make_async_copy(src, dst, self.sem())
        copy.start()
        return copy.wait

    def keep(self, src, dst):
        self.ends.append((None, self.move(src, dst)))

    def arrive(self, buf, recv_sem):
        pltpu.make_async_remote_copy(
            src_ref=buf,
            dst_ref=buf,
            send_sem=recv_sem,
            recv_sem=recv_sem,
            device_id=self.to_k,
            device_id_type=MESH,
        ).wait_recv()

    def finish(self):
        for buf, sem in self.late:
            self.arrive(buf, sem)
        for cond, end in self.ends:
            if cond is None:
                end()
            else:
                pl.when(cond)(end)


def take_turns(*steps):
    steps = list(steps)
    while steps:
        for one in list(steps):
            if next(one, steps) is steps:
                steps.remove(one)


def advance(steps, n):
    for _ in range(n):
        next(steps, None)


def exhaust(*many):
    for steps in many:
        for _ in steps:
            pass


def line(at):
    places = []
    for d in range(1, at.nz):
        places.append((d, -1, (at.z + at.nz - d) % at.nz, at.z >= d))
        places.append((d, 1, (at.z + d) % at.nz, at.z + d < at.nz))
    return places


def z_steps(at):
    return 2 * at.nz - 1


def gather_steps(comm, own, o_ref, lo, size):
    at = comm.at
    z, x, k, nz = at.z, at.x, at.k, at.nz
    rows = own.shape[0]
    places = [(0, 0, z, None)] + line(at)
    n = len(places)
    sem_z, sem_x, sem_k = (comm.sems(m * n) for m in (1, 1, 2))

    def part(slot):
        return o_ref.at[pl.ds(pl.multiple_of(slot * rows + lo, size), size), :]

    for i, (d, side, zi, cond) in enumerate(places):
        slot = slot_of(zi, x, k)
        here = own.at[pl.ds(lo, size), :] if d == 0 else part(slot)
        if d:
            comm.step([(part(slot), sem_z[i])], [], cond)
        for way in (1, -1):
            if d < nz - 1 and side != way:
                on = (z < nz - 1) if way == 1 else (z > 0)
                if cond is not None:
                    on = on & cond
                to = at.device((z + nz + way) % nz, at.y, x, k)
                j = next(j for j, p in enumerate(places) if p[0] == d + 1 and p[1] == -way)
                comm.step([], [(here, part(slot), sem_z[j], to)], on)
        comm.step(
            [],
            [
                (here, part(slot), sem_x[i], comm.to_x),
                (here, part(slot), sem_k[i], comm.to_k),
            ],
            cond,
        )
        if d == 0:
            moved = comm.move(here, part(slot))
        yield
    for i, (d, side, zi, cond) in enumerate(places):
        slot = slot_of(zi, 1 - x, k)
        comm.step(
            [(part(slot), sem_x[i])], [(part(slot), part(slot), sem_k[n + i], comm.to_k)], cond
        )
        yield
    for h, xh in enumerate((x, 1 - x)):
        for i, (d, side, zi, cond) in enumerate(places):
            comm.step([(part(slot_of(zi, xh, 1 - k)), sem_k[h * n + i])], [], cond)
    moved()


def add_rows(dst, terms):
    rows = dst.shape[0]
    step = math.gcd(rows, 16)

    def some_rows(i, _):
        r = pl.ds(pl.multiple_of(i * step, step), step)
        total = terms[0][r, :].astype(f32)
        for term in terms[1:]:
            total = total + term[r, :].astype(f32)
        dst[r, :] = total.astype(dst.dtype)
        return 0

    lax.fori_loop(0, rows // step, some_rows, 0)


def far_first(at):
    nz = at.nz
    orders = []
    for z in range(nz):
        others = sorted((c for c in range(nz) if c != z), key=lambda c: (-abs(c - z), c))
        orders.append([(abs(c - z), 1 if c > z else -1, c) for c in others] + [(0, 0, z)])
    here = [1 - ((at.z - c) * (at.z - c) + nz * nz - 1) // (nz * nz) for c in range(nz)]
    return [
        tuple(sum(here[c] * orders[c][t][i] for c in range(nz)) for i in range(3))
        for t in range(nz)
    ]


class Scatter:
    def __init__(self, comm, p_ref, bufs, total, lo, size):
        nz = comm.at.nz
        self.comm, self.p_ref, self.bufs = comm, p_ref, bufs
        self.range = pl.ds(lo, size)
        self.total = total.at[self.range, :]
        self.targets = far_first(comm.at)
        self.sem_k, self.sem_x = comm.sems(2 * nz), comm.sems(nz)
        self.sem_z = comm.used
        comm.sems(2 * nz)

    def buf(self, b, j):
        return self.bufs[b].at[j, self.range, :]

    def mine(self, zi, flip, core):
        x = self.comm.at.x
        return self.p_ref.at[slot_of(zi, 1 - x if flip else x, core), self.range, :]

    def passing(self, side, d):
        i = (side + 1) // 2 * self.comm.at.nz + d
        return self.buf(2, i), self.comm.pool.at[self.sem_z + i]

    def first(self, t):
        comm, nz, k = self.comm, self.comm.at.nz, self.comm.at.k
        zi = self.targets[t][2]
        comm.step(
            [],
            [
                (self.mine(zi, flip, 1 - k), self.buf(0, flip * nz + zi),
                 self.sem_k[flip * nz + t], comm.to_k)
                for flip in (1, 0)
            ],
        )

    def second(self, t):
        comm, nz, k = self.comm, self.comm.at.nz, self.comm.at.k
        zi = self.targets[t][2]
        b = self.buf(0, nz + zi)
        comm.step(
            [(b, self.sem_k[nz + t])],
            [(b, self.buf(1, zi), self.sem_x[t], comm.to_x)],
            None,
            lambda: add_rows(b, [b, self.mine(zi, 1, k)]),
        )

    def third(self, t):
        comm, at = self.comm, self.comm.at
        z, nz, k = at.z, at.nz, at.k
        d, side, zi = self.targets[t]
        b, landed = self.buf(0, zi), self.buf(1, zi)
        terms = [b, self.mine(zi, 0, k), landed]
        comm.arrive(b, self.sem_k[t])
        comm.arrive(landed, self.sem_x[t])
        if t == nz - 1:
            add_rows(self.total, terms)
            for way, on in ((1, z > 0), (-1, z < nz - 1)):
                buf, sem = self.passing(way, 0)

                @pl.when(on)
                def _():
                    comm.arrive(buf, sem)
                    add_rows(self.total, [self.total, buf])

            return
        add_rows(b, terms)
        buf, sem = self.passing(side, d)
        behind = z - side

        @pl.when((behind >= 0) & (behind < nz))
        def _():
            comm.arrive(buf, sem)
            add_rows(b, [b, buf])

        dst, sem = self.passing(side, d - 1)
        comm.step([], [(b, dst, sem, at.device(z + side, at.y, at.x, k))])

    def steps(self, produce=None):
        nz = self.comm.at.nz
        for i in range(nz + 2):
            if i < nz:
                if produce is not None:
                    produce(self.targets[i][2])
                self.first(i)
            yield
            for stage, lag in ((self.second, 1), (self.third, 2)):
                if 0 <= i - lag < nz:
                    stage(i - lag)
                    yield


def scatter_bufs(nz, rows, width):
    return [pltpu.VMEM((n * nz, rows, width), bf16) for n in (2, 1, 2)]


def along(ref, axis, i, size):
    r = pl.ds(pl.multiple_of(i * size, size), size)
    before = (slice(None),) * (len(ref.shape) - axis)
    return ref.at[before + (r,) + (slice(None),) * (axis - 1)]


class Swap:
    def __init__(self, array, unit_axis, feature_axis, units, depth, shape, plane=None, groups=1):
        self.array, self.shape, self.plane = array, shape, plane
        self.unit_axis, self.feature_axis, self.units, self.depth = unit_axis, feature_axis, units, depth
        self.groups = groups if feature_axis == 2 else 1
        self.out = jax.ShapeDtypeStruct(shape, bf16)

    def of_units(self, ref, z):
        if self.plane is not None:
            ref = ref.at[self.plane]
        return along(ref, self.unit_axis, z, self.units)

    def of_features(self, ref, z, y):
        return along(ref, self.feature_axis, 2 * z + y, self.depth)

    def runs(self, ref, nz, z, y):
        if self.groups == 1:
            return [self.of_features(ref, z, y)]
        r = self.depth // self.groups
        return [along(ref, 2, i * 2 * nz + 2 * z + y, r) for i in range(self.groups)]

    def cuts(self, piece):
        if self.groups == 1:
            return [piece]
        r = self.depth // self.groups
        return [along(piece, 2, i, r) for i in range(self.groups)]


def swap_in(comm, one, src, dst):
    at = comm.at
    z, y, x, k, nz = at.z, at.y, at.x, at.k, at.nz
    sem_z = [comm.sems(one.groups) for _ in range(nz)]
    sem_y = [comm.sems(one.groups) for _ in range(nz)]
    moved = []

    def sends():
        mine = one.runs(dst, nz, z, y)
        for d in range(1, nz):
            zi = (z + d) % nz
            parts = one.cuts(one.of_units(src, zi))
            for part, to, sem in zip(parts, mine, sem_z[d]):
                comm.step([], [(part, to, sem, at.device(zi, y, x, k))])
            yield
        for part, to, sem in zip(one.cuts(one.of_units(src, z)), mine, sem_y[0]):
            comm.step([], [(part, to, sem, comm.to_y)])
            moved.append(comm.move(part, to))
        yield

    def passes():
        for d in range(1, nz):
            for run, sem, on in zip(one.runs(dst, nz, (z + nz - d) % nz, y), sem_z[d], sem_y[d]):
                comm.step([(run, sem)], [(run, run, on, comm.to_y)])
            yield

    def arrivals():
        for d in range(nz):
            for run, sem in zip(one.runs(dst, nz, (z + nz - d) % nz, 1 - y), sem_y[d]):
                comm.arrive(run, sem)
        for wait in moved:
            wait()

    return sends(), passes(), arrivals


def add_piece(dst, src):
    if len(dst.shape) == 3:
        for p in range(dst.shape[0]):
            add_rows(dst.at[p], [dst.at[p], src.at[p]])
    else:
        add_rows(dst, [dst, src])


def swap_out_y(comm, one, src, landed):
    at = comm.at
    z, y, nz = at.z, at.y, at.nz
    order = list(range(1, nz)) + [0]
    sems = comm.sems(nz)

    def sends():
        for d in order:
            zi = (z + d) % nz
            comm.step([], [(one.of_features(src, zi, 1 - y), landed.at[zi], sems[d], comm.to_y)])
            yield

    def sums():
        for d in order:
            zi = (z + d) % nz
            comm.arrive(landed.at[zi], sems[d])
            add_piece(landed.at[zi], one.of_features(src, zi, y))
            yield

    return sends(), sums()


def swap_out_z(comm, one, summed, dst):
    at = comm.at
    z, y, x, k, nz = at.z, at.y, at.x, at.k, at.nz
    mine = one.of_units(dst, z)
    sems = comm.sems(nz)
    for d in list(range(1, nz)) + [0]:
        zi = (z + d) % nz
        if d:
            comm.step([], [(summed.at[zi], mine, sems[d], at.device(zi, y, x, k))])
            comm.late.append((one.of_units(dst, (z + nz - d) % nz), sems[d]))
        else:
            comm.keep(summed.at[zi], mine)
        yield


def paired(first, second):
    for _ in first:
        next(second, None)
        yield
    yield from second


def lagged(first, second, lag):
    n = 0
    for _ in first:
        n += 1
        if n > lag:
            next(second, None)
        yield
    yield from second


def chain(*many):
    for steps in many:
        yield from steps


def landing(nz, one, user_shape):
    shape = list(user_shape)
    shape[len(shape) - one.feature_axis] = one.depth
    return pltpu.VMEM((nz, *shape), bf16)


def comm_kernel(nz, groups, work, swaps, extra, n_in, n_out, *refs):
    given = [one for one in swaps if one.array is not None]
    m, g = len(swaps), len(given)
    ins, srcs = refs[:n_in], refs[n_in : n_in + g]
    outs = refs[n_in + g : n_in + g + n_out]
    dsts = refs[n_in + g + n_out : n_in + g + n_out + m]
    scratch = refs[n_in + g + n_out + m :]
    comm = Comm(Place(nz), scratch[-1], groups)
    work(comm, (swaps + extra, srcs, dsts), ins, outs, scratch[:-1])
    comm.finish()


def comm_call(name, nz, collective, work, ins, outs, scratch, swaps, swap_spec=ANY, vmem=48, groups=1, extra=()):
    given = [one.array for one in swaps if one.array is not None]
    return pl.pallas_call(
        functools.partial(comm_kernel, nz, groups, work, swaps, list(extra), len(ins), len(outs)),
        out_shape=[jax.ShapeDtypeStruct(s, d) for s, d, _ in outs] + [one.out for one in swaps],
        in_specs=[s for _, s in ins] + [swap_spec] * len(given),
        out_specs=[s for _, _, s in outs] + [ANY] * len(swaps),
        scratch_shapes=scratch + [DMA((700,))],
        compiler_params=pltpu.CompilerParams(
            collective_id=collective, has_side_effects=True, vmem_limit_bytes=vmem * 2**20
        ),
        name=name,
    )(*[v for v, _ in ins], *given)


def by_rows(lo, size, do):
    step = math.gcd(size, 16)

    def some_rows(i, _):
        do(pl.ds(pl.multiple_of(lo + i * step, step), step))
        return 0

    lax.fori_loop(0, size // step, some_rows, 0)


def two_parts(rows):
    return [(0, rows // 2), (rows // 2, rows // 2)]


def making_steps(nz):
    return 3 * nz - 5


def feature_pieces(nz, groups, d_model):
    a = 2 * nz
    r = d_model // a // groups
    return [(c, i * r, (i * a + c) * r, r) for c in range(a) for i in range(groups)]


def sum_gains(comm, groups, sums, sorted_sums, landed, total):
    at = comm.at
    z, y, x, k, nz = at.z, at.y, at.x, at.k, at.nz
    for c, lo, col, r in feature_pieces(nz, groups, sums.shape[1]):
        sorted_sums[c % 2, c // 2, :, lo : lo + r] = sums[:, col : col + r]
    sem = comm.sems(4 + nz)
    comm.step([], [(sorted_sums.at[1 - y], landed.at[pl.ds(0, nz)], sem[0], comm.to_y)])
    comm.arrive(landed.at[pl.ds(0, nz)], sem[0])
    sorted_sums[y] += landed[0:nz]
    for d in range(1, nz):
        zi = (z + d) % nz
        comm.step([], [(sorted_sums.at[y, zi], landed.at[nz + d], sem[d], at.device(zi, y, x, k))])
    total[...] = sorted_sums[y, z]
    for d in range(1, nz):
        comm.arrive(landed.at[nz + d], sem[d])
        total[...] += landed[nz + d]
    landed[nz] = total[...]
    for i, to in enumerate((comm.to_k, comm.to_x, comm.to_xk)):
        comm.step([], [(landed.at[nz], landed.at[2 * nz + i], sem[nz + i], to)])
    for i in range(3):
        comm.arrive(landed.at[2 * nz + i], sem[nz + i])
        total[...] += landed[2 * nz + i]


def gains_of_group(comm, groups, gain_ref, landed, gains):
    at = comm.at
    z, y, x, k, nz = at.z, at.y, at.x, at.k, at.nz
    sem = comm.sems(nz + 1)
    for d in range(1, nz):
        to = at.device((z + d) % nz, y, x, k)
        comm.step([], [(gain_ref, landed.at[y, z], sem[d], to)])
    landed[y, z] = gain_ref[...]
    yield
    for d in range(1, nz):
        comm.arrive(landed.at[y, (z + nz - d) % nz], sem[d])
    comm.step([], [(landed.at[y], landed.at[y], sem[0], comm.to_y)])
    comm.arrive(landed.at[1 - y], sem[0])
    for c, lo, col, r in feature_pieces(nz, groups, gains.shape[1]):
        gains[:, col : col + r] = landed[c % 2, c // 2, :, lo : lo + r].astype(f32)


def product_into(p_ref, rows, at_slot, lhs, rhs, rhs_dims):
    n = p_ref.shape[2]
    wide = math.gcd(n, 512)
    count = lhs[0].shape[0] // rows
    for j in range(n // wide):
        cols = slice(j * wide, (j + 1) * wide)
        total = None
        for one, right, dims in zip(lhs, rhs, rhs_dims):
            block = right[:, cols] if dims == 0 else right[cols, :]
            term = lax.dot_general(one, block, (((1,), (dims,)), ((), ())), preferred_element_type=f32)
            total = term if total is None else total + term
        p_ref[pl.ds(at_slot, count), :, cols] = total.astype(bf16).reshape(count, rows, wide)


def row_blocks(rows, keys, do):
    step = math.gcd(rows, 256)
    fine = max(16, min(128, 128 * 2048 // keys))
    for i in range(rows // step):

        def some(j, _):
            do(pl.ds(pl.multiple_of(i * step + j * fine, fine), fine))
            return 0

        lax.fori_loop(0, step // fine, some, 0)
        yield


def attend(heads, q_ref, k_ref, v_ref, at_q, at_k, o_ref, lse_ref):
    def block(r):
        visible = at_k[...] <= at_q[r, :]
        for h in range(heads):
            c = slice(h * HD, (h + 1) * HD)
            scores = lax.dot_general(
                q_ref[r, c], k_ref[:, c], (((1,), (1,)), ((), ())), preferred_element_type=f32
            )
            scores = jnp.where(visible, scores, -1e30)
            peak = jnp.max(scores, axis=-1, keepdims=True)
            weights = jnp.exp(scores - peak)
            total = jnp.sum(weights, axis=-1, keepdims=True)
            probs = (weights * (1.0 / total)).astype(bf16)
            o_ref[r, c] = jnp.dot(probs, v_ref[:, c], preferred_element_type=f32).astype(bf16)
            lse_ref[r, h : h + 1] = peak + jnp.log(total)

    yield from row_blocks(q_ref.shape[0], k_ref.shape[0], block)


def attend_back(heads, q_ref, k_ref, v_ref, at_q, at_k, o_ref, lse_ref, do_ref, dq_ref, dk_ref, dv_ref):
    over_rows = (((0,), (0,)), ((), ()))
    over_cols = (((1,), (1,)), ((), ()))
    dk_ref[...] = jnp.zeros_like(dk_ref)
    dv_ref[...] = jnp.zeros_like(dv_ref)

    def block(r):
        visible = at_k[...] <= at_q[r, :]
        for h in range(heads):
            c = slice(h * HD, (h + 1) * HD)
            q, grad = q_ref[r, c], do_ref[r, c]
            scores = lax.dot_general(q, k_ref[:, c], over_cols, preferred_element_type=f32)
            scores = jnp.where(visible, scores, -1e30)
            probs = jnp.exp(scores - lse_ref[r, h : h + 1])
            delta = jnp.sum(
                grad.astype(f32) * o_ref[r, c].astype(f32), axis=-1, keepdims=True
            )
            prob_grad = lax.dot_general(grad, v_ref[:, c], over_cols, preferred_element_type=f32)
            score_grad = (probs * (prob_grad - delta)).astype(bf16)
            dq_ref[r, c] = jnp.dot(score_grad, k_ref[:, c], preferred_element_type=f32) * HD ** (-0.5)
            dk_ref[c, :] += lax.dot_general(q, score_grad, over_rows, preferred_element_type=f32)
            dv_ref[c, :] += lax.dot_general(
                grad, probs.astype(bf16), over_rows, preferred_element_type=f32
            )

    yield from row_blocks(q_ref.shape[0], k_ref.shape[0], block)


def other_halves(u):
    width = u.shape[1]
    low = lax.broadcasted_iota(jnp.int32, (1, width), 1) % HD < HD // 2
    return jnp.where(low, pltpu.roll(u, width - HD // 2, 1), pltpu.roll(u, HD // 2, 1))


def forward_work(heads, groups, comm, swap, ins, outs, scratch):
    x_ref, gain_ref, cos, sin, at_q, at_k = ins
    gains, q_ref, o_ref, lse_ref, hidden, rows_attn, k_out, v_out, rows_mlp = outs
    normed, landed, rows_v, qkv_v, out_v, k_all, v_all, p_ref = scratch[:8]
    bufs = scratch[8:]
    swaps, srcs, dsts = swap
    at = comm.at
    y, nz = at.y, at.nz
    rows, d_model = x_ref.shape
    tall = 4 * rows
    keys = q_ref.shape[0]
    width = q_ref.shape[1]

    places = (qkv_v, out_v) + tuple(dsts[2:])
    qkv, out, down, gate, up = [swap_in(comm, *v) for v in zip(swaps, srcs, places)]
    gaining = gains_of_group(comm, groups, gain_ref, landed, gains)
    advance(gaining, 1)
    advance(qkv[0], nz - 1)
    exhaust(gaining, qkv[0])

    def norm_1(r):
        x = x_ref[r, :].astype(f32)
        normed[r, :] = (x * inv_rms(x) * gains[0:1, :]).astype(bf16)

    by_rows(0, rows, norm_1)
    shards = gather_steps(comm, normed, rows_v, 0, rows)
    advance(shards, z_steps(at))
    take_turns(shards, chain(out[0], qkv[1], down[0]))
    qkv[2]()
    comm.keep(qkv_v, dsts[0])
    comm.keep(rows_v, rows_attn)

    def half(ref, g, yy):
        return ref.at[pl.ds(pl.multiple_of((yy * groups + g) * keys, keys), keys), :]

    group = at.first // (2 * nz)
    mine = [half(ref, group, y) for ref in (k_all, v_all)]

    def project(i, _):
        r = pl.ds(pl.multiple_of(i * tall, tall), tall)
        block = rows_v[r, :]

        def turned(p):
            u = jnp.dot(block, qkv_v[p], preferred_element_type=f32)
            return (u * cos[r, :] + other_halves(u) * sin[r, :]).astype(bf16)

        q_ref[r, :] = turned(0) * jnp.asarray(HD ** (-0.5), bf16)
        mine[0][r, :] = turned(1)
        mine[1][r, :] = jnp.dot(block, qkv_v[2], preferred_element_type=f32).astype(bf16)
        return 0

    lax.fori_loop(0, nz, project, 0)
    sem = comm.sems(4 * groups)
    for i, ref in enumerate(mine):
        comm.step([], [(ref, ref, sem[i], comm.to_y)])
        for g, f, device in comm.afar:
            comm.step([], [(ref, ref, sem[2 + (2 * g + f) * 2 + i - 2], device)])
    exhaust(gate[0], out[1])
    out[2]()
    comm.keep(out_v, dsts[1])
    for i, (ref, dst) in enumerate(((k_all, k_out), (v_all, v_out))):
        comm.arrive(half(ref, group, 1 - y), sem[i])
        for g, f, device in comm.afar:
            come = half(ref, (group + groups - g) % groups, y + f * (1 - 2 * y))
            comm.arrive(come, sem[2 + (2 * g + f) * 2 + i - 2])
        comm.keep(ref, dst)
    take_turns(
        attend(heads, q_ref, k_all, v_all, at_q, at_k, o_ref, lse_ref), chain(down[1], up[0], gate[1])
    )

    def norm_2(r):
        h = hidden[r, :] + x_ref[r, :].astype(f32)
        hidden[r, :] = h
        normed_2[r, :] = (h * inv_rms(h) * gains[1:2, :]).astype(bf16)

    def produce(zi):
        r = pl.ds(pl.multiple_of(zi * tall, tall), tall)
        product_into(p_ref, rows, zi * 4, [o_ref[r, :]], [out_v], [0])

    normed_2, total = bufs[3], bufs[4]

    def part(lo, size, making):
        yield from Scatter(comm, p_ref, bufs[:3], total, lo, size).steps(making)
        r = pl.ds(lo, size)
        for c, piece, col, n in feature_pieces(nz, groups, d_model) if groups > 1 else [(0, 0, 0, d_model)]:
            frm = c * (d_model // (2 * nz)) + piece
            hidden[r, col : col + n] = total[r, frm : frm + n]
        by_rows(lo, size, norm_2)
        yield
        yield from gather_steps(comm, normed_2, rows_mlp, lo, size)

    front, rear = [part(lo, size, None if lo else produce) for lo, size in two_parts(rows)]
    advance(front, making_steps(nz))
    take_turns(lagged(front, rear, 1), up[1])
    for one in (down, gate, up):
        one[2]()


def norm_back(grad, unit, rms, gain):
    unit_grad = grad * gain
    return rms * (unit_grad - unit * jnp.mean(unit_grad * unit, axis=-1, keepdims=True))


def back_work(groups, comm, swap, ins, outs, scratch):
    rows_mlp, gate_hbm, up_hbm, dn_hbm, hidden, dy_ref, gains = ins
    residual, branch_rows, gain_sum, block_out, gate_out, up_out = outs
    total, rounded, p_ref, q_ref, pre, gates, n2, dy, gate_g, up_g, dn_g, dn_landed, gate_landed = scratch[:13]
    bufs, bufs_q, total_q, gate_w, up_w, dn_w = scratch[13:16], scratch[16:19], *scratch[19:]
    (down, gate_swap), _, dsts = swap
    at = comm.at
    nz = at.nz
    rows = hidden.shape[0]
    tall = 4 * rows
    gain_sum[...] = jnp.zeros_like(gain_sum)
    weights_here = [
        comm.move(src, dst) for src, dst in ((gate_hbm, gate_w), (up_hbm, up_w), (dn_hbm, dn_w))
    ]
    sems = comm.sems(nz)

    def load(t, zi):
        r = pl.ds(pl.multiple_of(zi * tall, tall), tall)
        return pltpu.make_async_copy(rows_mlp.at[r, :], n2.at[r, :], sems[t])

    for t, target in enumerate(far_first(at)):
        load(t, target[2]).start()
    turn = iter(range(nz))

    def forward(zi):
        load(next(turn), zi).wait()
        r = pl.ds(pl.multiple_of(zi * tall, tall), tall)
        x = n2[r, :]
        gate = jnp.dot(x, gate_w[...], preferred_element_type=f32)
        up = jnp.dot(x, up_w[...], preferred_element_type=f32)
        pre[0, r, :] = gate
        pre[1, r, :] = up
        hid = (gate * jax.nn.sigmoid(gate) * up).astype(bf16)
        gates[2, r, :] = hid
        product_into(q_ref, rows, zi * 4, [hid], [dn_w], [0])

    def backward(zi):
        r = pl.ds(pl.multiple_of(zi * tall, tall), tall)
        grad = lax.dot_general(
            dy[r, :], dn_w[...], (((1,), (1,)), ((), ())), preferred_element_type=f32
        )
        gate, up = pre[0, r, :], pre[1, r, :]
        sig = jax.nn.sigmoid(gate)
        gate_grad = (grad * up * (sig * (1.0 + gate * (1.0 - sig)))).astype(bf16)
        up_grad = (grad * (gate * sig)).astype(bf16)
        gates[0, r, :] = gate_grad
        gates[1, r, :] = up_grad
        product_into(p_ref, rows, zi * 4, [gate_grad, up_grad], [gate_w, up_w], [1, 1])

    def back(r):
        h = hidden[r, :]
        rms = inv_rms(h)
        unit, grad = h * rms, total[r, :]
        gain_sum[...] += jnp.sum(grad * unit, axis=0, keepdims=True)
        dh = dy_ref[r, :].astype(f32) + norm_back(grad, unit, rms, gains[1:2, :])
        residual[r, :] = dh
        rounded[r, :] = dh.astype(bf16)

    def out(r):
        block_out[r, :] = (hidden[r, :] + total_q[r, :]).astype(bf16)

    def gradients(which):
        d_model = n2.shape[1]
        depth = d_model // (2 * nz)
        over_rows = (((0,), (0,)), ((), ()))
        pieces = feature_pieces(nz, groups, d_model)
        per = max(1, len(pieces) // 4)
        for j in range(0, len(pieces), per):
            for c, lo, col, r in pieces[j : j + per]:
                f, to = slice(col, col + r), slice(c * depth + lo, c * depth + lo + r)
                if which == 2:
                    dn_g[:, to] = lax.dot_general(
                        gates[2], dy[:, f], over_rows, preferred_element_type=f32
                    ).astype(bf16)
                else:
                    (gate_g, up_g)[which][to, :] = lax.dot_general(
                        n2[:, f], gates[which], over_rows, preferred_element_type=f32
                    ).astype(bf16)
            yield

    def output():
        yield from Scatter(comm, q_ref, bufs_q, total_q, 0, rows).steps(forward)
        by_rows(0, rows, out)

    def part(lo, size, making):
        yield from Scatter(comm, p_ref, bufs, total, lo, size).steps(making)
        by_rows(lo, size, back)
        yield
        yield from gather_steps(comm, rounded, branch_rows, lo, size)

    shards = gather_steps(comm, dy_ref, dy, 0, rows)
    side = output()
    advance(shards, 1)
    for here in weights_here:
        here()
    for _ in range(making_steps(nz)):
        next(side)
        advance(shards, 1)
    for _ in shards:
        next(side, None)
    front, rear = [part(lo, size, None if lo else backward) for lo, size in two_parts(rows)]
    for _ in range(making_steps(nz)):
        next(front)
        advance(side, 1)
    down_sends, down_sums = swap_out_y(comm, down, dn_g, dn_landed)
    gate_sends, gate_sums = swap_out_y(comm, gate_swap, gate_g, gate_landed)

    def weights():
        yield from gradients(2)
        yield from down_sends
        yield from gradients(0)
        yield from gate_sends
        yield from gradients(1)
        comm.keep(up_g, up_out)
        yield from paired(down_sums, swap_out_z(comm, down, dn_landed, dsts[0]))
        yield from gate_sums

    take_turns(lagged(front, rear, 1), side, weights())
    comm.keep(gate_landed, gate_out)


def tail_work(heads, groups, comm, swap, ins, outs, scratch):
    (q_ref, k_ref, v_ref, at_q, at_k, o_ref, lse_ref, branch_rows, out_w, gate_sum, up_grad,
     rows_attn, cos, sin, qkv_w, residual, x_ref, gains, gain_sum_2) = ins
    grad_in, gain_out = outs
    (dq_ref, dk_ref, dv_ref, going, come, up_landed, out_landed, q_landed, kv_landed, proj, n1,
     q_g, kv_g, total, gain_sums, sorted_sums, landed, p_ref, dh, do_ref, out_g) = scratch[:21]
    bufs = scratch[21:]
    (gate, up, out, q_swap, kv_swap), _, dsts = swap
    dh_here = comm.move(branch_rows, dh)
    n1_here = comm.move(rows_attn, n1)
    at = comm.at
    y, nz = at.y, at.nz
    keys, width = q_ref.shape
    rows, d_model = x_ref.shape
    tall = 4 * rows
    gain_sums[0:1, :] = jnp.zeros_like(gain_sum_2)
    gain_sums[1:2, :] = gain_sum_2[...]

    up_sends, up_sums = swap_out_y(comm, up, up_grad, up_landed)
    exhaust(up_sends, swap_out_z(comm, gate, gate_sum, dsts[0]))
    depth = d_model // (2 * nz)
    pieces = feature_pieces(nz, groups, d_model)
    dh_here()

    def attention_grads(i, _):
        r = pl.ds(pl.multiple_of(i * tall, tall), tall)
        do_ref[r, :] = lax.dot_general(
            dh[r, :], out_w[...], (((1,), (1,)), ((), ())), preferred_element_type=f32
        ).astype(bf16)
        return 0

    lax.fori_loop(0, nz, attention_grads, 0)
    for c, lo, col, n in pieces:
        out_g[:, c * depth + lo : c * depth + lo + n] = lax.dot_general(
            o_ref[...], dh[:, col : col + n], (((0,), (0,)), ((), ())), preferred_element_type=f32
        ).astype(bf16)
    out_sends, out_sums = swap_out_y(comm, out, out_g, out_landed)
    exhaust(out_sends)
    more = chain(
        paired(up_sums, swap_out_z(comm, up, up_landed, dsts[1])),
        paired(out_sums, swap_out_z(comm, out, out_landed, dsts[2])),
    )
    compute = attend_back(
        heads, q_ref, k_ref, v_ref, at_q, at_k, o_ref, lse_ref, do_ref, dq_ref, dk_ref, dv_ref
    )
    take_turns(compute, more)

    group = at.first // (2 * nz)

    def share(ref, g, yy):
        return ref.at[:, pl.ds(pl.multiple_of((yy * groups + g) * keys, keys), keys)]

    others = [(0, 1, comm.to_y)] + comm.afar
    sem = comm.sems(2 * len(others))
    for j, (g, f, device) in enumerate(others):
        for i, ref in enumerate((dk_ref, dv_ref)):
            theirs = share(ref, (group + g) % groups, y + f * (1 - 2 * y))
            going[j, i] = theirs[...].astype(bf16)
            comm.step([], [(going.at[j, i], come.at[j, i], sem[2 * j + i], device)])

    def unturned(u, r):
        return (u * cos[r, :] - other_halves(u) * sin[r, :]).astype(bf16)

    every = pl.ds(0, keys)
    proj[:, 0:width] = unturned(dq_ref[...], every)

    def product(col, n, cols):
        return lax.dot_general(
            n1[:, col : col + n], proj[:, cols], (((0,), (0,)), ((), ())),
            preferred_element_type=f32,
        ).astype(bf16)

    n1_here()
    for c, lo, col, n in pieces:
        q_g[c * depth + lo : c * depth + lo + n, :] = product(col, n, slice(0, width))
    q_sends, q_sums = swap_out_y(comm, q_swap, q_g, q_landed)
    exhaust(q_sends)
    for i, ref in enumerate((dk_ref, dv_ref)):
        grad = share(ref, group, y)[...]
        for j in range(len(others)):
            comm.arrive(come.at[j, i], sem[2 * j + i])
            grad = grad + come[j, i].astype(f32)
        grad = grad.T
        cols = slice((i + 1) * width, (i + 2) * width)
        proj[:, cols] = unturned(grad, every) if i == 0 else grad.astype(bf16)

    def back(r):
        x = x_ref[r, :].astype(f32)
        rms = inv_rms(x)
        unit, grad = x * rms, total[r, :]
        gain_sums[0:1, :] += jnp.sum(grad * unit, axis=0, keepdims=True)
        grad_in[r, :] = residual[r, :] + norm_back(grad, unit, rms, gains[0:1, :])

    def produce(zi):
        r = pl.ds(pl.multiple_of(zi * tall, tall), tall)
        lhs = [proj[r, p * width : (p + 1) * width] for p in range(3)]
        product_into(p_ref, rows, zi * 4, lhs, [qkv_w.at[p] for p in range(3)], [1] * 3)

    kv_sends, kv_sums = swap_out_y(comm, kv_swap, kv_g, kv_landed)

    def weights():
        per = max(1, len(pieces) // 4)
        for j in range(0, len(pieces), per):
            for c, lo, col, n in pieces[j : j + per]:
                grad = product(col, n, slice(width, 3 * width))
                for p in (0, 1):
                    kv_g[p, c * depth + lo : c * depth + lo + n, :] = grad[:, p * width : (p + 1) * width]
            yield
        yield from kv_sends
        yield from paired(q_sums, swap_out_z(comm, q_swap, q_landed, dsts[3]))
        yield from paired(kv_sums, swap_out_z(comm, kv_swap, kv_landed, dsts[4]))

    steps = Scatter(comm, p_ref, bufs, total, 0, rows).steps(produce)
    advance(steps, making_steps(nz))
    take_turns(weights(), steps)
    by_rows(0, rows, back)
    sum_gains(comm, groups, gain_sums, sorted_sums, landed, gain_out)


def body(
    block_input,
    qkv_weight,
    out_weight,
    gate_up_weight,
    down_weight,
    norm_gains,
    positions,
    layer_output_gradient,
):
    n_ctx, n_tp = lax.axis_size("ctx"), lax.axis_size("tp")
    nz = math.gcd(qkv_weight.shape[2] // HD, n_ctx // 2)
    nz = math.gcd(nz, 4)
    a = 2 * nz
    b = n_ctx // a
    assert n_tp == 4
    depth = qkv_weight.shape[1] * b
    d_model = depth * a
    width = qkv_weight.shape[2] // nz
    heads = width // HD
    units = down_weight.shape[0] // nz
    rows = block_input.shape[0]
    across = [[i * a + j for i in range(b)] for j in range(a)]

    def over_groups(v, axis):
        return lax.all_gather(v, "ctx", axis=axis, tiled=True, axis_index_groups=across) if b > 1 else v

    def to_groups(v, axis):
        if b == 1:
            return v
        return lax.psum_scatter(
            v, "ctx", scatter_dimension=axis, tiled=True, axis_index_groups=across
        )

    def model_order(v, axis):
        if b == 1:
            return v
        s = v.shape
        w = v.reshape(s[:axis] + (a, b, depth // b) + s[axis + 1 :])
        return jnp.swapaxes(w, axis, axis + 1).reshape(s)

    my_gains = over_groups(norm_gains, 1)
    group_rows = 4 * nz * rows
    n_keys = 2 * b * group_rows
    y, group = lax.axis_index("ctx") % 2, lax.axis_index("ctx") // a
    by_place = positions.reshape(b, nz, 2, n_tp * rows)
    key_pos = by_place.transpose(2, 0, 1, 3).reshape(2 * b, group_rows)
    own_pos = lax.dynamic_index_in_dim(key_pos, y * b + group, 0, keepdims=False)
    cos_tab, sin_tab = rope_tables(own_pos, HD)
    cos_wide = jnp.tile(cos_tab[:, 0, :], (1, 2 * heads))
    sin_wide = jnp.tile(jnp.concatenate([-sin_tab, sin_tab], axis=-1)[:, 0, :], (1, heads))
    places = [(own_pos[:, None], VMEM), (key_pos.reshape(1, -1), VMEM)]
    gu_all = over_groups(gate_up_weight, 1)
    partials = pltpu.VMEM((4 * nz, rows, d_model), bf16)
    (gains, query_bf, attn_bf, log_total, hidden, rows_attn, key_all, value_all, rows_mlp,
     qkv_w, out_w, dn_w, gate_w, up_w) = comm_call(
        "forward", nz, 0, functools.partial(forward_work, heads, b),
        [(block_input, VMEM), (my_gains, VMEM), (cos_wide, VMEM), (sin_wide, VMEM)] + places,
        [((2, d_model), f32, VMEM), ((group_rows, width), bf16, VMEM),
         ((group_rows, width), bf16, VMEM), ((group_rows, heads), f32, VMEM),
         ((rows, d_model), f32, VMEM), ((group_rows, d_model), bf16, ANY),
         ((n_keys, width), bf16, ANY), ((n_keys, width), bf16, ANY),
         ((group_rows, d_model), bf16, ANY)],
        [pltpu.VMEM((rows, d_model), bf16), pltpu.VMEM((2, nz) + my_gains.shape, bf16),
         pltpu.VMEM((group_rows, d_model), bf16), pltpu.VMEM((3, d_model, width), bf16),
         pltpu.VMEM((width, d_model), bf16), pltpu.VMEM((n_keys, width), bf16),
         pltpu.VMEM((n_keys, width), bf16), partials]
        + scatter_bufs(nz, rows, d_model)
        + [pltpu.VMEM((rows, d_model), bf16), pltpu.VMEM((rows, d_model), f32)],
        [Swap(over_groups(qkv_weight, 1), 1, 2, width, depth, (3, d_model, width), None, b),
         Swap(over_groups(out_weight, 1), 2, 1, width, depth, (width, d_model)),
         Swap(over_groups(down_weight, 1), 2, 1, units, depth, (units, d_model))]
        + [Swap(gu_all, 1, 2, units, depth, (d_model, units), p, b) for p in (0, 1)],
        groups=b,
    )
    out_w, dn_w = model_order(out_w, 1), model_order(dn_w, 1)
    down_swap = Swap(None, 2, 1, units, depth, (nz * units, depth))
    half_swap = Swap(None, 1, 2, units, depth, (depth, nz * units))
    residual_grad, branch_rows, gain_sum_2, block_output, gate_sum, up_grad, dn_back = comm_call(
        "back", nz, 3, functools.partial(back_work, b),
        [(rows_mlp, ANY), (gate_w, ANY), (up_w, ANY), (dn_w, ANY),
         (hidden, VMEM), (layer_output_gradient, VMEM), (gains, VMEM)],
        [((rows, d_model), f32, VMEM), ((group_rows, d_model), bf16, ANY),
         ((1, d_model), f32, VMEM), ((rows, d_model), bf16, VMEM),
         ((nz, depth, units), bf16, ANY), ((d_model, units), bf16, ANY)],
        [pltpu.VMEM((rows, d_model), f32), pltpu.VMEM((rows, d_model), bf16), partials, partials,
         pltpu.VMEM((2, group_rows, units), f32), pltpu.VMEM((3, group_rows, units), bf16),
         pltpu.VMEM((group_rows, d_model), bf16), pltpu.VMEM((group_rows, d_model), bf16),
         pltpu.VMEM((d_model, units), bf16), pltpu.VMEM((d_model, units), bf16),
         pltpu.VMEM((units, d_model), bf16),
         landing(nz, down_swap, (units, d_model)), landing(nz, half_swap, (d_model, units))]
        + scatter_bufs(nz, rows, d_model) + scatter_bufs(nz, rows, d_model)
        + [pltpu.VMEM((rows, d_model), f32), pltpu.VMEM((d_model, units), bf16),
           pltpu.VMEM((d_model, units), bf16), pltpu.VMEM((units, d_model), bf16)],
        [down_swap],
        vmem=60,
        extra=[half_swap],
    )
    out_swap = Swap(None, 2, 1, width, depth, (nz * width, depth))
    q_swap = Swap(None, 1, 2, width, depth, (depth, nz * width))
    kv_swap = Swap(None, 1, 2, width, depth, (2, depth, nz * width))
    others = 2 * b - 1
    layer_input_gradient, gain_sums, gate_back, up_back, out_back, q_back, kv_back = comm_call(
        "tail", nz, 4, functools.partial(tail_work, heads, b),
        [(query_bf, VMEM), (key_all, VMEM), (value_all, VMEM)] + places
        + [(attn_bf, VMEM), (log_total, VMEM), (branch_rows, ANY), (out_w, VMEM), (gate_sum, VMEM),
           (up_grad, VMEM),
           (rows_attn, ANY), (cos_wide, VMEM), (sin_wide, VMEM), (qkv_w, VMEM),
           (residual_grad, VMEM), (block_input, VMEM), (gains, VMEM), (gain_sum_2, VMEM)],
        [((rows, d_model), f32, VMEM), ((2, depth), f32, VMEM)],
        [pltpu.VMEM((group_rows, width), f32),
         pltpu.VMEM((width, n_keys), f32), pltpu.VMEM((width, n_keys), f32),
         pltpu.VMEM((others, 2, width, group_rows), bf16),
         pltpu.VMEM((others, 2, width, group_rows), bf16),
         landing(nz, half_swap, (d_model, units)), landing(nz, out_swap, (width, d_model)),
         landing(nz, q_swap, (d_model, width)), landing(nz, kv_swap, (2, d_model, width)),
         pltpu.VMEM((group_rows, 3 * width), bf16), pltpu.VMEM((group_rows, d_model), bf16),
         pltpu.VMEM((d_model, width), bf16), pltpu.VMEM((2, d_model, width), bf16),
         pltpu.VMEM((rows, d_model), f32), pltpu.VMEM((2, d_model), f32),
         pltpu.VMEM((2, nz, 2, depth), f32), pltpu.VMEM((2 * nz + 3, 2, depth), f32), partials,
         pltpu.VMEM((group_rows, d_model), bf16), pltpu.VMEM((group_rows, width), bf16),
         pltpu.VMEM((width, d_model), bf16)]
        + scatter_bufs(nz, rows, d_model),
        [half_swap, half_swap, out_swap, q_swap, kv_swap],
        vmem=63,
        groups=b,
    )
    gu_back = jnp.stack([gate_back, up_back])
    qkv_back = jnp.concatenate([q_back[None], kv_back])
    if b > 1:
        gain_sums = lax.psum(gain_sums, "ctx", axis_index_groups=across)
    gain_cols = d_model // (n_ctx * n_tp)
    gain_part = lax.dynamic_slice_in_dim(
        gain_sums, (group * n_tp + lax.axis_index("tp")) * gain_cols, gain_cols, 1
    )
    return (
        block_output,
        layer_input_gradient,
        to_groups(qkv_back, 1).astype(f32),
        to_groups(out_back, 1).astype(f32),
        to_groups(gu_back, 1).astype(f32),
        to_groups(dn_back, 1).astype(f32),
        gain_part,
    )


def solution(mesh):
    placed = (
        P(("ctx", "tp"), None),
        P(None, "ctx", "tp"),
        P("tp", "ctx"),
        P(None, "ctx", "tp"),
        P("tp", "ctx"),
        P(None, "ctx"),
        P(),
        P(("ctx", "tp"), None),
    )
    return jax.shard_map(
        body,
        mesh=mesh,
        in_specs=placed,
        out_specs=(
            P(("ctx", "tp"), None),
            P(("ctx", "tp"), None),
            P(None, "ctx", "tp"),
            P("tp", "ctx"),
            P(None, "ctx", "tp"),
            P("tp", "ctx"),
            P(None, ("ctx", "tp")),
        ),
        check_vma=False,
    )
```

```python
import functools
import math

import jax
import jax.numpy as jnp
from jax import lax
from jax.experimental import pallas as pl
from jax.experimental.pallas import tpu as pltpu
from jax.sharding import PartitionSpec as P

HD = 64
MESH = pl.DeviceIdType.MESH
DMA = pltpu.SemaphoreType.DMA
ANY = pl.BlockSpec(memory_space=pl.ANY)
VMEM = pl.BlockSpec(memory_space=pltpu.VMEM)
bf16 = jnp.bfloat16
f32 = jnp.float32

norm_eps = 1e-05
rope_base = 130000.0


def inv_rms(values):
    return lax.rsqrt(jnp.mean(values * values, axis=-1, keepdims=True) + norm_eps)


def rope_tables(where_at, head_dim):
    half_dim = head_dim // 2
    inv_freq = rope_base ** (-(jnp.arange(half_dim, dtype=f32) * 2.0 / head_dim))
    angles = where_at.astype(f32)[:, None] * inv_freq[None, :]
    return (jnp.cos(angles)[:, None, :], jnp.sin(angles)[:, None, :])


def rotate(values, cos_tab, sin_tab, n_heads, head_dim):
    shaped = values.reshape(values.shape[0], n_heads, head_dim)
    half_dim = head_dim // 2
    lower_half, upper_half = (shaped[..., :half_dim], shaped[..., half_dim:])
    turned = jnp.concatenate(
        [lower_half * cos_tab - upper_half * sin_tab, upper_half * cos_tab + lower_half * sin_tab],
        axis=-1,
    )
    return turned.reshape(values.shape[0], n_heads * head_dim)


def unrotate(values, cos_tab, sin_tab, n_heads, head_dim):
    return rotate(values, cos_tab, -sin_tab, n_heads, head_dim)


class Place:
    def __init__(self, nz):
        ctx, tp = lax.axis_index("ctx"), lax.axis_index("tp")
        self.nz = nz
        self.first = ctx // (2 * nz) * (2 * nz)
        self.z, self.y = (ctx - self.first) // 2, (ctx - self.first) % 2
        self.x, self.k = tp // 2, tp % 2

    def device(self, z, y, x, k):
        return {"ctx": self.first + 2 * z + y, "tp": 2 * x + k}

    def elsewhere(self, g, flip):
        n = lax.axis_size("ctx")
        y = self.y + flip * (1 - 2 * self.y)
        return {"ctx": (self.first + g * 2 * self.nz) % n + 2 * self.z + y}


def slot_of(z, x, k):
    return (z * 2 + x) * 2 + k


class Comm:
    def __init__(self, at, pool, groups=1):
        self.at, self.pool, self.used, self.ends, self.late = at, pool, 0, [], []
        z, y, x, k, nz = at.z, at.y, at.x, at.k, at.nz
        self.to_x = at.device(z, y, 1 - x, k)
        self.to_k = at.device(z, y, x, 1 - k)
        self.to_y = at.device(z, 1 - y, x, k)
        self.to_xk = at.device(z, y, 1 - x, 1 - k)
        peers = [self.to_x, self.to_k, self.to_y, self.to_xk]
        self.afar = [(g, f, at.elsewhere(g, f)) for g in range(1, groups) for f in (0, 1)]
        peers += [device for _, _, device in self.afar]
        peers += [at.device((z + d) % nz, y, x, k) for d in range(1, nz)]
        barrier = pltpu.get_barrier_semaphore()
        for peer in peers:
            pl.semaphore_signal(barrier, inc=1, device_id=peer, device_id_type=MESH)
        pl.semaphore_wait(barrier, len(peers))

    def sem(self):
        self.used += 1
        return self.pool.at[self.used - 1]

    def sems(self, n):
        return [self.sem() for _ in range(n)]

    def step(self, arrivals, copies, cond=None, then=None):
        sems = self.sems(len(copies))

        def copy(i):
            src, dst, recv_sem, device = copies[i]
            return pltpu.make_async_remote_copy(
                src_ref=src,
                dst_ref=dst,
                send_sem=sems[i],
                recv_sem=recv_sem,
                device_id=device,
                device_id_type=MESH,
            )

        def go():
            for buf, sem in arrivals:
                self.arrive(buf, sem)
            if then is not None:
                then()
            for i in range(len(copies)):
                copy(i).start()

        def end():
            for i in range(len(copies)):
                copy(i).wait_send()

        if cond is None:
            go()
        else:
            pl.when(cond)(go)
        if copies:
            self.ends.append((cond, end))

    def move(self, src, dst):
        copy = pltpu.make_async_copy(src, dst, self.sem())
        copy.start()
        return copy.wait

    def keep(self, src, dst):
        self.ends.append((None, self.move(src, dst)))

    def arrive(self, buf, recv_sem):
        pltpu.make_async_remote_copy(
            src_ref=buf,
            dst_ref=buf,
            send_sem=recv_sem,
            recv_sem=recv_sem,
            device_id=self.to_k,
            device_id_type=MESH,
        ).wait_recv()

    def finish(self):
        for buf, sem in self.late:
            self.arrive(buf, sem)
        for cond, end in self.ends:
            if cond is None:
                end()
            else:
                pl.when(cond)(end)


def take_turns(*steps):
    steps = list(steps)
    while steps:
        for one in list(steps):
            if next(one, steps) is steps:
                steps.remove(one)


def advance(steps, n):
    for _ in range(n):
        next(steps, None)


def exhaust(*many):
    for steps in many:
        for _ in steps:
            pass


def line(at):
    places = []
    for d in range(1, at.nz):
        places.append((d, -1, (at.z + at.nz - d) % at.nz, at.z >= d))
        places.append((d, 1, (at.z + d) % at.nz, at.z + d < at.nz))
    return places


def z_steps(at):
    return 2 * at.nz - 1


def gather_steps(comm, own, o_ref, lo, size):
    at = comm.at
    z, x, k, nz = at.z, at.x, at.k, at.nz
    rows = own.shape[0]
    places = [(0, 0, z, None)] + line(at)
    n = len(places)
    sem_z, sem_x, sem_k = (comm.sems(m * n) for m in (1, 1, 2))

    def part(slot):
        return o_ref.at[pl.ds(pl.multiple_of(slot * rows + lo, size), size), :]

    for i, (d, side, zi, cond) in enumerate(places):
        slot = slot_of(zi, x, k)
        here = own.at[pl.ds(lo, size), :] if d == 0 else part(slot)
        if d:
            comm.step([(part(slot), sem_z[i])], [], cond)
        for way in (1, -1):
            if d < nz - 1 and side != way:
                on = (z < nz - 1) if way == 1 else (z > 0)
                if cond is not None:
                    on = on & cond
                to = at.device((z + nz + way) % nz, at.y, x, k)
                j = next(j for j, p in enumerate(places) if p[0] == d + 1 and p[1] == -way)
                comm.step([], [(here, part(slot), sem_z[j], to)], on)
        comm.step(
            [],
            [
                (here, part(slot), sem_x[i], comm.to_x),
                (here, part(slot), sem_k[i], comm.to_k),
            ],
            cond,
        )
        if d == 0:
            moved = comm.move(here, part(slot))
        yield
    for i, (d, side, zi, cond) in enumerate(places):
        slot = slot_of(zi, 1 - x, k)
        comm.step(
            [(part(slot), sem_x[i])], [(part(slot), part(slot), sem_k[n + i], comm.to_k)], cond
        )
        yield
    for h, xh in enumerate((x, 1 - x)):
        for i, (d, side, zi, cond) in enumerate(places):
            comm.step([(part(slot_of(zi, xh, 1 - k)), sem_k[h * n + i])], [], cond)
    moved()


def add_rows(dst, terms):
    rows = dst.shape[0]
    step = math.gcd(rows, 16)

    def some_rows(i, _):
        r = pl.ds(pl.multiple_of(i * step, step), step)
        total = terms[0][r, :].astype(f32)
        for term in terms[1:]:
            total = total + term[r, :].astype(f32)
        dst[r, :] = total.astype(dst.dtype)
        return 0

    lax.fori_loop(0, rows // step, some_rows, 0)


def far_first(at):
    nz = at.nz
    orders = []
    for z in range(nz):
        others = sorted((c for c in range(nz) if c != z), key=lambda c: (-abs(c - z), c))
        orders.append([(abs(c - z), 1 if c > z else -1, c) for c in others] + [(0, 0, z)])
    here = [1 - ((at.z - c) * (at.z - c) + nz * nz - 1) // (nz * nz) for c in range(nz)]
    return [
        tuple(sum(here[c] * orders[c][t][i] for c in range(nz)) for i in range(3))
        for t in range(nz)
    ]


class Scatter:
    def __init__(self, comm, p_ref, bufs, total, lo, size):
        nz = comm.at.nz
        self.comm, self.p_ref, self.bufs = comm, p_ref, bufs
        self.range = pl.ds(lo, size)
        self.total = total.at[self.range, :]
        self.targets = far_first(comm.at)
        self.sem_k, self.sem_x = comm.sems(2 * nz), comm.sems(nz)
        self.sem_z = comm.used
        comm.sems(2 * nz)

    def buf(self, b, j):
        return self.bufs[b].at[j, self.range, :]

    def mine(self, zi, flip, core):
        x = self.comm.at.x
        return self.p_ref.at[slot_of(zi, 1 - x if flip else x, core), self.range, :]

    def passing(self, side, d):
        i = (side + 1) // 2 * self.comm.at.nz + d
        return self.buf(2, i), self.comm.pool.at[self.sem_z + i]

    def first(self, t):
        comm, nz, k = self.comm, self.comm.at.nz, self.comm.at.k
        zi = self.targets[t][2]
        comm.step(
            [],
            [
                (self.mine(zi, flip, 1 - k), self.buf(0, flip * nz + zi),
                 self.sem_k[flip * nz + t], comm.to_k)
                for flip in (1, 0)
            ],
        )

    def second(self, t):
        comm, nz, k = self.comm, self.comm.at.nz, self.comm.at.k
        zi = self.targets[t][2]
        b = self.buf(0, nz + zi)
        comm.step(
            [(b, self.sem_k[nz + t])],
            [(b, self.buf(1, zi), self.sem_x[t], comm.to_x)],
            None,
            lambda: add_rows(b, [b, self.mine(zi, 1, k)]),
        )

    def third(self, t):
        comm, at = self.comm, self.comm.at
        z, nz, k = at.z, at.nz, at.k
        d, side, zi = self.targets[t]
        b, landed = self.buf(0, zi), self.buf(1, zi)
        terms = [b, self.mine(zi, 0, k), landed]
        comm.arrive(b, self.sem_k[t])
        comm.arrive(landed, self.sem_x[t])
        if t == nz - 1:
            add_rows(self.total, terms)
            for way, on in ((1, z > 0), (-1, z < nz - 1)):
                buf, sem = self.passing(way, 0)

                @pl.when(on)
                def _():
                    comm.arrive(buf, sem)
                    add_rows(self.total, [self.total, buf])

            return
        add_rows(b, terms)
        buf, sem = self.passing(side, d)
        behind = z - side

        @pl.when((behind >= 0) & (behind < nz))
        def _():
            comm.arrive(buf, sem)
            add_rows(b, [b, buf])

        dst, sem = self.passing(side, d - 1)
        comm.step([], [(b, dst, sem, at.device(z + side, at.y, at.x, k))])

    def steps(self, produce=None):
        nz = self.comm.at.nz
        for i in range(nz + 2):
            if i < nz:
                if produce is not None:
                    produce(self.targets[i][2])
                self.first(i)
            yield
            for stage, lag in ((self.second, 1), (self.third, 2)):
                if 0 <= i - lag < nz:
                    stage(i - lag)
                    yield


def scatter_bufs(nz, rows, width):
    return [pltpu.VMEM((n * nz, rows, width), bf16) for n in (2, 1, 2)]


def along(ref, axis, i, size):
    r = pl.ds(pl.multiple_of(i * size, size), size)
    before = (slice(None),) * (len(ref.shape) - axis)
    return ref.at[before + (r,) + (slice(None),) * (axis - 1)]


class Swap:
    def __init__(self, array, unit_axis, feature_axis, units, depth, shape, plane=None, groups=1):
        self.array, self.shape, self.plane = array, shape, plane
        self.unit_axis, self.feature_axis, self.units, self.depth = unit_axis, feature_axis, units, depth
        self.groups = groups if feature_axis == 2 else 1
        self.out = jax.ShapeDtypeStruct(shape, bf16)

    def of_units(self, ref, z):
        if self.plane is not None:
            ref = ref.at[self.plane]
        return along(ref, self.unit_axis, z, self.units)

    def of_features(self, ref, z, y):
        return along(ref, self.feature_axis, 2 * z + y, self.depth)

    def runs(self, ref, nz, z, y):
        if self.groups == 1:
            return [self.of_features(ref, z, y)]
        r = self.depth // self.groups
        return [along(ref, 2, i * 2 * nz + 2 * z + y, r) for i in range(self.groups)]

    def cuts(self, piece):
        if self.groups == 1:
            return [piece]
        r = self.depth // self.groups
        return [along(piece, 2, i, r) for i in range(self.groups)]


def swap_in(comm, one, src, dst):
    at = comm.at
    z, y, x, k, nz = at.z, at.y, at.x, at.k, at.nz
    sem_z = [comm.sems(one.groups) for _ in range(nz)]
    sem_y = [comm.sems(one.groups) for _ in range(nz)]
    moved = []

    def sends():
        mine = one.runs(dst, nz, z, y)
        for d in range(1, nz):
            zi = (z + d) % nz
            parts = one.cuts(one.of_units(src, zi))
            for part, to, sem in zip(parts, mine, sem_z[d]):
                comm.step([], [(part, to, sem, at.device(zi, y, x, k))])
            yield
        for part, to, sem in zip(one.cuts(one.of_units(src, z)), mine, sem_y[0]):
            comm.step([], [(part, to, sem, comm.to_y)])
            moved.append(comm.move(part, to))
        yield

    def passes():
        for d in range(1, nz):
            for run, sem, on in zip(one.runs(dst, nz, (z + nz - d) % nz, y), sem_z[d], sem_y[d]):
                comm.step([(run, sem)], [(run, run, on, comm.to_y)])
            yield

    def arrivals():
        for d in range(nz):
            for run, sem in zip(one.runs(dst, nz, (z + nz - d) % nz, 1 - y), sem_y[d]):
                comm.arrive(run, sem)
        for wait in moved:
            wait()

    return sends(), passes(), arrivals


def add_piece(dst, src):
    if len(dst.shape) == 3:
        for p in range(dst.shape[0]):
            add_rows(dst.at[p], [dst.at[p], src.at[p]])
    else:
        add_rows(dst, [dst, src])


def swap_out_y(comm, one, src, landed):
    at = comm.at
    z, y, nz = at.z, at.y, at.nz
    order = list(range(1, nz)) + [0]
    sems = comm.sems(nz)

    def sends():
        for d in order:
            zi = (z + d) % nz
            comm.step([], [(one.of_features(src, zi, 1 - y), landed.at[zi], sems[d], comm.to_y)])
            yield

    def sums():
        for d in order:
            zi = (z + d) % nz
            comm.arrive(landed.at[zi], sems[d])
            add_piece(landed.at[zi], one.of_features(src, zi, y))
            yield

    return sends(), sums()


def swap_out_z(comm, one, summed, dst):
    at = comm.at
    z, y, x, k, nz = at.z, at.y, at.x, at.k, at.nz
    mine = one.of_units(dst, z)
    sems = comm.sems(nz)
    for d in list(range(1, nz)) + [0]:
        zi = (z + d) % nz
        if d:
            comm.step([], [(summed.at[zi], mine, sems[d], at.device(zi, y, x, k))])
            comm.late.append((one.of_units(dst, (z + nz - d) % nz), sems[d]))
        else:
            comm.keep(summed.at[zi], mine)
        yield


def paired(first, second):
    for _ in first:
        next(second, None)
        yield
    yield from second


def lagged(first, second, lag):
    n = 0
    for _ in first:
        n += 1
        if n > lag:
            next(second, None)
        yield
    yield from second


def chain(*many):
    for steps in many:
        yield from steps


def landing(nz, one, user_shape):
    shape = list(user_shape)
    shape[len(shape) - one.feature_axis] = one.depth
    return pltpu.VMEM((nz, *shape), bf16)


def comm_kernel(nz, groups, work, swaps, extra, n_in, n_out, *refs):
    given = [one for one in swaps if one.array is not None]
    m, g = len(swaps), len(given)
    ins, srcs = refs[:n_in], refs[n_in : n_in + g]
    outs = refs[n_in + g : n_in + g + n_out]
    dsts = refs[n_in + g + n_out : n_in + g + n_out + m]
    scratch = refs[n_in + g + n_out + m :]
    comm = Comm(Place(nz), scratch[-1], groups)
    work(comm, (swaps + extra, srcs, dsts), ins, outs, scratch[:-1])
    comm.finish()


def comm_call(name, nz, collective, work, ins, outs, scratch, swaps, swap_spec=ANY, vmem=48, groups=1, extra=()):
    given = [one.array for one in swaps if one.array is not None]
    return pl.pallas_call(
        functools.partial(comm_kernel, nz, groups, work, swaps, list(extra), len(ins), len(outs)),
        out_shape=[jax.ShapeDtypeStruct(s, d) for s, d, _ in outs] + [one.out for one in swaps],
        in_specs=[s for _, s in ins] + [swap_spec] * len(given),
        out_specs=[s for _, _, s in outs] + [ANY] * len(swaps),
        scratch_shapes=scratch + [DMA((700,))],
        compiler_params=pltpu.CompilerParams(
            collective_id=collective, has_side_effects=True, vmem_limit_bytes=vmem * 2**20
        ),
        name=name,
    )(*[v for v, _ in ins], *given)


def by_rows(lo, size, do):
    step = math.gcd(size, 16)

    def some_rows(i, _):
        do(pl.ds(pl.multiple_of(lo + i * step, step), step))
        return 0

    lax.fori_loop(0, size // step, some_rows, 0)


def two_parts(rows):
    return [(0, rows // 2), (rows // 2, rows // 2)]


def making_steps(nz):
    return 3 * nz - 5


def feature_pieces(nz, groups, d_model):
    a = 2 * nz
    r = d_model // a // groups
    return [(c, i * r, (i * a + c) * r, r) for c in range(a) for i in range(groups)]


def sum_gains(comm, groups, sums, sorted_sums, landed, total):
    at = comm.at
    z, y, x, k, nz = at.z, at.y, at.x, at.k, at.nz
    for c, lo, col, r in feature_pieces(nz, groups, sums.shape[1]):
        sorted_sums[c % 2, c // 2, :, lo : lo + r] = sums[:, col : col + r]
    sem = comm.sems(4 + nz)
    comm.step([], [(sorted_sums.at[1 - y], landed.at[pl.ds(0, nz)], sem[0], comm.to_y)])
    comm.arrive(landed.at[pl.ds(0, nz)], sem[0])
    sorted_sums[y] += landed[0:nz]
    for d in range(1, nz):
        zi = (z + d) % nz
        comm.step([], [(sorted_sums.at[y, zi], landed.at[nz + d], sem[d], at.device(zi, y, x, k))])
    total[...] = sorted_sums[y, z]
    for d in range(1, nz):
        comm.arrive(landed.at[nz + d], sem[d])
        total[...] += landed[nz + d]
    landed[nz] = total[...]
    for i, to in enumerate((comm.to_k, comm.to_x, comm.to_xk)):
        comm.step([], [(landed.at[nz], landed.at[2 * nz + i], sem[nz + i], to)])
    for i in range(3):
        comm.arrive(landed.at[2 * nz + i], sem[nz + i])
        total[...] += landed[2 * nz + i]


def gains_of_group(comm, groups, gain_ref, landed, gains):
    at = comm.at
    z, y, x, k, nz = at.z, at.y, at.x, at.k, at.nz
    sem = comm.sems(nz + 1)
    for d in range(1, nz):
        to = at.device((z + d) % nz, y, x, k)
        comm.step([], [(gain_ref, landed.at[y, z], sem[d], to)])
    landed[y, z] = gain_ref[...]
    yield
    for d in range(1, nz):
        comm.arrive(landed.at[y, (z + nz - d) % nz], sem[d])
    comm.step([], [(landed.at[y], landed.at[y], sem[0], comm.to_y)])
    comm.arrive(landed.at[1 - y], sem[0])
    for c, lo, col, r in feature_pieces(nz, groups, gains.shape[1]):
        gains[:, col : col + r] = landed[c % 2, c // 2, :, lo : lo + r].astype(f32)


def product_into(p_ref, rows, at_slot, lhs, rhs, rhs_dims):
    n = p_ref.shape[2]
    wide = math.gcd(n, 512)
    count = lhs[0].shape[0] // rows
    for j in range(n // wide):
        cols = slice(j * wide, (j + 1) * wide)
        total = None
        for one, right, dims in zip(lhs, rhs, rhs_dims):
            block = right[:, cols] if dims == 0 else right[cols, :]
            term = lax.dot_general(one, block, (((1,), (dims,)), ((), ())), preferred_element_type=f32)
            total = term if total is None else total + term
        p_ref[pl.ds(at_slot, count), :, cols] = total.astype(bf16).reshape(count, rows, wide)


def row_blocks(rows, keys, do):
    step = math.gcd(rows, 256)
    fine = max(16, min(128, 128 * 2048 // keys))
    for i in range(rows // step):

        def some(j, _):
            do(pl.ds(pl.multiple_of(i * step + j * fine, fine), fine))
            return 0

        lax.fori_loop(0, step // fine, some, 0)
        yield


def attend(heads, q_ref, k_ref, v_ref, at_q, at_k, o_ref, lse_ref):
    def block(r):
        visible = at_k[...] <= at_q[r, :]
        for h in range(heads):
            c = slice(h * HD, (h + 1) * HD)
            scores = lax.dot_general(
                q_ref[r, c], k_ref[:, c], (((1,), (1,)), ((), ())), preferred_element_type=f32
            )
            scores = jnp.where(visible, scores, -1e30)
            peak = jnp.max(scores, axis=-1, keepdims=True)
            weights = jnp.exp(scores - peak)
            total = jnp.sum(weights, axis=-1, keepdims=True)
            probs = (weights * (1.0 / total)).astype(bf16)
            o_ref[r, c] = jnp.dot(probs, v_ref[:, c], preferred_element_type=f32).astype(bf16)
            lse_ref[r, h : h + 1] = peak + jnp.log(total)

    yield from row_blocks(q_ref.shape[0], k_ref.shape[0], block)


def attend_back(heads, q_ref, k_ref, v_ref, at_q, at_k, o_ref, lse_ref, do_ref, dq_ref, dk_ref, dv_ref):
    over_rows = (((0,), (0,)), ((), ()))
    over_cols = (((1,), (1,)), ((), ()))
    dk_ref[...] = jnp.zeros_like(dk_ref)
    dv_ref[...] = jnp.zeros_like(dv_ref)

    def block(r):
        visible = at_k[...] <= at_q[r, :]
        for h in range(heads):
            c = slice(h * HD, (h + 1) * HD)
            q, grad = q_ref[r, c], do_ref[r, c]
            scores = lax.dot_general(q, k_ref[:, c], over_cols, preferred_element_type=f32)
            scores = jnp.where(visible, scores, -1e30)
            probs = jnp.exp(scores - lse_ref[r, h : h + 1])
            delta = jnp.sum(
                grad.astype(f32) * o_ref[r, c].astype(f32), axis=-1, keepdims=True
            )
            prob_grad = lax.dot_general(grad, v_ref[:, c], over_cols, preferred_element_type=f32)
            score_grad = (probs * (prob_grad - delta)).astype(bf16)
            dq_ref[r, c] = jnp.dot(score_grad, k_ref[:, c], preferred_element_type=f32) * HD ** (-0.5)
            dk_ref[c, :] += lax.dot_general(q, score_grad, over_rows, preferred_element_type=f32)
            dv_ref[c, :] += lax.dot_general(
                grad, probs.astype(bf16), over_rows, preferred_element_type=f32
            )

    yield from row_blocks(q_ref.shape[0], k_ref.shape[0], block)


def other_halves(u):
    width = u.shape[1]
    low = lax.broadcasted_iota(jnp.int32, (1, width), 1) % HD < HD // 2
    return jnp.where(low, pltpu.roll(u, width - HD // 2, 1), pltpu.roll(u, HD // 2, 1))


def forward_work(heads, groups, comm, swap, ins, outs, scratch):
    x_ref, gain_ref, cos, sin, at_q, at_k = ins
    gains, q_ref, o_ref, lse_ref, hidden, rows_attn, k_out, v_out, rows_mlp = outs
    normed, landed, rows_v, qkv_v, out_v, k_all, v_all, p_ref = scratch[:8]
    bufs = scratch[8:]
    swaps, srcs, dsts = swap
    at = comm.at
    y, nz = at.y, at.nz
    rows, d_model = x_ref.shape
    tall = 4 * rows
    keys = q_ref.shape[0]
    width = q_ref.shape[1]

    places = (qkv_v, out_v) + tuple(dsts[2:])
    qkv, out, down, gate, up = [swap_in(comm, *v) for v in zip(swaps, srcs, places)]
    gaining = gains_of_group(comm, groups, gain_ref, landed, gains)
    advance(gaining, 1)
    advance(qkv[0], nz - 1)
    exhaust(gaining, qkv[0])

    def norm_1(r):
        x = x_ref[r, :].astype(f32)
        normed[r, :] = (x * inv_rms(x) * gains[0:1, :]).astype(bf16)

    by_rows(0, rows, norm_1)
    shards = gather_steps(comm, normed, rows_v, 0, rows)
    advance(shards, z_steps(at))
    take_turns(shards, chain(out[0], qkv[1], down[0]))
    qkv[2]()
    comm.keep(qkv_v, dsts[0])
    comm.keep(rows_v, rows_attn)

    def half(ref, g, yy):
        return ref.at[pl.ds(pl.multiple_of((yy * groups + g) * keys, keys), keys), :]

    group = at.first // (2 * nz)
    mine = [half(ref, group, y) for ref in (k_all, v_all)]

    def project(i, _):
        r = pl.ds(pl.multiple_of(i * tall, tall), tall)
        block = rows_v[r, :]

        def turned(p):
            u = jnp.dot(block, qkv_v[p], preferred_element_type=f32)
            return (u * cos[r, :] + other_halves(u) * sin[r, :]).astype(bf16)

        q_ref[r, :] = turned(0) * jnp.asarray(HD ** (-0.5), bf16)
        mine[0][r, :] = turned(1)
        mine[1][r, :] = jnp.dot(block, qkv_v[2], preferred_element_type=f32).astype(bf16)
        return 0

    lax.fori_loop(0, nz, project, 0)
    sem = comm.sems(4 * groups)
    for i, ref in enumerate(mine):
        comm.step([], [(ref, ref, sem[i], comm.to_y)])
        for g, f, device in comm.afar:
            comm.step([], [(ref, ref, sem[2 + (2 * g + f) * 2 + i - 2], device)])
    exhaust(gate[0], out[1])
    out[2]()
    comm.keep(out_v, dsts[1])
    for i, (ref, dst) in enumerate(((k_all, k_out), (v_all, v_out))):
        comm.arrive(half(ref, group, 1 - y), sem[i])
        for g, f, device in comm.afar:
            come = half(ref, (group + groups - g) % groups, y + f * (1 - 2 * y))
            comm.arrive(come, sem[2 + (2 * g + f) * 2 + i - 2])
        comm.keep(ref, dst)
    take_turns(
        attend(heads, q_ref, k_all, v_all, at_q, at_k, o_ref, lse_ref), chain(up[0], down[1], gate[1])
    )

    def norm_2(r):
        h = hidden[r, :] + x_ref[r, :].astype(f32)
        hidden[r, :] = h
        normed_2[r, :] = (h * inv_rms(h) * gains[1:2, :]).astype(bf16)

    def produce(zi):
        r = pl.ds(pl.multiple_of(zi * tall, tall), tall)
        product_into(p_ref, rows, zi * 4, [o_ref[r, :]], [out_v], [0])

    normed_2, total = bufs[3], bufs[4]

    def part(lo, size, making):
        yield from Scatter(comm, p_ref, bufs[:3], total, lo, size).steps(making)
        r = pl.ds(lo, size)
        for c, piece, col, n in feature_pieces(nz, groups, d_model) if groups > 1 else [(0, 0, 0, d_model)]:
            frm = c * (d_model // (2 * nz)) + piece
            hidden[r, col : col + n] = total[r, frm : frm + n]
        by_rows(lo, size, norm_2)
        yield
        yield from gather_steps(comm, normed_2, rows_mlp, lo, size)

    front, rear = [part(lo, size, None if lo else produce) for lo, size in two_parts(rows)]
    advance(front, making_steps(nz))
    take_turns(lagged(front, rear, 1), up[1])
    for one in (down, gate, up):
        one[2]()


def norm_back(grad, unit, rms, gain):
    unit_grad = grad * gain
    return rms * (unit_grad - unit * jnp.mean(unit_grad * unit, axis=-1, keepdims=True))


def back_work(groups, comm, swap, ins, outs, scratch):
    rows_mlp, gate_hbm, up_hbm, dn_hbm, hidden, dy_ref, gains = ins
    residual, branch_rows, gain_sum, block_out, gate_out, up_out = outs
    total, rounded, p_ref, q_ref, pre, gates, n2, dy, gate_g, up_g, dn_g, dn_landed, gate_landed = scratch[:13]
    bufs, bufs_q, total_q, gate_w, up_w, dn_w = scratch[13:16], scratch[16:19], *scratch[19:]
    (down, gate_swap), _, dsts = swap
    at = comm.at
    nz = at.nz
    rows = hidden.shape[0]
    tall = 4 * rows
    gain_sum[...] = jnp.zeros_like(gain_sum)
    weights_here = [
        comm.move(src, dst) for src, dst in ((gate_hbm, gate_w), (up_hbm, up_w), (dn_hbm, dn_w))
    ]
    sems = comm.sems(nz)

    def load(t, zi):
        r = pl.ds(pl.multiple_of(zi * tall, tall), tall)
        return pltpu.make_async_copy(rows_mlp.at[r, :], n2.at[r, :], sems[t])

    for t, target in enumerate(far_first(at)):
        load(t, target[2]).start()
    turn = iter(range(nz))

    def forward(zi):
        load(next(turn), zi).wait()
        r = pl.ds(pl.multiple_of(zi * tall, tall), tall)
        x = n2[r, :]
        gate = jnp.dot(x, gate_w[...], preferred_element_type=f32)
        up = jnp.dot(x, up_w[...], preferred_element_type=f32)
        pre[0, r, :] = gate
        pre[1, r, :] = up
        hid = (gate * jax.nn.sigmoid(gate) * up).astype(bf16)
        gates[2, r, :] = hid
        product_into(q_ref, rows, zi * 4, [hid], [dn_w], [0])

    def backward(zi):
        r = pl.ds(pl.multiple_of(zi * tall, tall), tall)
        grad = lax.dot_general(
            dy[r, :], dn_w[...], (((1,), (1,)), ((), ())), preferred_element_type=f32
        )
        gate, up = pre[0, r, :], pre[1, r, :]
        sig = jax.nn.sigmoid(gate)
        gate_grad = (grad * up * (sig * (1.0 + gate * (1.0 - sig)))).astype(bf16)
        up_grad = (grad * (gate * sig)).astype(bf16)
        gates[0, r, :] = gate_grad
        gates[1, r, :] = up_grad
        product_into(p_ref, rows, zi * 4, [gate_grad, up_grad], [gate_w, up_w], [1, 1])

    def back(r):
        h = hidden[r, :]
        rms = inv_rms(h)
        unit, grad = h * rms, total[r, :]
        gain_sum[...] += jnp.sum(grad * unit, axis=0, keepdims=True)
        dh = dy_ref[r, :].astype(f32) + norm_back(grad, unit, rms, gains[1:2, :])
        residual[r, :] = dh
        rounded[r, :] = dh.astype(bf16)

    def out(r):
        block_out[r, :] = (hidden[r, :] + total_q[r, :]).astype(bf16)

    def gradients(which):
        d_model = n2.shape[1]
        depth = d_model // (2 * nz)
        over_rows = (((0,), (0,)), ((), ()))
        pieces = feature_pieces(nz, groups, d_model)
        per = max(1, len(pieces) // 4)
        for j in range(0, len(pieces), per):
            for c, lo, col, r in pieces[j : j + per]:
                f, to = slice(col, col + r), slice(c * depth + lo, c * depth + lo + r)
                if which == 2:
                    dn_g[:, to] = lax.dot_general(
                        gates[2], dy[:, f], over_rows, preferred_element_type=f32
                    ).astype(bf16)
                else:
                    (gate_g, up_g)[which][to, :] = lax.dot_general(
                        n2[:, f], gates[which], over_rows, preferred_element_type=f32
                    ).astype(bf16)
            yield

    def output():
        yield from Scatter(comm, q_ref, bufs_q, total_q, 0, rows).steps(forward)
        by_rows(0, rows, out)

    def part(lo, size, making):
        yield from Scatter(comm, p_ref, bufs, total, lo, size).steps(making)
        by_rows(lo, size, back)
        yield
        yield from gather_steps(comm, rounded, branch_rows, lo, size)

    shards = gather_steps(comm, dy_ref, dy, 0, rows)
    side = output()
    advance(shards, 1)
    for here in weights_here:
        here()
    for _ in range(making_steps(nz)):
        next(side)
        advance(shards, 1)
    for _ in shards:
        next(side, None)
    front, rear = [part(lo, size, None if lo else backward) for lo, size in two_parts(rows)]
    for _ in range(making_steps(nz)):
        next(front)
        advance(side, 1)
    down_sends, down_sums = swap_out_y(comm, down, dn_g, dn_landed)
    gate_sends, gate_sums = swap_out_y(comm, gate_swap, gate_g, gate_landed)

    def weights():
        yield from gradients(2)
        yield from down_sends
        yield from gradients(0)
        yield from gate_sends
        yield from gradients(1)
        comm.keep(up_g, up_out)
        yield from paired(down_sums, swap_out_z(comm, down, dn_landed, dsts[0]))
        yield from gate_sums

    take_turns(lagged(front, rear, 1), side, weights())
    comm.keep(gate_landed, gate_out)


def tail_work(heads, groups, comm, swap, ins, outs, scratch):
    (q_ref, k_ref, v_ref, at_q, at_k, o_ref, lse_ref, branch_rows, out_w, gate_sum, up_grad,
     rows_attn, cos, sin, qkv_w, residual, x_ref, gains, gain_sum_2) = ins
    grad_in, gain_out = outs
    (dq_ref, dk_ref, dv_ref, going, come, up_landed, out_landed, q_landed, kv_landed, proj, n1,
     q_g, kv_g, total, gain_sums, sorted_sums, landed, p_ref, dh, do_ref, out_g) = scratch[:21]
    bufs = scratch[21:]
    (gate, up, out, q_swap, kv_swap), _, dsts = swap
    dh_here = comm.move(branch_rows, dh)
    n1_here = comm.move(rows_attn, n1)
    at = comm.at
    y, nz = at.y, at.nz
    keys, width = q_ref.shape
    rows, d_model = x_ref.shape
    tall = 4 * rows
    gain_sums[0:1, :] = jnp.zeros_like(gain_sum_2)
    gain_sums[1:2, :] = gain_sum_2[...]

    up_sends, up_sums = swap_out_y(comm, up, up_grad, up_landed)
    exhaust(up_sends, swap_out_z(comm, gate, gate_sum, dsts[0]))
    depth = d_model // (2 * nz)
    pieces = feature_pieces(nz, groups, d_model)
    dh_here()

    def attention_grads(i, _):
        r = pl.ds(pl.multiple_of(i * tall, tall), tall)
        do_ref[r, :] = lax.dot_general(
            dh[r, :], out_w[...], (((1,), (1,)), ((), ())), preferred_element_type=f32
        ).astype(bf16)
        return 0

    lax.fori_loop(0, nz, attention_grads, 0)
    for c, lo, col, n in pieces:
        out_g[:, c * depth + lo : c * depth + lo + n] = lax.dot_general(
            o_ref[...], dh[:, col : col + n], (((0,), (0,)), ((), ())), preferred_element_type=f32
        ).astype(bf16)
    out_sends, out_sums = swap_out_y(comm, out, out_g, out_landed)
    exhaust(out_sends)
    more = chain(
        paired(up_sums, swap_out_z(comm, up, up_landed, dsts[1])),
        paired(out_sums, swap_out_z(comm, out, out_landed, dsts[2])),
    )
    compute = attend_back(
        heads, q_ref, k_ref, v_ref, at_q, at_k, o_ref, lse_ref, do_ref, dq_ref, dk_ref, dv_ref
    )
    take_turns(compute, more)

    group = at.first // (2 * nz)

    def share(ref, g, yy):
        return ref.at[:, pl.ds(pl.multiple_of((yy * groups + g) * keys, keys), keys)]

    others = [(0, 1, comm.to_y)] + comm.afar
    sem = comm.sems(2 * len(others))
    for j, (g, f, device) in enumerate(others):
        for i, ref in enumerate((dk_ref, dv_ref)):
            theirs = share(ref, (group + g) % groups, y + f * (1 - 2 * y))
            going[j, i] = theirs[...].astype(bf16)
            comm.step([], [(going.at[j, i], come.at[j, i], sem[2 * j + i], device)])

    def unturned(u, r):
        return (u * cos[r, :] - other_halves(u) * sin[r, :]).astype(bf16)

    every = pl.ds(0, keys)
    proj[:, 0:width] = unturned(dq_ref[...], every)

    def product(col, n, cols):
        return lax.dot_general(
            n1[:, col : col + n], proj[:, cols], (((0,), (0,)), ((), ())),
            preferred_element_type=f32,
        ).astype(bf16)

    n1_here()
    for c, lo, col, n in pieces:
        q_g[c * depth + lo : c * depth + lo + n, :] = product(col, n, slice(0, width))
    q_sends, q_sums = swap_out_y(comm, q_swap, q_g, q_landed)
    exhaust(q_sends)
    for i, ref in enumerate((dk_ref, dv_ref)):
        grad = share(ref, group, y)[...]
        for j in range(len(others)):
            comm.arrive(come.at[j, i], sem[2 * j + i])
            grad = grad + come[j, i].astype(f32)
        grad = grad.T
        cols = slice((i + 1) * width, (i + 2) * width)
        proj[:, cols] = unturned(grad, every) if i == 0 else grad.astype(bf16)

    def back(r):
        x = x_ref[r, :].astype(f32)
        rms = inv_rms(x)
        unit, grad = x * rms, total[r, :]
        gain_sums[0:1, :] += jnp.sum(grad * unit, axis=0, keepdims=True)
        grad_in[r, :] = residual[r, :] + norm_back(grad, unit, rms, gains[0:1, :])

    def produce(zi):
        r = pl.ds(pl.multiple_of(zi * tall, tall), tall)
        lhs = [proj[r, p * width : (p + 1) * width] for p in range(3)]
        product_into(p_ref, rows, zi * 4, lhs, [qkv_w.at[p] for p in range(3)], [1] * 3)

    kv_sends, kv_sums = swap_out_y(comm, kv_swap, kv_g, kv_landed)

    def weights():
        per = max(1, len(pieces) // 4)
        for j in range(0, len(pieces), per):
            for c, lo, col, n in pieces[j : j + per]:
                grad = product(col, n, slice(width, 3 * width))
                for p in (0, 1):
                    kv_g[p, c * depth + lo : c * depth + lo + n, :] = grad[:, p * width : (p + 1) * width]
            yield
        yield from kv_sends
        yield from paired(q_sums, swap_out_z(comm, q_swap, q_landed, dsts[3]))
        yield from paired(kv_sums, swap_out_z(comm, kv_swap, kv_landed, dsts[4]))

    steps = Scatter(comm, p_ref, bufs, total, 0, rows).steps(produce)
    advance(steps, making_steps(nz))
    take_turns(weights(), steps)
    by_rows(0, rows, back)
    sum_gains(comm, groups, gain_sums, sorted_sums, landed, gain_out)


def body(
    block_input,
    qkv_weight,
    out_weight,
    gate_up_weight,
    down_weight,
    norm_gains,
    positions,
    layer_output_gradient,
):
    n_ctx, n_tp = lax.axis_size("ctx"), lax.axis_size("tp")
    nz = math.gcd(qkv_weight.shape[2] // HD, n_ctx // 2)
    nz = math.gcd(nz, 4)
    a = 2 * nz
    b = n_ctx // a
    assert n_tp == 4
    depth = qkv_weight.shape[1] * b
    d_model = depth * a
    width = qkv_weight.shape[2] // nz
    heads = width // HD
    units = down_weight.shape[0] // nz
    rows = block_input.shape[0]
    across = [[i * a + j for i in range(b)] for j in range(a)]

    def over_groups(v, axis):
        return lax.all_gather(v, "ctx", axis=axis, tiled=True, axis_index_groups=across) if b > 1 else v

    def to_groups(v, axis):
        if b == 1:
            return v
        return lax.psum_scatter(
            v, "ctx", scatter_dimension=axis, tiled=True, axis_index_groups=across
        )

    def model_order(v, axis):
        if b == 1:
            return v
        s = v.shape
        w = v.reshape(s[:axis] + (a, b, depth // b) + s[axis + 1 :])
        return jnp.swapaxes(w, axis, axis + 1).reshape(s)

    my_gains = over_groups(norm_gains, 1)
    group_rows = 4 * nz * rows
    n_keys = 2 * b * group_rows
    y, group = lax.axis_index("ctx") % 2, lax.axis_index("ctx") // a
    by_place = positions.reshape(b, nz, 2, n_tp * rows)
    key_pos = by_place.transpose(2, 0, 1, 3).reshape(2 * b, group_rows)
    own_pos = lax.dynamic_index_in_dim(key_pos, y * b + group, 0, keepdims=False)
    cos_tab, sin_tab = rope_tables(own_pos, HD)
    cos_wide = jnp.tile(cos_tab[:, 0, :], (1, 2 * heads))
    sin_wide = jnp.tile(jnp.concatenate([-sin_tab, sin_tab], axis=-1)[:, 0, :], (1, heads))
    places = [(own_pos[:, None], VMEM), (key_pos.reshape(1, -1), VMEM)]
    gu_all = over_groups(gate_up_weight, 1)
    partials = pltpu.VMEM((4 * nz, rows, d_model), bf16)
    (gains, query_bf, attn_bf, log_total, hidden, rows_attn, key_all, value_all, rows_mlp,
     qkv_w, out_w, dn_w, gate_w, up_w) = comm_call(
        "forward", nz, 0, functools.partial(forward_work, heads, b),
        [(block_input, VMEM), (my_gains, VMEM), (cos_wide, VMEM), (sin_wide, VMEM)] + places,
        [((2, d_model), f32, VMEM), ((group_rows, width), bf16, VMEM),
         ((group_rows, width), bf16, VMEM), ((group_rows, heads), f32, VMEM),
         ((rows, d_model), f32, VMEM), ((group_rows, d_model), bf16, ANY),
         ((n_keys, width), bf16, ANY), ((n_keys, width), bf16, ANY),
         ((group_rows, d_model), bf16, ANY)],
        [pltpu.VMEM((rows, d_model), bf16), pltpu.VMEM((2, nz) + my_gains.shape, bf16),
         pltpu.VMEM((group_rows, d_model), bf16), pltpu.VMEM((3, d_model, width), bf16),
         pltpu.VMEM((width, d_model), bf16), pltpu.VMEM((n_keys, width), bf16),
         pltpu.VMEM((n_keys, width), bf16), partials]
        + scatter_bufs(nz, rows, d_model)
        + [pltpu.VMEM((rows, d_model), bf16), pltpu.VMEM((rows, d_model), f32)],
        [Swap(over_groups(qkv_weight, 1), 1, 2, width, depth, (3, d_model, width), None, b),
         Swap(over_groups(out_weight, 1), 2, 1, width, depth, (width, d_model)),
         Swap(over_groups(down_weight, 1), 2, 1, units, depth, (units, d_model))]
        + [Swap(gu_all, 1, 2, units, depth, (d_model, units), p, b) for p in (0, 1)],
        vmem=63,
        groups=b,
    )
    out_w, dn_w = model_order(out_w, 1), model_order(dn_w, 1)
    down_swap = Swap(None, 2, 1, units, depth, (nz * units, depth))
    half_swap = Swap(None, 1, 2, units, depth, (depth, nz * units))
    residual_grad, branch_rows, gain_sum_2, block_output, gate_sum, up_grad, dn_back = comm_call(
        "back", nz, 3, functools.partial(back_work, b),
        [(rows_mlp, ANY), (gate_w, ANY), (up_w, ANY), (dn_w, ANY),
         (hidden, VMEM), (layer_output_gradient, VMEM), (gains, VMEM)],
        [((rows, d_model), f32, VMEM), ((group_rows, d_model), bf16, ANY),
         ((1, d_model), f32, VMEM), ((rows, d_model), bf16, VMEM),
         ((nz, depth, units), bf16, ANY), ((d_model, units), bf16, ANY)],
        [pltpu.VMEM((rows, d_model), f32), pltpu.VMEM((rows, d_model), bf16), partials, partials,
         pltpu.VMEM((2, group_rows, units), f32), pltpu.VMEM((3, group_rows, units), bf16),
         pltpu.VMEM((group_rows, d_model), bf16), pltpu.VMEM((group_rows, d_model), bf16),
         pltpu.VMEM((d_model, units), bf16), pltpu.VMEM((d_model, units), bf16),
         pltpu.VMEM((units, d_model), bf16),
         landing(nz, down_swap, (units, d_model)), landing(nz, half_swap, (d_model, units))]
        + scatter_bufs(nz, rows, d_model) + scatter_bufs(nz, rows, d_model)
        + [pltpu.VMEM((rows, d_model), f32), pltpu.VMEM((d_model, units), bf16),
           pltpu.VMEM((d_model, units), bf16), pltpu.VMEM((units, d_model), bf16)],
        [down_swap],
        vmem=60,
        extra=[half_swap],
    )
    out_swap = Swap(None, 2, 1, width, depth, (nz * width, depth))
    q_swap = Swap(None, 1, 2, width, depth, (depth, nz * width))
    kv_swap = Swap(None, 1, 2, width, depth, (2, depth, nz * width))
    others = 2 * b - 1
    layer_input_gradient, gain_sums, gate_back, up_back, out_back, q_back, kv_back = comm_call(
        "tail", nz, 4, functools.partial(tail_work, heads, b),
        [(query_bf, VMEM), (key_all, VMEM), (value_all, VMEM)] + places
        + [(attn_bf, VMEM), (log_total, VMEM), (branch_rows, ANY), (out_w, VMEM), (gate_sum, VMEM),
           (up_grad, VMEM),
           (rows_attn, ANY), (cos_wide, VMEM), (sin_wide, VMEM), (qkv_w, VMEM),
           (residual_grad, VMEM), (block_input, VMEM), (gains, VMEM), (gain_sum_2, VMEM)],
        [((rows, d_model), f32, VMEM), ((2, depth), f32, VMEM)],
        [pltpu.VMEM((group_rows, width), f32),
         pltpu.VMEM((width, n_keys), f32), pltpu.VMEM((width, n_keys), f32),
         pltpu.VMEM((others, 2, width, group_rows), bf16),
         pltpu.VMEM((others, 2, width, group_rows), bf16),
         landing(nz, half_swap, (d_model, units)), landing(nz, out_swap, (width, d_model)),
         landing(nz, q_swap, (d_model, width)), landing(nz, kv_swap, (2, d_model, width)),
         pltpu.VMEM((group_rows, 3 * width), bf16), pltpu.VMEM((group_rows, d_model), bf16),
         pltpu.VMEM((d_model, width), bf16), pltpu.VMEM((2, d_model, width), bf16),
         pltpu.VMEM((rows, d_model), f32), pltpu.VMEM((2, d_model), f32),
         pltpu.VMEM((2, nz, 2, depth), f32), pltpu.VMEM((2 * nz + 3, 2, depth), f32), partials,
         pltpu.VMEM((group_rows, d_model), bf16), pltpu.VMEM((group_rows, width), bf16),
         pltpu.VMEM((width, d_model), bf16)]
        + scatter_bufs(nz, rows, d_model),
        [half_swap, half_swap, out_swap, q_swap, kv_swap],
        vmem=63,
        groups=b,
    )
    gu_back = jnp.stack([gate_back, up_back])
    qkv_back = jnp.concatenate([q_back[None], kv_back])
    if b > 1:
        gain_sums = lax.psum(gain_sums, "ctx", axis_index_groups=across)
    gain_cols = d_model // (n_ctx * n_tp)
    gain_part = lax.dynamic_slice_in_dim(
        gain_sums, (group * n_tp + lax.axis_index("tp")) * gain_cols, gain_cols, 1
    )
    return (
        block_output,
        layer_input_gradient,
        to_groups(qkv_back, 1).astype(f32),
        to_groups(out_back, 1).astype(f32),
        to_groups(gu_back, 1).astype(f32),
        to_groups(dn_back, 1).astype(f32),
        gain_part,
    )


def solution(mesh):
    placed = (
        P(("ctx", "tp"), None),
        P(None, "ctx", "tp"),
        P("tp", "ctx"),
        P(None, "ctx", "tp"),
        P("tp", "ctx"),
        P(None, "ctx"),
        P(),
        P(("ctx", "tp"), None),
    )
    return jax.shard_map(
        body,
        mesh=mesh,
        in_specs=placed,
        out_specs=(
            P(("ctx", "tp"), None),
            P(("ctx", "tp"), None),
            P(None, "ctx", "tp"),
            P("tp", "ctx"),
            P(None, "ctx", "tp"),
            P("tp", "ctx"),
            P(None, ("ctx", "tp")),
        ),
        check_vma=False,
    )
```
